32 devices in a mesh: gx: 8 (over z, x), gy: 4 (over y, core).
Axes of the slice: x: 2, y: 2, z: 4, core: 2. Of those that a mesh axis runs over, the one named last changes fastest.
Arguments:
- fine_disp: float32 [3, 128, 64, 128], P(None, 'gx', 'gy'), may hold values from -12 to 12
- fine_prev: float32 [3, 128, 64, 128], P(None, 'gx', 'gy'), may hold values from -12 to 12
- coarse_disp: float32 [3, 64, 32, 256], P(None, 'gx', 'gy'), may hold values from -12 to 12
- coarse_prev: float32 [3, 64, 32, 256], P(None, 'gx', 'gy'), may hold values from -12 to 12
- fine_density: float32 [128, 64, 128], P('gx', 'gy'), may hold values from 0.6 to 1.8
- fine_lame: float32 [128, 64, 128], P('gx', 'gy'), may hold values from 0.5 to 2
- fine_rigidity: float32 [128, 64, 128], P('gx', 'gy'), may hold values from 0.3 to 1.5
- fine_metric: float32 [128, 64, 128], P('gx', 'gy'), may hold values from 0.7 to 1.4
- coarse_density: float32 [64, 32, 256], P('gx', 'gy'), may hold values from 0.6 to 1.8
- coarse_lame: float32 [64, 32, 256], P('gx', 'gy'), may hold values from 0.5 to 2
- coarse_rigidity: float32 [64, 32, 256], P('gx', 'gy'), may hold values from 0.3 to 1.5
- coarse_metric: float32 [64, 32, 256], P('gx', 'gy'), may hold values from 0.7 to 1.4
- offsets: int32 [2, 128, 64], P(None, 'gx', 'gy'), may hold values from -1 to 1
Outputs:
- fine_final: float32 [3, 128, 64, 128], P(None, 'gx', 'gy')
- coarse_final: float32 [3, 64, 32, 256], P(None, 'gx', 'gy')
- energy: float32 [3, 2], replicated
The draws below stay inside these ranges and needn't reach their ends.
All inputs are finite; a program needn't handle non-finite values.
Results may differ from the reference program's by a relative error of at most 0.00021.
Values sent between devices are 32-bit elements; how exact they have to be, the bound alone decides.
A program may use at most 64 MiB of HBM per device.

```python
import math
import jax
import jax.numpy as jnp

FZ = 128
STEPS = 3
CZ = 256
NXF = 128
NYF = 64
NXC = 64
NYC = 32


def rough_field(key, cells_x, cells_y, cells_z):
    key_scale, key_rough, key_common = jax.random.split(key, 3)
    blocks_x = (cells_x + 7) // 8
    blocks_y = (cells_y + 7) // 8
    log_scale = jax.random.uniform(key_scale, (blocks_x, blocks_y), jnp.float32, -1.1, 1.1)
    rough_part = jax.random.truncated_normal(key_rough, -4.0, 4.0, (3, cells_x, cells_y, cells_z), jnp.float32)
    amplitude = jnp.repeat(jnp.repeat(jnp.exp(log_scale), 8, axis=0), 8, axis=1)[:cells_x, :cells_y]
    return jnp.clip(rough_part * amplitude[None, :, :, None], -12.0, 12.0)


def draw_fine_disp(key, part):
    return rough_field(jax.random.fold_in(key, 11), NXF, NYF, FZ)


def draw_fine_prev(key, part):
    return rough_field(jax.random.fold_in(key, 12), NXF, NYF, FZ)


def draw_coarse_disp(key, part):
    return rough_field(jax.random.fold_in(key, 13), NXC, NYC, CZ)


def draw_coarse_prev(key, part):
    return rough_field(jax.random.fold_in(key, 14), NXC, NYC, CZ)


def touch_ends(drawn, key, least, top_value):
    spot = [jax.random.randint(jax.random.fold_in(key, axis), (), 0, length) for axis, length in enumerate(drawn.shape)]
    main_axis = drawn.shape.index(max(drawn.shape))
    next_to = spot[:main_axis] + [(spot[main_axis] + 1) % drawn.shape[main_axis]] + spot[main_axis + 1:]
    return drawn.at[tuple(spot)].set(least).at[tuple(next_to)].set(top_value)


def block_scale(own_key, shape, shards, least, top_value):
    loudness = 1.0
    for position, parts in shards:
        steps = jax.random.uniform(jax.random.fold_in(jax.random.fold_in(own_key, 6), position), (parts,), jnp.float32, least / len(shards), top_value / len(shards))
        loudness = loudness * jnp.repeat(jnp.exp(steps), shape[position] // parts).reshape((-1,) + (1,) * (len(shape) - 1 - position))
    return loudness


def setup_inputs(seed: int = 0) -> dict:
    key_of = jax.random.split(jax.random.key(seed), 14)
    return {
        "fine_disp": draw_fine_disp(jax.random.fold_in(key_of[13], 71), 0),
        "fine_prev": draw_fine_prev(jax.random.fold_in(key_of[13], 71), 0),
        "coarse_disp": draw_coarse_disp(jax.random.fold_in(key_of[13], 71), 0),
        "coarse_prev": draw_coarse_prev(jax.random.fold_in(key_of[13], 71), 0),
        "fine_density": jnp.clip(jnp.exp(math.log(1.8) - 1.0986122 * jax.random.uniform(key_of[4], (NXF, NYF, FZ), jnp.float32) ** block_scale(key_of[4], (NXF, NYF, FZ), ((0, 8), (1, 4)), -0.2, 0.2)), 0.6, 1.8),
        "fine_lame": jnp.clip(jnp.exp(math.log(2.0) - 1.3862944 * jax.random.uniform(key_of[5], (NXF, NYF, FZ), jnp.float32) ** block_scale(key_of[5], (NXF, NYF, FZ), ((0, 8), (1, 4)), -0.2, 0.2)), 0.5, 2.0),
        "fine_rigidity": jnp.clip(jnp.exp(math.log(1.5) - 1.60943787 * jax.random.uniform(key_of[6], (NXF, NYF, FZ), jnp.float32) ** block_scale(key_of[6], (NXF, NYF, FZ), ((0, 8), (1, 4)), -0.2, 0.2)), 0.3, 1.5),
        "fine_metric": jnp.clip(jnp.exp(math.log(1.4) - 0.6931472 * jax.random.uniform(key_of[7], (NXF, NYF, FZ), jnp.float32) ** block_scale(key_of[7], (NXF, NYF, FZ), ((0, 8), (1, 4)), -0.2, 0.2)), 0.7, 1.4),
        "coarse_density": jnp.clip(jnp.exp(math.log(1.8) - 1.0986122 * jax.random.uniform(key_of[8], (NXC, NYC, CZ), jnp.float32) ** block_scale(key_of[8], (NXC, NYC, CZ), ((0, 8), (1, 4)), -0.2, 0.2)), 0.6, 1.8),
        "coarse_lame": jnp.clip(jnp.exp(math.log(2.0) - 1.3862944 * jax.random.uniform(key_of[9], (NXC, NYC, CZ), jnp.float32) ** block_scale(key_of[9], (NXC, NYC, CZ), ((0, 8), (1, 4)), -0.2, 0.2)), 0.5, 2.0),
        "coarse_rigidity": jnp.clip(jnp.exp(math.log(1.5) - 1.60943787 * jax.random.uniform(key_of[10], (NXC, NYC, CZ), jnp.float32) ** block_scale(key_of[10], (NXC, NYC, CZ), ((0, 8), (1, 4)), -0.2, 0.2)), 0.3, 1.5),
        "coarse_metric": jnp.clip(jnp.exp(math.log(1.4) - 0.6931472 * jax.random.uniform(key_of[11], (NXC, NYC, CZ), jnp.float32) ** block_scale(key_of[11], (NXC, NYC, CZ), ((0, 8), (1, 4)), -0.2, 0.2)), 0.7, 1.4),
        "offsets": touch_ends(jax.random.randint(key_of[12], (2, NXF, NYF), -1, 2), jax.random.fold_in(key_of[12], 1), -1, 1).astype(jnp.int32),
    }


step_factor = 0.15


def vertical_slope(values):
    middle = 0.5 * (values[..., 2:] - values[..., :-2])
    first = values[..., 1:2] - values[..., 0:1]
    final = values[..., -1:] - values[..., -2:-1]
    return jnp.concatenate([first, middle, final], axis=-1)


def divergence(along_x, along_y, along_z, inverse):
    return 0.5 * (along_x[2:] - along_x[:-2]) + 0.5 * (along_y[:, 2:] - along_y[:, :-2]) + inverse * vertical_slope(along_z)


def interpolate(plane_ext, offsets):
    coarse_x = plane_ext.shape[1] - 4
    coarse_y = plane_ext.shape[2] - 4
    near_x = jnp.where((jnp.arange(2 * coarse_x) % 2) == 0, 0.75, 0.25)[:, None]
    near_y = jnp.where((jnp.arange(2 * coarse_y) % 2) == 0, 0.75, 0.25)[None, :]
    offset_x = offsets[0]
    offset_y = offsets[1]
    summed = jnp.zeros((3, 2 * coarse_x, 2 * coarse_y), plane_ext.dtype)
    for shift_x in (-1, 0, 1, 2):
        weight_x = jnp.where(offset_x == shift_x, near_x, 0.0) + jnp.where(offset_x + 1 == shift_x, 1.0 - near_x, 0.0)
        row_band = jnp.repeat(plane_ext[:, 2 + shift_x:2 + shift_x + coarse_x, :], 2, axis=1)
        for shift_y in (-1, 0, 1, 2):
            weight_y = jnp.where(offset_y == shift_y, near_y, 0.0) + jnp.where(offset_y + 1 == shift_y, 1.0 - near_y, 0.0)
            tile_band = jnp.repeat(row_band[:, :, 2 + shift_y:2 + shift_y + coarse_y], 2, axis=2)
            summed = summed + (weight_x * weight_y)[None] * tile_band
    return summed


def restrict(plane):
    half_x = plane.shape[1] // 2
    half_y = plane.shape[2] // 2
    return 0.25 * jnp.sum(plane.reshape(3, half_x, 2, half_y, 2), axis=(2, 4))


def elastic_rate(extended, mats_ext, div_ext, displace, top_ghost, bottom_ghost, density, lame_first, rigidity):
    wide_ext = mats_ext[0]
    inverse = mats_ext[1, 1:-1, 1:-1]
    face_x = 0.5 * (wide_ext[:-1, 1:-1] + wide_ext[1:, 1:-1])
    flux_x = face_x * (extended[:, 1:, 1:-1] - extended[:, :-1, 1:-1])
    face_y = 0.5 * (wide_ext[1:-1, :-1] + wide_ext[1:-1, 1:])
    flux_y = face_y * (extended[:, 1:-1, 1:] - extended[:, 1:-1, :-1])
    vertical = rigidity * inverse
    face_z = jnp.concatenate([vertical[:, :, :1], 0.5 * (vertical[:, :, :-1] + vertical[:, :, 1:]), vertical[:, :, -1:]], axis=2)
    column = jnp.concatenate([top_ghost[:, :, :, None], displace, bottom_ghost[:, :, :, None]], axis=3)
    flux_z = face_z * (column[:, :, :, 1:] - column[:, :, :, :-1])
    spread = (flux_x[:, 1:] - flux_x[:, :-1]) + (flux_y[:, :, 1:] - flux_y[:, :, :-1]) + (flux_z[:, :, :, 1:] - flux_z[:, :, :, :-1])
    grad_x = 0.5 * (div_ext[2:, 1:-1] - div_ext[:-2, 1:-1])
    grad_y = 0.5 * (div_ext[1:-1, 2:] - div_ext[1:-1, :-2])
    grad_z = inverse * vertical_slope(div_ext[1:-1, 1:-1])
    gradient = jnp.stack([grad_x, grad_y, grad_z])
    return spread * (inverse / density) + ((lame_first + rigidity) / density) * gradient


def energy_part(updated, displace, rate, density, metric, cell_count):
    change = updated - displace
    inner_sum = jnp.sum(change * change - step_factor * updated * rate, axis=0)
    return jnp.sum(density * metric * inner_sum) / cell_count


def reference(fine_disp, fine_prev, coarse_disp, coarse_prev, fine_density, fine_lame, fine_rigidity, fine_metric, coarse_density, coarse_lame, coarse_rigidity, coarse_metric, offsets):
    pad_cells = ((1, 1), (1, 1), (0, 0))
    pad_fields = ((0, 0), (1, 1), (1, 1), (0, 0))
    fine_mats = jnp.pad(jnp.stack([fine_rigidity * fine_metric, 1.0 / fine_metric]), pad_fields)
    coarse_mats = jnp.pad(jnp.stack([coarse_rigidity * coarse_metric, 1.0 / coarse_metric]), pad_fields)
    fine_cells = fine_disp.shape[1] * fine_disp.shape[2] * fine_disp.shape[3]
    coarse_cells = coarse_disp.shape[1] * coarse_disp.shape[2] * coarse_disp.shape[3]
    energies = []
    for step_index in range(STEPS):
        fine_ext = jnp.pad(fine_disp, pad_fields)
        coarse_ext = jnp.pad(coarse_disp, pad_fields)
        fine_div = divergence(fine_ext[0, :, 1:-1], fine_ext[1, 1:-1, :], fine_disp[2], fine_mats[1, 1:-1, 1:-1])
        coarse_div = divergence(coarse_ext[0, :, 1:-1], coarse_ext[1, 1:-1, :], coarse_disp[2], coarse_mats[1, 1:-1, 1:-1])
        fine_div_ext = jnp.pad(fine_div, pad_cells)
        coarse_div_ext = jnp.pad(coarse_div, pad_cells)
        plane_ext = jnp.pad(coarse_disp[:, :, :, 0], ((0, 0), (2, 2), (2, 2)))
        fine_bottom = interpolate(plane_ext, offsets)
        fine_top = fine_disp[:, :, :, 0]
        coarse_top = restrict(fine_disp[:, :, :, -1])
        coarse_bottom = jnp.zeros_like(coarse_top)
        fine_rate = elastic_rate(fine_ext, fine_mats, fine_div_ext, fine_disp, fine_top, fine_bottom, fine_density, fine_lame, fine_rigidity)
        coarse_rate = elastic_rate(coarse_ext, coarse_mats, coarse_div_ext, coarse_disp, coarse_top, coarse_bottom, coarse_density, coarse_lame, coarse_rigidity)
        fine_new = 2.0 * fine_disp - fine_prev + step_factor * fine_rate
        coarse_new = 2.0 * coarse_disp - coarse_prev + step_factor * coarse_rate
        energies.append(jnp.stack([
            energy_part(fine_new, fine_disp, fine_rate, fine_density, fine_metric, fine_cells),
            energy_part(coarse_new, coarse_disp, coarse_rate, coarse_density, coarse_metric, coarse_cells)]))
        fine_prev, fine_disp = fine_disp, fine_new
        coarse_prev, coarse_disp = coarse_disp, coarse_new
    return (fine_disp, coarse_disp, jnp.stack(energies))
```

```python
import functools

import jax
import jax.numpy as jnp
from jax import lax
from jax.experimental import pallas as pl
from jax.experimental.pallas import tpu as pltpu
from jax.sharding import PartitionSpec as P

STEPS = 3
FACTOR = 0.15
MESH = pl.DeviceIdType.MESH
L = 128
SIDES = ((1, 0), (-1, 0), (0, 1), (0, -1))
CORNERS = ((1, 1), (1, -1), (-1, 1), (-1, -1))


class Level:
    def __init__(self, shape):
        _, self.X, self.Y, Z = shape
        self.H = Z // L
        self.XE = self.X + 4
        self.R = self.Y + 16
        while (self.H * self.R) % 8 != 4:
            self.R += 1
        self.NB = self.Y // 8

    def row(self, c, x, h, r):
        return ((c * self.XE + x) * self.H + h) * self.R + r

    def field_rows(self):
        return self.XE * self.H * self.R


def side_pieces(lev, axis, coarse):
    out = [(c, 1, h) for c in range(3) for h in range(lev.H)]
    out += [(axis, 2, h) for h in range(lev.H)]
    if coarse:
        out += [(c, 2, 0) for c in range(3) if c != axis]
    return out


def corner_pieces(lev, coarse):
    if not coarse:
        return [(c, 1, 1, 0) for c in (0, 1)]
    out = [(c, 1, 1, h) for c in (0, 1) for h in range(1, lev.H)]
    out += [(c, a, b, 0) for c in range(3) for a in (1, 2) for b in (1, 2)]
    return out


def inner(length, d, ring):
    return length - ring if d > 0 else ring - 1


def outer(length, d, ring):
    return -ring if d > 0 else length + ring - 1


def line(lev, d, ring, h, c, place):
    if d[0]:
        return lev.row(c, 2 + place(lev.X, d[0], ring), h, 8), lev.Y, 1
    return lev.row(c, 2, h, 8 + place(lev.Y, d[1], ring)), lev.X, lev.H * lev.R


def rows_of(start, count, stride):
    return pl.ds(start, count) if stride == 1 else pl.ds(start, count, stride)


def kernel(n_x, n_y, lf, lc, *refs):
    (fd, fp, cd, cp, fden, flam, frig, fmet, cden, clam, crig, cmet, offs, fo, co, eo) = refs[:16]
    (uf0, uf1, uf2, uc0, uc1, uc2, mf, mc, rep, pair, wts, ghost,
     ss0f, ss0c, rs0f, rs0c, ssf, ssc, rsf, rsc, scf, scc, rcf, rcc,
     es, mine, box, send_sem, recv_sem, en_send, en_recv, inside) = refs[16:]
    U = ((uf0, uf1, uf2), (uc0, uc1, uc2))
    M = (mf, mc)
    levs = (lf, lc)
    sside0, rside0, sside, rside = (ss0f, ss0c), (rs0f, rs0c), (ssf, ssc), (rsf, rsc)
    scorner, rcorner = (scf, scc), (rcf, rcc)
    disp, prev, out = (fd, cd), (fp, cp), (fo, co)
    den, lam, rig, met = (fden, cden), (flam, clam), (frig, crig), (fmet, cmet)
    ix, iy = lax.axis_index("gx"), lax.axis_index("gy")

    def has(d):
        conds = []
        if d[0] > 0:
            conds.append(ix < n_x - 1)
        if d[0] < 0:
            conds.append(ix > 0)
        if d[1] > 0:
            conds.append(iy < n_y - 1)
        if d[1] < 0:
            conds.append(iy > 0)
        return functools.reduce(jnp.logical_and, conds)

    DIRS = SIDES + CORNERS
    lane = lax.broadcasted_iota(jnp.int32, (8, L), 1)
    first, last = lane == 0, lane == L - 1

    IC, WIDE, FX, FY, FZP, FZM, A, B5, BZ, EN, DIV = range(11)

    def mrow(lev, name, x, h, r):
        return name * lev.field_rows() + (x * lev.H + h) * lev.R + r

    for d in SIDES:
        @pl.when(jnp.logical_not(has(d)))
        def _(d=d):
            for lev, us, m in zip(levs, U, M):
                zero = jnp.zeros((8, L), jnp.float32)
                if d[0]:
                    xs = (0, 1) if d[0] < 0 else (lev.X + 2, lev.X + 3)
                    rs = list(range(0, lev.Y + 16, 8))
                else:
                    xs = range(lev.XE)
                    rs = (0,) if d[1] < 0 else (lev.Y + 8,)
                for x in xs:
                    for h in range(lev.H):
                        for r in rs:
                            for u in us:
                                for c in range(3):
                                    u[pl.ds(lev.row(c, x, h, r), 8), :] = zero
                            for name in (IC, WIDE, DIV):
                                m[pl.ds(mrow(lev, name, x, h, r), 8), :] = zero

    barrier = pltpu.get_barrier_semaphore()

    def signal(x, y):
        pl.semaphore_signal(barrier, inc=1, device_id={"gx": x, "gy": y}, device_id_type=MESH)

    everyone = n_x * n_y
    me = ix * n_y + iy

    def place(o):
        to = lax.rem(me + o, everyone)
        return to, lax.div(to, n_y), lax.rem(to, n_y)

    greeted = jnp.int32(0)
    for d in DIRS:
        greeted = greeted + has(d).astype(jnp.int32)

        @pl.when(has(d))
        def _(d=d):
            signal(ix + d[0], iy + d[1])

    rings = ready_rings(n_x, n_y)

    def within(d):
        x, y = ix + d[0], iy + d[1]
        return (x >= 0) & (x < n_x) & (y >= 0) & (y < n_y)

    def ready_signal(i):
        for d in rings[i]:
            @pl.when(within(d))
            def _(d=d):
                pl.semaphore_signal(
                    inside.at[i], inc=1, device_id={"gx": ix + d[0], "gy": iy + d[1]}, device_id_type=MESH
                )

    def ready_wait(i):
        pl.semaphore_wait(inside.at[i], sum(within(d).astype(jnp.int32) for d in rings[i]))

    for lev, us, u_in in zip(levs, U, disp):
        @pl.loop(0, lev.X, unroll=4)
        def _(x, lev=lev, us=us, u_in=u_in):
            for c in range(3):
                for h in range(lev.H):
                    for b in range(lev.NB):
                        us[0][pl.ds(lev.row(c, x + 2, h, 8 + 8 * b), 8), :] = (
                            u_in[c, x, pl.ds(8 * b, 8), pl.ds(h * L, L)]
                        )

    def copy(k, d, step, n):
        if k >= 4:
            s, r = scorner[n].at[step, k - 4], rcorner[n].at[step, k - 4]
        elif step == 0:
            s, r = sside0[n].at[k], rside0[n].at[k]
        else:
            s, r = sside[n].at[step - 1, k], rside[n].at[step - 1, k]
        return pltpu.make_async_remote_copy(
            src_ref=s, dst_ref=r, send_sem=send_sem.at[n, step, k],
            recv_sem=recv_sem.at[n, step, k],
            device_id={"gx": ix + d[0], "gy": iy + d[1]}, device_id_type=MESH,
        )

    XS, YS, CS = (0, 1), (2, 3), (4, 5, 6, 7)

    def pack(step, n, which):
        lev, u = levs[n], U[n][step]
        for k in which:
            d = DIRS[k]
            if k >= 4:
                for at, (c, a, b, h) in enumerate(corner_pieces(lev, n == 1)):
                    r = lev.row(c, 2 + inner(lev.X, d[0], a), h, 8 + inner(lev.Y, d[1], b))
                    scorner[n][step, k - 4, pl.ds(at, 1), :] = u[pl.ds(r, 1), :]
                continue
            at = 0
            axis = 0 if d[0] else 1

            def put(value, k=k):
                nonlocal at
                size = value.shape[0]
                if step == 0:
                    sside0[n][k, pl.ds(at, size), :] = value
                else:
                    sside[n][step - 1, k, pl.ds(at, size), :] = value
                at += size

            for c, ring, h in side_pieces(lev, axis, n == 1):
                put(u[rows_of(*line(lev, d, ring, h, c, inner)), :])
            if step == 0:
                for f in (rig[n], met[n]):
                    for h in range(lev.H):
                        if d[0]:
                            put(f[inner(lev.X, d[0], 1), :, pl.ds(h * L, L)])
                        else:
                            put(f[:, inner(lev.Y, d[1], 1), pl.ds(h * L, L)])

    def start(step, n, which):
        for k in which:
            @pl.when(has(DIRS[k]))
            def _(k=k):
                copy(k, DIRS[k], step, n).start()

    def unpack(step, n):
        lev, u = levs[n], U[n][step]
        for k, d in enumerate(DIRS):
            back = (-d[0], -d[1])

            @pl.when(has(back))
            def _(k=k, d=d):
                copy(k, d, step, n).wait_recv()
                if k >= 4:
                    for at, (c, a, b, h) in enumerate(corner_pieces(lev, n == 1)):
                        r = lev.row(c, 2 + outer(lev.X, d[0], a), h, 8 + outer(lev.Y, d[1], b))
                        u[pl.ds(r, 1), :] = rcorner[n][step, k - 4, pl.ds(at, 1), :]
                    return
                axis = 0 if d[0] else 1
                size = lev.Y if d[0] else lev.X
                at = 0

                def get():
                    nonlocal at
                    at += size
                    if step == 0:
                        return rside0[n][k, pl.ds(at - size, size), :]
                    return rside[n][step - 1, k, pl.ds(at - size, size), :]

                for c, ring, h in side_pieces(lev, axis, n == 1):
                    u[rows_of(*line(lev, d, ring, h, c, outer)), :] = get()
                if step == 0:
                    got = [[get() for h in range(lev.H)] for f in range(2)]
                    for h in range(lev.H):
                        r_, m_ = got[0][h], got[1][h]
                        at_row, count, stride = line(lev, d, 1, h, 0, outer)
                        fr = lev.field_rows()
                        M[n][rows_of(WIDE * fr + at_row, count, stride), :] = r_ * m_
                        M[n][rows_of(IC * fr + at_row, count, stride), :] = (1.0 / m_) * coef(lev, h, size)

    def coef(lev, h, rows):
        ln = lax.broadcasted_iota(jnp.int32, (rows, L), 1)
        value = jnp.full((rows, L), 0.5, jnp.float32)
        if h == 0:
            value = jnp.where(ln == 0, 1.0, value)
        if h == lev.H - 1:
            value = jnp.where(ln == L - 1, 1.0, value)
        return value

    def shifts(vals):
        n = len(vals)
        ups = [pltpu.roll(v, L - 1, 1) for v in vals]
        dns = [pltpu.roll(v, 1, 1) for v in vals]
        lane_v = lane if vals[0].shape[0] == 8 else lax.broadcasted_iota(jnp.int32, vals[0].shape, 1)
        fst, lst = lane_v == 0, lane_v == L - 1
        hi = [jnp.where(lst, ups[i + 1] if i + 1 < n else vals[i], ups[i]) for i in range(n)]
        lo = [jnp.where(fst, dns[i - 1] if i > 0 else vals[i], dns[i]) for i in range(n)]
        return hi, lo

    for n in (1, 0):
        pack(0, n, XS + CS + YS)
    X, Y = lf.X, lf.Y
    sub = lax.broadcasted_iota(jnp.int32, (8, Y), 0)
    lan = lax.broadcasted_iota(jnp.int32, (8, Y), 1)
    even_y = (lax.broadcasted_iota(jnp.int32, (8, L), 0) % 2) == 0
    near_y = jnp.where(even_y, 0.75, 0.25)
    wrow = lambda x, b, s: ((x * lf.NB + b) * 8 + s) * 8
    for x in range(X):
        near_x = 0.75 if x % 2 == 0 else 0.25
        for b in range(lf.NB):
            for axis, near in ((0, near_x), (1, near_y)):
                o_row = jnp.broadcast_to(offs[axis, pl.ds(x, 1), :].astype(jnp.float32), (8, Y))
                o_col = jnp.sum(jnp.where(lan == sub + 8 * b, o_row, 0.0), axis=1, keepdims=True)
                o_all = jnp.broadcast_to(o_col, (8, L))
                for s in range(4):
                    w = jnp.where(o_all == float(s - 1), near, 0.0) + jnp.where(
                        o_all == float(s - 2), 1.0 - near, 0.0
                    )
                    wts[pl.ds(wrow(x, b, axis * 4 + s), 8), :] = w

    pl.semaphore_wait(barrier, greeted)
    for n in (1, 0):
        start(0, n, XS + CS + YS)

    for n, lev in enumerate(levs):
        m = M[n]

        @pl.loop(0, lev.X, unroll=4)
        def _(x, n=n, lev=lev, m=m):
            for b in range(lev.NB):
                def at(name, h):
                    return pl.ds(mrow(lev, name, x + 2, h, 8 + 8 * b), 8)

                vs = []
                for h in range(lev.H):
                    src = (x, pl.ds(8 * b, 8), pl.ds(h * L, L))
                    g, de, la, ri = met[n][src], den[n][src], lam[n][src], rig[n][src]
                    inv, rden = 1.0 / g, 1.0 / de
                    ic = inv * coef(lev, h, 8)
                    bb = (FACTOR * (la + ri)) * rden
                    m[at(IC, h), :] = ic
                    m[at(WIDE, h), :] = ri * g
                    m[at(A, h), :] = FACTOR * inv * rden
                    m[at(B5, h), :] = 0.5 * bb
                    m[at(BZ, h), :] = bb * ic
                    m[at(EN, h), :] = de * g
                    vs.append(ri * inv)
                hi, lo = shifts(vs)
                for h in range(lev.H):
                    m[at(FZP, h), :] = 0.5 * (vs[h] + hi[h])
                    m[at(FZM, h), :] = 0.5 * (vs[h] + lo[h])

    def faces(n):
        for lev, m in ((levs[n], M[n]),):
            @pl.loop(0, lev.X + 1, unroll=True)
            def _(x, lev=lev, m=m):
                for h in range(lev.H):
                    for b in range(lev.NB):
                        r = 8 + 8 * b
                        w0 = m[pl.ds(mrow(lev, WIDE, x + 1, h, r), 8), :]
                        w1 = m[pl.ds(mrow(lev, WIDE, x + 2, h, r), 8), :]
                        m[pl.ds(mrow(lev, FX, x + 1, h, r), 8), :] = 0.5 * (w0 + w1)
                    for b in range(lev.NB + 1):
                        r = 8 + 8 * b
                        w0 = m[pl.ds(mrow(lev, WIDE, x + 1, h, r - 1), 8), :]
                        w1 = m[pl.ds(mrow(lev, WIDE, x + 1, h, r), 8), :]
                        m[pl.ds(mrow(lev, FY, x + 1, h, r), 8), :] = 0.5 * (w0 + w1)

    def divergences(step, n, edge):
        for lev in (levs[n],):
            u, m = U[n][step], M[n]
            SX = lev.H * lev.R

            def block(start, count, stride, flag, lev=lev, u=u, m=m, SX=SX):
                cs = lev.field_rows()
                get = lambda c, h, off: u[rows_of(start + c * cs + h * lev.R + off, count, stride), :]
                hi, lo = shifts([get(2, h, 0) for h in range(lev.H)])
                for h in range(lev.H):
                    v = 0.5 * ((get(0, h, SX) - get(0, h, -SX)) + (get(1, h, 1) - get(1, h, -1)))
                    ic = m[rows_of(IC * cs + start + h * lev.R, count, stride), :]
                    v = v + ic * (hi[h] - lo[h])
                    m[rows_of(DIV * cs + start + h * lev.R, count, stride), :] = v

            if not edge:
                @pl.loop(3, lev.X - 3, unroll=True)
                def _(x, lev=lev, block=block):
                    for b in range(lev.NB):
                        block(lev.row(0, x + 2, 0, 8 + 8 * b), 8, 1, None)
                continue
            for x in (0, 1, 2, lev.X - 3, lev.X - 2, lev.X - 1):
                for b in range(lev.NB):
                    block(lev.row(0, x + 2, 0, 8 + 8 * b), 8, 1, None)

            for d in SIDES:
                @pl.when(has(d))
                def _(d=d, lev=lev, block=block, SX=SX):
                    if d[0]:
                        x = 1 if d[0] < 0 else lev.X + 2
                        for b in range(lev.NB):
                            block(lev.row(0, x, 0, 8 + 8 * b), 8, 1, None)
                    else:
                        r = 7 if d[1] < 0 else lev.Y + 8
                        for q in range(lev.X // 8):
                            block(lev.row(0, 2 + 8 * q, 0, r), 8, SX, None)

    RR = 2 * lc.Y + 16

    def ghosts(step):
        uc, uf = U[1][step], U[0][step]

        @pl.loop(0, lc.XE, unroll=4)
        def _(x):
            for c in range(3):
                base = (c * lc.XE + x) * RR
                for q in range(0, lc.Y + 8, 8):
                    p = pltpu.roll(uc[pl.ds(lc.row(c, x, 0, 6 + q), 8), :], L - 1, 1)
                    rep[pl.ds(base + 2 * q, 8, 2), :] = p
                    rep[pl.ds(base + 2 * q + 1, 8, 2), :] = p

        @pl.loop(0, lc.X, unroll=2)
        def _(xc):
            for b in range(lf.NB):
                for c in range(3):
                    plane = [[rep[pl.ds((c * lc.XE + xc + 1 + sx) * RR + 8 * b + 2 + 2 * sy, 8), :]
                              for sy in range(4)] for sx in range(4)]
                    for half in range(2):
                        x = 2 * xc + half
                        w = [wts[pl.ds(wrow(x, b, s), 8), :] for s in range(8)]
                        total = None
                        for sx in range(4):
                            part = w[4] * plane[sx][0]
                            for sy in range(1, 4):
                                part = part + w[4 + sy] * plane[sx][sy]
                            part = w[sx] * part
                            total = part if total is None else total + part
                        ghost[pl.ds(((c * lf.X + x) * lf.NB + b) * 8, 8), :] = total

    def top_ghost(step, x, c):
        uf = U[0][step]
        base = c * lf.Y
        for b in range(lf.NB):
            pair[pl.ds(base + 8 * b, 8), :] = (
                uf[pl.ds(lf.row(c, 2 * x + 2, 0, 8 + 8 * b), 8), :]
                + uf[pl.ds(lf.row(c, 2 * x + 3, 0, 8 + 8 * b), 8), :]
            )
        s = pair[pl.ds(base, 8, 2), :] + pair[pl.ds(base + 1, 8, 2), :]
        return pltpu.roll(0.25 * s, 1, 1)

    def update(step, n, edge):
        lev = levs[n]
        u, m = U[n][step], M[n]
        SX = lev.H * lev.R
        H = lev.H

        def body(x, acc):
            for b in range(lev.NB):
                r0 = 8 + 8 * b

                def mat(name, h, off=0):
                    return m[pl.ds(mrow(lev, name, x + 2, h, r0) + off, 8), :]

                dv = [mat(DIV, h) for h in range(H)]
                dhi, dlo = shifts(dv)
                cells = [None] * H
                for c in range(3):
                    get = lambda h, off=0, c=c: u[pl.ds(lev.row(c, x + 2, h, r0) + off, 8), :]
                    cur = [get(h) for h in range(H)]
                    hi, lo = shifts(cur)
                    if n == 0:
                        g = ghost[pl.ds(((c * lev.X + x) * lev.NB + b) * 8, 8), :]
                        hi[H - 1] = jnp.where(last, g, hi[H - 1])
                    else:
                        hi[H - 1] = jnp.where(last, 0.0, hi[H - 1])
                        lo[0] = jnp.where(first, top_ghost(step, x, c), lo[0])
                    for h in range(H):
                        v = cur[h]
                        flux = mat(FX, h) * (get(h, SX) - v) - mat(FX, h, -SX) * (v - get(h, -SX))
                        flux = flux + (mat(FY, h, 1) * (get(h, 1) - v) - mat(FY, h) * (v - get(h, -1)))
                        flux = flux + (mat(FZP, h) * (hi[h] - v) - mat(FZM, h) * (v - lo[h]))
                        if c == 0:
                            grad = mat(B5, h) * (mat(DIV, h, SX) - mat(DIV, h, -SX))
                        elif c == 1:
                            grad = mat(B5, h) * (mat(DIV, h, 1) - mat(DIV, h, -1))
                        else:
                            grad = mat(BZ, h) * (dhi[h] - dlo[h])
                        rate = mat(A, h) * flux + grad
                        if step == 0:
                            p = prev[n][c, x, pl.ds(8 * b, 8), pl.ds(h * L, L)]
                        else:
                            p = U[n][step - 1][pl.ds(lev.row(c, x + 2, h, r0), 8), :]
                        change = (v - p) + rate
                        new = v + change
                        if step == STEPS - 1:
                            out[n][c, x, pl.ds(8 * b, 8), pl.ds(h * L, L)] = new
                        else:
                            U[n][step + 1][pl.ds(lev.row(c, x + 2, h, r0), 8), :] = new
                        e = change * change - new * rate
                        cells[h] = e if cells[h] is None else cells[h] + e
                for h in range(H):
                    acc = acc + mat(EN, h) * cells[h]
            return acc

        acc = jnp.zeros((8, L), jnp.float32)
        if edge:
            for x in (0, 1, lev.X - 2, lev.X - 1):
                acc = body(x, acc)
        else:
            acc = lax.fori_loop(2, lev.X - 2, body, acc, unroll=4)
        row = pl.ds(4 * n + step, 1)
        es[row, :] = es[row, :] + jnp.sum(acc, axis=0, keepdims=True)

    es[...] = jnp.zeros((8, L), jnp.float32)
    for step in range(STEPS):
        for n in (1, 0):
            unpack(step, n)
            if step == 0:
                faces(n)
            divergences(step, n, True)
            if n == 0:
                ghosts(step)
            update(step, n, True)
            if step < STEPS - 1:
                pack(step + 1, n, XS + CS)
                start(step + 1, n, XS + CS)
        for n in (1, 0):
            divergences(step, n, False)
            update(step, n, False)
            if step < STEPS - 1:
                pack(step + 1, n, YS)
                start(step + 1, n, YS)
        if step < len(rings):
            if step:
                ready_wait(step - 1)
            ready_signal(step)
    for i in range(min(STEPS, len(rings)) - 1, len(rings)):
        ready_wait(i)
        if i + 1 < len(rings):
            ready_signal(i + 1)

    def share(o, arriving=False):
        to, x, y = place(o)
        source = to if arriving else me
        return pltpu.make_async_remote_copy(
            src_ref=mine, dst_ref=box.at[pl.ds(source, 1)], send_sem=en_send.at[o],
            recv_sem=en_recv.at[source], device_id={"gx": x, "gy": y}, device_id_type=MESH,
        )

    sums = jnp.sum(es[...], axis=1, keepdims=True)
    diagonal = lane == lax.broadcasted_iota(jnp.int32, (8, L), 0)
    row = jnp.sum(jnp.where(diagonal, sums, 0.0), axis=0, keepdims=True)
    mine[...] = row

    @pl.loop(1, everyone)
    def _(o):
        share(o).start()

    box[pl.ds(me, 1), :] = row

    @pl.loop(1, everyone)
    def _(o):
        share(o, True).wait_recv()

    total = jnp.sum(box[...], axis=0, keepdims=True)
    for n, lev in enumerate(levs):
        cells = lev.X * n_x * lev.Y * n_y * lev.H * L
        eo[pl.ds(n, 1), :] = total[:, 4 * n : 4 * n + STEPS] / cells

    @pl.loop(1, everyone)
    def _(o):
        share(o).wait_send()

    for step in range(STEPS):
        for k, d in enumerate(DIRS):
            @pl.when(has(d))
            def _(k=k, d=d, step=step):
                for n in range(2):
                    copy(k, d, step, n).wait_send()


def ready_rings(n_x, n_y):
    rings, reach = [], 2
    while reach < max(n_x, n_y) - 1:
        xs = (-reach, 0, reach) if reach < n_x - 1 else (0,)
        ys = (-reach, 0, reach) if reach < n_y - 1 else (0,)
        rings.append([(x, y) for x in xs for y in ys if x or y])
        reach *= 2
    return rings


def write_out(a, b, c, fine, coarse, energy, sem):
    copies = [
        pltpu.make_async_copy(src, dst, sem.at[i])
        for i, (src, dst) in enumerate(((a, fine), (b, coarse), (c, energy)))
    ]
    for copy in copies:
        copy.start()
    for copy in copies:
        copy.wait()


def side_rows(lev, coarse):
    longer = max(lev.X, lev.Y)
    size = longer * len(side_pieces(lev, 0, coarse))
    return size, size + 2 * lev.H * longer


def solution(mesh):
    n_x, n_y = mesh.shape["gx"], mesh.shape["gy"]

    def step(*args):
        lf, lc = Level(args[0].shape), Level(args[2].shape)
        sizes = [side_rows(lf, False), side_rows(lc, True)]
        corners = [len(corner_pieces(lf, False)), len(corner_pieces(lc, True))]
        f32 = jnp.float32
        vm = lambda *s: pltpu.VMEM(s, f32)
        results = pl.pallas_call(
            functools.partial(kernel, n_x, n_y, lf, lc),
            out_shape=(
                vm(*args[0].shape),
                vm(*args[2].shape),
                vm(2, STEPS),
            ),
            in_specs=[pl.BlockSpec(memory_space=pltpu.VMEM)] * len(args),
            out_specs=[pl.BlockSpec(memory_space=pltpu.VMEM)] * 3,
            scratch_shapes=(
                [vm(3 * lf.field_rows(), L)] * 3
                + [vm(3 * lc.field_rows(), L)] * 3
                + [
                    vm(11 * lf.field_rows(), L),
                    vm(11 * lc.field_rows(), L),
                    vm(3 * lc.XE * (2 * lc.Y + 16), L),
                    vm(3 * lf.Y, L),
                    vm(lf.X * lf.NB * 64, L),
                    vm(3 * lf.X * lf.Y, L),
                ]
                + [vm(4, size[1], L) for size in sizes] * 2
                + [vm(STEPS - 1, 4, size[0], L) for size in sizes] * 2
                + [vm(STEPS, 4, corner, L) for corner in corners] * 2
                + [
                    vm(8, L),
                    vm(1, L),
                    vm(n_x * n_y, L),
                    pltpu.SemaphoreType.DMA((2, STEPS, 8)),
                    pltpu.SemaphoreType.DMA((2, STEPS, 8)),
                    pltpu.SemaphoreType.DMA((n_x * n_y,)),
                    pltpu.SemaphoreType.DMA((n_x * n_y,)),
                    pltpu.SemaphoreType.REGULAR((max(1, len(ready_rings(n_x, n_y))),)),
                ]
            ),
            compiler_params=pltpu.CompilerParams(
                collective_id=0, has_side_effects=True, vmem_limit_bytes=60 * 1024 * 1024
            ),
        )(*args)
        results = [pltpu.with_memory_space_constraint(r, pltpu.VMEM) for r in results]
        fine, coarse, energy = pl.pallas_call(
            write_out,
            out_shape=tuple(jax.ShapeDtypeStruct(r.shape, f32) for r in results),
            in_specs=[pl.BlockSpec(memory_space=pltpu.VMEM)] * 3,
            out_specs=[pl.BlockSpec(memory_space=pl.ANY)] * 3,
            scratch_shapes=[pltpu.SemaphoreType.DMA((3,))],
        )(*results)
        return fine, coarse, energy.T

    field, cells = P(None, "gx", "gy", None), P("gx", "gy", None)
    return jax.shard_map(
        step,
        mesh=mesh,
        in_specs=(field,) * 4 + (cells,) * 8 + (P(None, "gx", "gy"),),
        out_specs=(field, field, P()),
        check_vma=False,
    )
```

```python
import functools

import jax
import jax.numpy as jnp
from jax import lax
from jax.experimental import pallas as pl
from jax.experimental.pallas import tpu as pltpu
from jax.sharding import PartitionSpec as P

STEPS = 3
FACTOR = 0.15
MESH = pl.DeviceIdType.MESH
L = 128
SIDES = ((1, 0), (-1, 0), (0, 1), (0, -1))
CORNERS = ((1, 1), (1, -1), (-1, 1), (-1, -1))


class Level:
    def __init__(self, shape):
        _, self.X, self.Y, Z = shape
        self.H = Z // L
        self.XE = self.X + 4
        self.R = self.Y + 16
        while (self.H * self.R) % 8 != 4:
            self.R += 1
        self.NB = self.Y // 8

    def row(self, c, x, h, r):
        return ((c * self.XE + x) * self.H + h) * self.R + r

    def field_rows(self):
        return self.XE * self.H * self.R


def side_pieces(lev, d, coarse, step):
    out = [("u", c, h) for c in range(3) for h in range(lev.H)]
    out += [("div", 0, h) for h in range(lev.H)]
    if step == 0:
        out += [("wide", 0, h) for h in range(lev.H)]
    if coarse and d[0] + d[1] < 0:
        out += [("plane", 0, 0)]
    return out


def corner_extras(d):
    rings = [(a, b) for a in ((1, 2) if d[0] < 0 else (1,)) for b in ((1, 2) if d[1] < 0 else (1,))]
    return [(2, 1, 1)] + [(c, a, b) for a, b in rings if (a, b) != (1, 1) for c in range(3)]


def corner_rows(lev, coarse):
    return 2 * lev.H + int(coarse)


def inner(length, d, ring):
    return length - ring if d > 0 else ring - 1


def outer(length, d, ring):
    return -ring if d > 0 else length + ring - 1


def line(lev, d, ring, h, c, place):
    if d[0]:
        return lev.row(c, 2 + place(lev.X, d[0], ring), h, 8), lev.Y, 1
    return lev.row(c, 2, h, 8 + place(lev.Y, d[1], ring)), lev.X, lev.H * lev.R


def rows_of(start, count, stride):
    return pl.ds(start, count) if stride == 1 else pl.ds(start, count, stride)


def kernel(n_x, n_y, lf, lc, *refs):
    given, (fo, co, eo) = refs[:13], refs[13:16]
    held = refs[16:29]
    (fd, fp, cd, cp, fden, flam, frig, fmet, cden, clam, crig, cmet, offs) = held
    (uf0, uf1, uf2, uc0, uc1, uc2, mf, mc, rep, pair, wts, ghost,
     ss0f, ss0c, rs0f, rs0c, ssf, ssc, rsf, rsc, scf, scc, rcf, rcc,
     es, mine, box, load_sem, send_sem, recv_sem, en_send, en_recv, inside) = refs[29:]
    U = ((uf0, uf1, uf2), (uc0, uc1, uc2))
    M = (mf, mc)
    levs = (lf, lc)
    sside0, rside0, sside, rside = (ss0f, ss0c), (rs0f, rs0c), (ssf, ssc), (rsf, rsc)
    scorner, rcorner = (scf, scc), (rcf, rcc)
    disp, prev, out = (fd, cd), (fp, cp), (fo, co)
    den, lam, rig, met = (fden, cden), (flam, clam), (frig, crig), (fmet, cmet)
    ix, iy = lax.axis_index("gx"), lax.axis_index("gy")

    def has(d):
        conds = []
        if d[0] > 0:
            conds.append(ix < n_x - 1)
        if d[0] < 0:
            conds.append(ix > 0)
        if d[1] > 0:
            conds.append(iy < n_y - 1)
        if d[1] < 0:
            conds.append(iy > 0)
        return functools.reduce(jnp.logical_and, conds)

    DIRS = SIDES + CORNERS
    lane = lax.broadcasted_iota(jnp.int32, (8, L), 1)
    first, last = lane == 0, lane == L - 1

    IC, WIDE, FX, FY, FZP, FZM, A, B5, BZ, EN, DIV = range(11)

    def mrow(lev, name, x, h, r):
        return name * lev.field_rows() + (x * lev.H + h) * lev.R + r

    barrier = pltpu.get_barrier_semaphore()

    def signal(x, y):
        pl.semaphore_signal(barrier, inc=1, device_id={"gx": x, "gy": y}, device_id_type=MESH)

    everyone = n_x * n_y
    me = ix * n_y + iy

    def place(o):
        to = lax.rem(me + o, everyone)
        return to, lax.div(to, n_y), lax.rem(to, n_y)

    greeted = jnp.int32(0)
    for d in DIRS:
        greeted = greeted + has(d).astype(jnp.int32)

        @pl.when(has(d))
        def _(d=d):
            signal(ix + d[0], iy + d[1])

    rings = ready_rings(n_x, n_y)

    def within(d):
        x, y = ix + d[0], iy + d[1]
        return (x >= 0) & (x < n_x) & (y >= 0) & (y < n_y)

    def ready_signal(i):
        for d in rings[i]:
            @pl.when(within(d))
            def _(d=d):
                pl.semaphore_signal(
                    inside.at[i], inc=1, device_id={"gx": ix + d[0], "gy": iy + d[1]}, device_id_type=MESH
                )

    def ready_wait(i):
        pl.semaphore_wait(inside.at[i], sum(within(d).astype(jnp.int32) for d in rings[i]))

    def coef(lev, h, rows):
        ln = lax.broadcasted_iota(jnp.int32, (rows, L), 1)
        value = jnp.full((rows, L), 0.5, jnp.float32)
        if h == 0:
            value = jnp.where(ln == 0, 1.0, value)
        if h == lev.H - 1:
            value = jnp.where(ln == L - 1, 1.0, value)
        return value

    def shifts(vals):
        n = len(vals)
        ups = [pltpu.roll(v, L - 1, 1) for v in vals]
        dns = [pltpu.roll(v, 1, 1) for v in vals]
        lane_v = lane if vals[0].shape[0] == 8 else lax.broadcasted_iota(jnp.int32, vals[0].shape, 1)
        fst, lst = lane_v == 0, lane_v == L - 1
        hi = [jnp.where(lst, ups[i + 1] if i + 1 < n else vals[i], ups[i]) for i in range(n)]
        lo = [jnp.where(fst, dns[i - 1] if i > 0 else vals[i], dns[i]) for i in range(n)]
        return hi, lo

    def load(i):
        return pltpu.make_async_copy(given[i], held[i], load_sem.at[i])

    FIRST = (2, 0, 11, 10, 7, 6)
    LATER = tuple(i for i in range(13) if i not in FIRST)
    for i in FIRST + LATER:
        load(i).start()

    zero = jnp.zeros((8, L), jnp.float32)
    for lev, us, m in zip(levs, U, M):
        lines = lev.XE * lev.H

        @pl.loop(0, 3 * lines, unroll=4)
        def _(q, lev=lev, us=us):
            for u in us:
                u[pl.ds(q * lev.R, 8), :] = zero
                u[pl.ds(q * lev.R + lev.Y + 8, 8), :] = zero

        @pl.loop(0, lines, unroll=4)
        def _(q, lev=lev, m=m):
            for name in (WIDE, DIV):
                m[pl.ds(name * lev.field_rows() + q * lev.R, 8), :] = zero
                m[pl.ds(name * lev.field_rows() + q * lev.R + lev.Y + 8, 8), :] = zero

        for x in (0, 1, lev.X + 2, lev.X + 3):
            for h in range(lev.H):
                for b in range(lev.NB):
                    for u in us:
                        for c in range(3):
                            u[pl.ds(lev.row(c, x, h, 8 + 8 * b), 8), :] = zero
                    for name in (WIDE, DIV):
                        m[pl.ds(mrow(lev, name, x, h, 8 + 8 * b), 8), :] = zero

    for i in FIRST:
        load(i).wait()

    for n in (1, 0):
        lev, us, u_in, m = levs[n], U[n], disp[n], M[n]

        @pl.loop(0, lev.X, unroll=4)
        def _(x, n=n, lev=lev, us=us, u_in=u_in, m=m):
            for h in range(lev.H):
                for b in range(lev.NB):
                    src = (x, pl.ds(8 * b, 8), pl.ds(h * L, L))
                    g = met[n][src]
                    m[pl.ds(mrow(lev, IC, x + 2, h, 8 + 8 * b), 8), :] = (1.0 / g) * coef(lev, h, 8)
                    m[pl.ds(mrow(lev, WIDE, x + 2, h, 8 + 8 * b), 8), :] = rig[n][src] * g
                    for c in range(3):
                        us[0][pl.ds(lev.row(c, x + 2, h, 8 + 8 * b), 8), :] = u_in[(c,) + src]

    def side_size(n, d):
        return levs[n].Y if d[0] else levs[n].X

    def copy(k, d, step, n):
        if k >= 4:
            s, r = scorner[n].at[step, k - 4], rcorner[n].at[step, k - 4]
        else:
            rows = pl.ds(0, side_size(n, d) * len(side_pieces(levs[n], d, n == 1, step)))
            if step == 0:
                s, r = sside0[n].at[k, rows], rside0[n].at[k, rows]
            else:
                s, r = sside[n].at[step - 1, k, rows], rside[n].at[step - 1, k, rows]
        return pltpu.make_async_remote_copy(
            src_ref=s, dst_ref=r, send_sem=send_sem.at[n, step, k],
            recv_sem=recv_sem.at[n, step, k],
            device_id={"gx": ix + d[0], "gy": iy + d[1]}, device_id_type=MESH,
        )

    XS, YS, CS = (0, 1), (2, 3), (4, 5, 6, 7)

    def divergence(step, n, start, count, stride):
        lev, u, m = levs[n], U[n][step], M[n]
        SX, cs = lev.H * lev.R, lev.field_rows()
        get = lambda c, h, off: u[rows_of(start + c * cs + h * lev.R + off, count, stride), :]
        hi, lo = shifts([get(2, h, 0) for h in range(lev.H)])
        values = []
        for h in range(lev.H):
            v = 0.5 * ((get(0, h, SX) - get(0, h, -SX)) + (get(1, h, 1) - get(1, h, -1)))
            ic = m[rows_of(IC * cs + start + h * lev.R, count, stride), :]
            values.append(v + ic * (hi[h] - lo[h]))
        return values

    def lanes_of(rows):
        return lax.broadcasted_iota(jnp.int32, (rows, L), 1)

    def merged(values):
        total, ln = values[0], lanes_of(values[0].shape[0])
        for i, v in enumerate(values[1:], 1):
            total = jnp.where(ln == i, pltpu.roll(v, i, 1), total)
        return total

    def parted(value, i):
        return pltpu.roll(value, L - i, 1) if i else value

    def corner_row(lev, d, c, a, b, h, place):
        return pl.ds(lev.row(c, 2 + place(lev.X, d[0], a), h, 8 + place(lev.Y, d[1], b)), 1)

    def pack(step, n, which):
        lev, u, m = levs[n], U[n][step], M[n]
        for k in which:
            d = DIRS[k]
            if k >= 4:
                for c in range(2):
                    for h in range(lev.H):
                        scorner[n][step, k - 4, pl.ds(c * lev.H + h, 1), :] = u[
                            corner_row(lev, d, c, 1, 1, h, inner), :
                        ]
                if n:
                    extras = [u[corner_row(lev, d, c, a, b, 0, inner), :] for c, a, b in corner_extras(d)]
                    scorner[n][step, k - 4, pl.ds(2 * lev.H, 1), :] = merged(extras)
                continue
            size = side_size(n, d)
            parts = divergence(step, n, *line(lev, d, 1, 0, 0, inner))
            for at, (kind, c, h) in enumerate(side_pieces(lev, d, n == 1, step)):
                first_row, count, stride = line(lev, d, 1, h, c, inner)
                if kind == "u":
                    value = u[rows_of(first_row, count, stride), :]
                elif kind == "div":
                    value = parts[h]
                elif kind == "wide":
                    value = m[rows_of(WIDE * lev.field_rows() + first_row, count, stride), :]
                else:
                    value = merged([u[rows_of(*line(lev, d, 2, 0, e, inner)), :] for e in range(3)])
                if step == 0:
                    sside0[n][k, pl.ds(at * size, size), :] = value
                else:
                    sside[n][step - 1, k, pl.ds(at * size, size), :] = value

    def start(step, n, which):
        for k in which:
            @pl.when(has(DIRS[k]))
            def _(k=k):
                copy(k, DIRS[k], step, n).start()

    def unpack(step, n, which):
        lev, u, m = levs[n], U[n][step], M[n]
        fr = lev.field_rows()
        for k in which:
            d = DIRS[k]
            back = (-d[0], -d[1])

            @pl.when(has(back))
            def _(k=k, d=d, back=back):
                copy(k, d, step, n).wait_recv()
                if k >= 4:
                    for c in range(2):
                        for h in range(lev.H):
                            value = rcorner[n][step, k - 4, pl.ds(c * lev.H + h, 1), :]
                            u[corner_row(lev, d, c, 1, 1, h, outer), :] = value
                            if c == 0:
                                beside = lev.row(0, 2 + inner(lev.X, back[0], 1), h, 8 + outer(lev.Y, d[1], 1))
                                sign = back[0]
                            else:
                                beside = lev.row(0, 2 + outer(lev.X, d[0], 1), h, 8 + inner(lev.Y, back[1], 1))
                                sign = back[1]
                            at = pl.ds(DIV * fr + beside, 1)
                            m[at, :] = m[at, :] + (0.5 * sign) * value
                    if n:
                        value = rcorner[n][step, k - 4, pl.ds(2 * lev.H, 1), :]
                        for i, (c, a, b) in enumerate(corner_extras(d)):
                            u[corner_row(lev, d, c, a, b, 0, outer), :] = parted(value, i)
                    return
                axis, size = (0 if d[0] else 1), side_size(n, d)
                for at, (kind, c, h) in enumerate(side_pieces(lev, d, n == 1, step)):
                    rows = pl.ds(at * size, size)
                    got = rside0[n][k, rows, :] if step == 0 else rside[n][step - 1, k, rows, :]
                    first_row, count, stride = line(lev, d, 1, h, c, outer)
                    if kind == "u":
                        u[rows_of(first_row, count, stride), :] = got
                    elif kind == "div":
                        own = u[rows_of(*line(lev, back, 1, h, axis, inner)), :]
                        m[rows_of(DIV * fr + first_row, count, stride), :] = got + (0.5 * (d[0] + d[1])) * own
                    elif kind == "wide":
                        m[rows_of(WIDE * fr + first_row, count, stride), :] = got
                    else:
                        for e in range(3):
                            u[rows_of(*line(lev, d, 2, 0, e, outer)), :] = parted(got, e)

    for n in (1, 0):
        pack(0, n, XS + CS + YS)
    pl.semaphore_wait(barrier, greeted)
    for n in (1, 0):
        start(0, n, YS + CS + XS)
    for i in LATER:
        load(i).wait()

    X, Y = lf.X, lf.Y
    sub = lax.broadcasted_iota(jnp.int32, (8, Y), 0)
    lan = lax.broadcasted_iota(jnp.int32, (8, Y), 1)
    even_y = (lax.broadcasted_iota(jnp.int32, (8, L), 0) % 2) == 0
    near_y = jnp.where(even_y, 0.75, 0.25)
    wrow = lambda x, b, s: ((x * lf.NB + b) * 8 + s) * 8
    for x in range(X):
        near_x = 0.75 if x % 2 == 0 else 0.25
        for b in range(lf.NB):
            for axis, near in ((0, near_x), (1, near_y)):
                o_row = jnp.broadcast_to(offs[axis, pl.ds(x, 1), :].astype(jnp.float32), (8, Y))
                o_col = jnp.sum(jnp.where(lan == sub + 8 * b, o_row, 0.0), axis=1, keepdims=True)
                o_all = jnp.broadcast_to(o_col, (8, L))
                for s in range(4):
                    w = jnp.where(o_all == float(s - 1), near, 0.0) + jnp.where(
                        o_all == float(s - 2), 1.0 - near, 0.0
                    )
                    wts[pl.ds(wrow(x, b, axis * 4 + s), 8), :] = w

    for n, lev in enumerate(levs):
        m = M[n]

        @pl.loop(0, lev.X, unroll=4)
        def _(x, n=n, lev=lev, m=m):
            for b in range(lev.NB):
                def at(name, h):
                    return pl.ds(mrow(lev, name, x + 2, h, 8 + 8 * b), 8)

                vs = []
                for h in range(lev.H):
                    src = (x, pl.ds(8 * b, 8), pl.ds(h * L, L))
                    g, de, la, ri = met[n][src], den[n][src], lam[n][src], rig[n][src]
                    rden = 1.0 / de
                    ic = m[at(IC, h), :]
                    inv = ic * (1.0 / coef(lev, h, 8))
                    bb = (FACTOR * (la + ri)) * rden
                    m[at(A, h), :] = FACTOR * inv * rden
                    m[at(B5, h), :] = 0.5 * bb
                    m[at(BZ, h), :] = bb * ic
                    m[at(EN, h), :] = de * g
                    vs.append(ri * inv)
                hi, lo = shifts(vs)
                for h in range(lev.H):
                    m[at(FZP, h), :] = 0.5 * (vs[h] + hi[h])
                    m[at(FZM, h), :] = 0.5 * (vs[h] + lo[h])

    def faces_x(n, xs):
        lev, m = levs[n], M[n]
        for x in xs:
            for h in range(lev.H):
                for b in range(lev.NB):
                    r = 8 + 8 * b
                    w0 = m[pl.ds(mrow(lev, WIDE, x + 1, h, r), 8), :]
                    w1 = m[pl.ds(mrow(lev, WIDE, x + 2, h, r), 8), :]
                    m[pl.ds(mrow(lev, FX, x + 1, h, r), 8), :] = 0.5 * (w0 + w1)

    def faces_y(n):
        lev, m = levs[n], M[n]

        @pl.loop(0, lev.X, unroll=4)
        def _(x):
            for h in range(lev.H):
                for b in range(lev.NB + 1):
                    r = 8 + 8 * b
                    w0 = m[pl.ds(mrow(lev, WIDE, x + 2, h, r - 1), 8), :]
                    w1 = m[pl.ds(mrow(lev, WIDE, x + 2, h, r), 8), :]
                    m[pl.ds(mrow(lev, FY, x + 2, h, r), 8), :] = 0.5 * (w0 + w1)

    def divergences(step, n, xs):
        lev, m = levs[n], M[n]

        def column(x):
            for b in range(lev.NB):
                values = divergence(step, n, lev.row(0, x + 2, 0, 8 + 8 * b), 8, 1)
                for h in range(lev.H):
                    m[pl.ds(mrow(lev, DIV, x + 2, h, 8 + 8 * b), 8), :] = values[h]

        for x in xs:
            column(x)

    RR = 2 * lc.Y + 16

    def ghosts(step):
        uc, uf = U[1][step], U[0][step]

        @pl.loop(0, lc.XE, unroll=4)
        def _(x):
            for c in range(3):
                base = (c * lc.XE + x) * RR
                for q in range(0, lc.Y + 8, 8):
                    p = pltpu.roll(uc[pl.ds(lc.row(c, x, 0, 6 + q), 8), :], L - 1, 1)
                    rep[pl.ds(base + 2 * q, 8, 2), :] = p
                    rep[pl.ds(base + 2 * q + 1, 8, 2), :] = p

        @pl.loop(0, lc.X, unroll=2)
        def _(xc):
            for b in range(lf.NB):
                for c in range(3):
                    plane = [[rep[pl.ds((c * lc.XE + xc + 1 + sx) * RR + 8 * b + 2 + 2 * sy, 8), :]
                              for sy in range(4)] for sx in range(4)]
                    for half in range(2):
                        x = 2 * xc + half
                        w = [wts[pl.ds(wrow(x, b, s), 8), :] for s in range(8)]
                        total = None
                        for sx in range(4):
                            part = w[4] * plane[sx][0]
                            for sy in range(1, 4):
                                part = part + w[4 + sy] * plane[sx][sy]
                            part = w[sx] * part
                            total = part if total is None else total + part
                        ghost[pl.ds(((c * lf.X + x) * lf.NB + b) * 8, 8), :] = total

    def top_ghost(step, x, c):
        uf = U[0][step]
        base = c * lf.Y
        for b in range(lf.NB):
            pair[pl.ds(base + 8 * b, 8), :] = (
                uf[pl.ds(lf.row(c, 2 * x + 2, 0, 8 + 8 * b), 8), :]
                + uf[pl.ds(lf.row(c, 2 * x + 3, 0, 8 + 8 * b), 8), :]
            )
        s = pair[pl.ds(base, 8, 2), :] + pair[pl.ds(base + 1, 8, 2), :]
        return pltpu.roll(0.25 * s, 1, 1)

    def update(step, n, columns, inside_x=None):
        lev = levs[n]
        u, m = U[n][step], M[n]
        SX = lev.H * lev.R
        H = lev.H

        def body(x, acc, comps=(0, 1, 2)):
            for b in range(lev.NB):
                r0 = 8 + 8 * b

                def mat(name, h, off=0):
                    return m[pl.ds(mrow(lev, name, x + 2, h, r0) + off, 8), :]

                dhi, dlo = shifts([mat(DIV, h) for h in range(H)]) if 2 in comps else (None, None)
                cells = [None] * H
                for c in comps:
                    get = lambda h, off=0, c=c: u[pl.ds(lev.row(c, x + 2, h, r0) + off, 8), :]
                    cur = [get(h) for h in range(H)]
                    hi, lo = shifts(cur)
                    if n == 0:
                        g = ghost[pl.ds(((c * lev.X + x) * lev.NB + b) * 8, 8), :]
                        hi[H - 1] = jnp.where(last, g, hi[H - 1])
                    else:
                        hi[H - 1] = jnp.where(last, 0.0, hi[H - 1])
                        lo[0] = jnp.where(first, top_ghost(step, x, c), lo[0])
                    for h in range(H):
                        v = cur[h]
                        flux = mat(FX, h) * (get(h, SX) - v) - mat(FX, h, -SX) * (v - get(h, -SX))
                        flux = flux + (mat(FY, h, 1) * (get(h, 1) - v) - mat(FY, h) * (v - get(h, -1)))
                        flux = flux + (mat(FZP, h) * (hi[h] - v) - mat(FZM, h) * (v - lo[h]))
                        if c == 0:
                            grad = mat(B5, h) * (mat(DIV, h, SX) - mat(DIV, h, -SX))
                        elif c == 1:
                            grad = mat(B5, h) * (mat(DIV, h, 1) - mat(DIV, h, -1))
                        else:
                            grad = mat(BZ, h) * (dhi[h] - dlo[h])
                        rate = mat(A, h) * flux + grad
                        if step == 0:
                            p = prev[n][c, x, pl.ds(8 * b, 8), pl.ds(h * L, L)]
                        else:
                            p = U[n][step - 1][pl.ds(lev.row(c, x + 2, h, r0), 8), :]
                        change = (v - p) + rate
                        new = v + change
                        if step == STEPS - 1:
                            out[n][c, x, pl.ds(8 * b, 8), pl.ds(h * L, L)] = new
                        else:
                            U[n][step + 1][pl.ds(lev.row(c, x + 2, h, r0), 8), :] = new
                        e = change * change - new * rate
                        cells[h] = e if cells[h] is None else cells[h] + e
                for h in range(H):
                    acc = acc + mat(EN, h) * cells[h]
            return acc

        acc = jnp.zeros((8, L), jnp.float32)
        for x, comps in columns:
            acc = body(x, acc, comps)
        if inside_x is not None:
            acc = lax.fori_loop(*inside_x, body, acc, unroll=4)
        row = pl.ds(4 * n + step, 1)
        es[row, :] = es[row, :] + jnp.sum(acc, axis=0, keepdims=True)

    es[...] = jnp.zeros((8, L), jnp.float32)
    ALL = (0, 1, 2)
    for n, lev in enumerate(levs):
        faces_x(n, range(1, lev.X))
    for step in range(STEPS):
        final = step == STEPS - 1
        for n in (1, 0):
            lev = levs[n]
            X = lev.X
            inner_first = n == 1 or final
            unpack(step, n, YS)
            if step == 0:
                faces_y(n)
            if inner_first:
                divergences(step, n, range(1, X - 1))
                update(step, n, (), (2, X - 2))
            unpack(step, n, XS + CS)
            if step == 0:
                faces_x(n, (0, X))
            divergences(step, n, (0, X - 1) if inner_first else (0, 1, 2, X - 3, X - 2, X - 1))
            if final:
                update(step, n, [(x, ALL) for x in (0, 1, X - 2, X - 1)])
            else:
                if n:
                    update(step, n, [(0, ALL), (1, ALL), (X - 1, ALL), (X - 2, (0,))])
                else:
                    update(step, n, [(0, ALL), (X - 1, ALL), (1, (0,)), (X - 2, (0,))])
                pack(step + 1, n, XS + CS)
                start(step + 1, n, CS + XS)
                rest = [(X - 2, (1, 2))] + ([] if n else [(1, (1, 2))])
                if inner_first:
                    update(step, n, rest)
                else:
                    divergences(step, n, range(3, X - 3))
                    update(step, n, rest, (2, X - 2))
                pack(step + 1, n, YS)
                start(step + 1, n, YS)
            if n:
                ghosts(step)
        if step < len(rings):
            if step:
                ready_wait(step - 1)
            ready_signal(step)
    for i in range(min(STEPS, len(rings)) - 1, len(rings)):
        ready_wait(i)
        if i + 1 < len(rings):
            ready_signal(i + 1)

    def share(o, arriving=False):
        to, x, y = place(o)
        source = to if arriving else me
        return pltpu.make_async_remote_copy(
            src_ref=mine, dst_ref=box.at[pl.ds(source, 1)], send_sem=en_send.at[o],
            recv_sem=en_recv.at[source], device_id={"gx": x, "gy": y}, device_id_type=MESH,
        )

    sums = jnp.sum(es[...], axis=1, keepdims=True)
    diagonal = lane == lax.broadcasted_iota(jnp.int32, (8, L), 0)
    row = jnp.sum(jnp.where(diagonal, sums, 0.0), axis=0, keepdims=True)
    mine[...] = row

    @pl.loop(1, everyone)
    def _(o):
        share(o).start()

    box[pl.ds(me, 1), :] = row

    @pl.loop(1, everyone)
    def _(o):
        share(o, True).wait_recv()

    total = jnp.sum(box[...], axis=0, keepdims=True)
    for n, lev in enumerate(levs):
        cells = lev.X * n_x * lev.Y * n_y * lev.H * L
        eo[pl.ds(n, 1), :] = total[:, 4 * n : 4 * n + STEPS] / cells

    @pl.loop(1, everyone)
    def _(o):
        share(o).wait_send()

    for step in range(STEPS):
        for k, d in enumerate(DIRS):
            @pl.when(has(d))
            def _(k=k, d=d, step=step):
                for n in range(2):
                    copy(k, d, step, n).wait_send()


def ready_rings(n_x, n_y):
    rings, reach = [], 2
    while reach < max(n_x, n_y) - 1:
        xs = (-reach, 0, reach) if reach < n_x - 1 else (0,)
        ys = (-reach, 0, reach) if reach < n_y - 1 else (0,)
        rings.append([(x, y) for x in xs for y in ys if x or y])
        reach *= 2
    return rings


def write_out(a, b, c, fine, coarse, energy, sem):
    copies = [
        pltpu.make_async_copy(src, dst, sem.at[i])
        for i, (src, dst) in enumerate(((a, fine), (b, coarse), (c, energy)))
    ]
    for copy in copies:
        copy.start()
    for copy in copies:
        copy.wait()


def side_rows(lev, coarse):
    longer = max(lev.X, lev.Y)
    return [longer * len(side_pieces(lev, (-1, 0), coarse, step)) for step in (1, 0)]


def solution(mesh):
    n_x, n_y = mesh.shape["gx"], mesh.shape["gy"]

    def step(*args):
        lf, lc = Level(args[0].shape), Level(args[2].shape)
        sizes = [side_rows(lf, False), side_rows(lc, True)]
        corners = [corner_rows(lf, False), corner_rows(lc, True)]
        f32 = jnp.float32
        vm = lambda *s: pltpu.VMEM(s, f32)
        results = pl.pallas_call(
            functools.partial(kernel, n_x, n_y, lf, lc),
            out_shape=(
                vm(*args[0].shape),
                vm(*args[2].shape),
                vm(2, STEPS),
            ),
            in_specs=[pl.BlockSpec(memory_space=pl.ANY)] * len(args),
            out_specs=[pl.BlockSpec(memory_space=pltpu.VMEM)] * 3,
            scratch_shapes=(
                [pltpu.VMEM(a.shape, a.dtype) for a in args]
                + [vm(3 * lf.field_rows(), L)] * 3
                + [vm(3 * lc.field_rows(), L)] * 3
                + [
                    vm(11 * lf.field_rows(), L),
                    vm(11 * lc.field_rows(), L),
                    vm(3 * lc.XE * (2 * lc.Y + 16), L),
                    vm(3 * lf.Y, L),
                    vm(lf.X * lf.NB * 64, L),
                    vm(3 * lf.X * lf.Y, L),
                ]
                + [vm(4, size[1], L) for size in sizes] * 2
                + [vm(STEPS - 1, 4, size[0], L) for size in sizes] * 2
                + [vm(STEPS, 4, corner, L) for corner in corners] * 2
                + [
                    vm(8, L),
                    vm(1, L),
                    vm(n_x * n_y, L),
                    pltpu.SemaphoreType.DMA((len(args),)),
                    pltpu.SemaphoreType.DMA((2, STEPS, 8)),
                    pltpu.SemaphoreType.DMA((2, STEPS, 8)),
                    pltpu.SemaphoreType.DMA((n_x * n_y,)),
                    pltpu.SemaphoreType.DMA((n_x * n_y,)),
                    pltpu.SemaphoreType.REGULAR((max(1, len(ready_rings(n_x, n_y))),)),
                ]
            ),
            compiler_params=pltpu.CompilerParams(
                collective_id=0, has_side_effects=True, vmem_limit_bytes=60 * 1024 * 1024
            ),
        )(*args)
        results = [pltpu.with_memory_space_constraint(r, pltpu.VMEM) for r in results]
        fine, coarse, energy = pl.pallas_call(
            write_out,
            out_shape=tuple(jax.ShapeDtypeStruct(r.shape, f32) for r in results),
            in_specs=[pl.BlockSpec(memory_space=pltpu.VMEM)] * 3,
            out_specs=[pl.BlockSpec(memory_space=pl.ANY)] * 3,
            scratch_shapes=[pltpu.SemaphoreType.DMA((3,))],
        )(*results)
        return fine, coarse, energy.T

    field, cells = P(None, "gx", "gy", None), P("gx", "gy", None)
    return jax.shard_map(
        step,
        mesh=mesh,
        in_specs=(field,) * 4 + (cells,) * 8 + (P(None, "gx", "gy"),),
        out_specs=(field, field, P()),
        check_vma=False,
    )
```

```python
import functools

import jax
import jax.numpy as jnp
from jax import lax
from jax.experimental import pallas as pl
from jax.experimental.pallas import tpu as pltpu
from jax.sharding import PartitionSpec as P

STEPS = 3
FACTOR = 0.15
MESH = pl.DeviceIdType.MESH
L = 128
SIDES = ((1, 0), (-1, 0), (0, 1), (0, -1))
CORNERS = ((1, 1), (1, -1), (-1, 1), (-1, -1))


class Level:
    def __init__(self, shape):
        _, self.X, self.Y, Z = shape
        self.H = Z // L
        self.XE = self.X + 4
        self.R = self.Y + 16
        while (self.H * self.R) % 8 != 4:
            self.R += 1
        self.NB = self.Y // 8

    def row(self, c, x, h, r):
        return ((c * self.XE + x) * self.H + h) * self.R + r

    def field_rows(self):
        return self.XE * self.H * self.R


def side_pieces(lev, d, coarse, step):
    out = [("u", c, h) for c in range(3) for h in range(lev.H)]
    out += [("div", 0, h) for h in range(lev.H)]
    if step == 0:
        out += [("wide", 0, h) for h in range(lev.H)]
    if coarse and d[0] + d[1] < 0:
        out += [("plane", 0, 0)]
    return out


def corner_extras(d):
    rings = [(a, b) for a in ((1, 2) if d[0] < 0 else (1,)) for b in ((1, 2) if d[1] < 0 else (1,))]
    return [(2, 1, 1)] + [(c, a, b) for a, b in rings if (a, b) != (1, 1) for c in range(3)]


def corner_rows(lev, coarse):
    return 2 * lev.H + int(coarse)


def inner(length, d, ring):
    return length - ring if d > 0 else ring - 1


def outer(length, d, ring):
    return -ring if d > 0 else length + ring - 1


def line(lev, d, ring, h, c, place):
    if d[0]:
        return lev.row(c, 2 + place(lev.X, d[0], ring), h, 8), lev.Y, 1
    return lev.row(c, 2, h, 8 + place(lev.Y, d[1], ring)), lev.X, lev.H * lev.R


def rows_of(start, count, stride):
    return pl.ds(start, count) if stride == 1 else pl.ds(start, count, stride)


def kernel(n_x, n_y, lf, lc, *refs):
    given, (fo, co, eo) = refs[:13], refs[13:16]
    held = refs[16:29]
    (fd, fp, cd, cp, fden, flam, frig, fmet, cden, clam, crig, cmet, offs) = held
    (uf0, uf1, uf2, uc0, uc1, uc2, mf, mc, plane, pair, wts, ghost,
     ss0f, ss0c, rs0f, rs0c, ssf, ssc, rsf, rsc, scf, scc, rcf, rcc,
     es, mine, box, load_sem, send_sem, recv_sem, en_send, en_recv, inside) = refs[29:]
    U = ((uf0, uf1, uf2), (uc0, uc1, uc2))
    M = (mf, mc)
    levs = (lf, lc)
    sside0, rside0, sside, rside = (ss0f, ss0c), (rs0f, rs0c), (ssf, ssc), (rsf, rsc)
    scorner, rcorner = (scf, scc), (rcf, rcc)
    disp, prev, out = (fd, cd), (fp, cp), (fo, co)
    den, lam, rig, met = (fden, cden), (flam, clam), (frig, crig), (fmet, cmet)
    ix, iy = lax.axis_index("gx"), lax.axis_index("gy")

    def has(d):
        conds = []
        if d[0] > 0:
            conds.append(ix < n_x - 1)
        if d[0] < 0:
            conds.append(ix > 0)
        if d[1] > 0:
            conds.append(iy < n_y - 1)
        if d[1] < 0:
            conds.append(iy > 0)
        return functools.reduce(jnp.logical_and, conds)

    DIRS = SIDES + CORNERS
    KG = plane_rows(lc)
    lane = lax.broadcasted_iota(jnp.int32, (8, L), 1)
    first, last = lane == 0, lane == L - 1

    IC, WIDE, FX, FY, FZP, FZM, A, B5, BZ, EN, DIV = range(11)

    def mrow(lev, name, x, h, r):
        return name * lev.field_rows() + (x * lev.H + h) * lev.R + r

    barrier = pltpu.get_barrier_semaphore()

    def signal(x, y):
        pl.semaphore_signal(barrier, inc=1, device_id={"gx": x, "gy": y}, device_id_type=MESH)

    everyone = n_x * n_y
    me = ix * n_y + iy

    def place(o):
        to = lax.rem(me + o, everyone)
        return to, lax.div(to, n_y), lax.rem(to, n_y)

    greeted = jnp.int32(0)
    for d in DIRS:
        greeted = greeted + has(d).astype(jnp.int32)

        @pl.when(has(d))
        def _(d=d):
            signal(ix + d[0], iy + d[1])

    rings = ready_rings(n_x, n_y)

    def within(d):
        x, y = ix + d[0], iy + d[1]
        return (x >= 0) & (x < n_x) & (y >= 0) & (y < n_y)

    def ready_signal(i):
        for d in rings[i]:
            @pl.when(within(d))
            def _(d=d):
                pl.semaphore_signal(
                    inside.at[i], inc=1, device_id={"gx": ix + d[0], "gy": iy + d[1]}, device_id_type=MESH
                )

    def ready_wait(i):
        pl.semaphore_wait(inside.at[i], sum(within(d).astype(jnp.int32) for d in rings[i]))

    def coef(lev, h, rows):
        ln = lax.broadcasted_iota(jnp.int32, (rows, L), 1)
        value = jnp.full((rows, L), 0.5, jnp.float32)
        if h == 0:
            value = jnp.where(ln == 0, 1.0, value)
        if h == lev.H - 1:
            value = jnp.where(ln == L - 1, 1.0, value)
        return value

    def shifts(vals):
        n = len(vals)
        ups = [pltpu.roll(v, L - 1, 1) for v in vals]
        dns = [pltpu.roll(v, 1, 1) for v in vals]
        lane_v = lane if vals[0].shape[0] == 8 else lax.broadcasted_iota(jnp.int32, vals[0].shape, 1)
        fst, lst = lane_v == 0, lane_v == L - 1
        hi = [jnp.where(lst, ups[i + 1] if i + 1 < n else vals[i], ups[i]) for i in range(n)]
        lo = [jnp.where(fst, dns[i - 1] if i > 0 else vals[i], dns[i]) for i in range(n)]
        return hi, lo

    def load(i):
        return pltpu.make_async_copy(given[i], held[i], load_sem.at[i])

    FIRST = (2, 0, 11, 10, 7, 6)
    LATER = tuple(i for i in range(13) if i not in FIRST)
    for i in FIRST + LATER:
        load(i).start()

    zero = jnp.zeros((8, L), jnp.float32)
    for lev, us, m in zip(levs, U, M):
        lines = lev.XE * lev.H

        @pl.loop(0, 3 * lines, unroll=4)
        def _(q, lev=lev, us=us):
            for u in us:
                u[pl.ds(q * lev.R, 8), :] = zero
                u[pl.ds(q * lev.R + lev.Y + 8, 8), :] = zero

        @pl.loop(0, lines, unroll=4)
        def _(q, lev=lev, m=m):
            for name in (WIDE, DIV):
                m[pl.ds(name * lev.field_rows() + q * lev.R, 8), :] = zero
                m[pl.ds(name * lev.field_rows() + q * lev.R + lev.Y + 8, 8), :] = zero

        for x in (0, 1, lev.X + 2, lev.X + 3):
            for h in range(lev.H):
                for b in range(lev.NB):
                    for u in us:
                        for c in range(3):
                            u[pl.ds(lev.row(c, x, h, 8 + 8 * b), 8), :] = zero
                    for name in (WIDE, DIV):
                        m[pl.ds(mrow(lev, name, x, h, 8 + 8 * b), 8), :] = zero

    @pl.loop(0, 3 * KG // 8, unroll=4)
    def _(q):
        plane[pl.ds(8 * q, 8), :] = zero

    plane[pl.ds(3 * KG, 8), :] = zero
    for k, d in enumerate(DIRS):
        @pl.when(jnp.logical_not(has((-d[0], -d[1]))))
        def _(k=k):
            for n in range(2):
                for step in range(STEPS):
                    if k >= 4:
                        rcorner[n][step, k - 4, :, :] = jnp.zeros(rcorner[n].shape[2:], jnp.float32)
                    elif step == 0:
                        rside0[n][k, :, :] = jnp.zeros(rside0[n].shape[1:], jnp.float32)
                    else:
                        rside[n][step - 1, k, :, :] = jnp.zeros(rside[n].shape[2:], jnp.float32)

    for i in FIRST:
        load(i).wait()

    for n in (1, 0):
        lev, us, u_in, m = levs[n], U[n], disp[n], M[n]

        @pl.loop(0, lev.X, unroll=4)
        def _(x, n=n, lev=lev, us=us, u_in=u_in, m=m):
            for h in range(lev.H):
                for b in range(lev.NB):
                    src = (x, pl.ds(8 * b, 8), pl.ds(h * L, L))
                    g = met[n][src]
                    m[pl.ds(mrow(lev, IC, x + 2, h, 8 + 8 * b), 8), :] = (1.0 / g) * coef(lev, h, 8)
                    m[pl.ds(mrow(lev, WIDE, x + 2, h, 8 + 8 * b), 8), :] = rig[n][src] * g
                    for c in range(3):
                        us[0][pl.ds(lev.row(c, x + 2, h, 8 + 8 * b), 8), :] = u_in[(c,) + src]

    def side_size(n, d):
        return levs[n].Y if d[0] else levs[n].X

    def copy(k, d, step, n):
        if k >= 4:
            s, r = scorner[n].at[step, k - 4], rcorner[n].at[step, k - 4]
        else:
            rows = pl.ds(0, side_size(n, d) * len(side_pieces(levs[n], d, n == 1, step)))
            if step == 0:
                s, r = sside0[n].at[k, rows], rside0[n].at[k, rows]
            else:
                s, r = sside[n].at[step - 1, k, rows], rside[n].at[step - 1, k, rows]
        return pltpu.make_async_remote_copy(
            src_ref=s, dst_ref=r, send_sem=send_sem.at[n, step, k],
            recv_sem=recv_sem.at[n, step, k],
            device_id={"gx": ix + d[0], "gy": iy + d[1]}, device_id_type=MESH,
        )

    XS, YS, CS = (0, 1), (2, 3), (4, 5, 6, 7)

    def divergence(step, n, start, count, stride):
        lev, u, m = levs[n], U[n][step], M[n]
        SX, cs = lev.H * lev.R, lev.field_rows()
        get = lambda c, h, off: u[rows_of(start + c * cs + h * lev.R + off, count, stride), :]
        hi, lo = shifts([get(2, h, 0) for h in range(lev.H)])
        values = []
        for h in range(lev.H):
            v = 0.5 * ((get(0, h, SX) - get(0, h, -SX)) + (get(1, h, 1) - get(1, h, -1)))
            ic = m[rows_of(IC * cs + start + h * lev.R, count, stride), :]
            values.append(v + ic * (hi[h] - lo[h]))
        return values

    def lanes_of(rows):
        return lax.broadcasted_iota(jnp.int32, (rows, L), 1)

    def merged(values):
        total, ln = values[0], lanes_of(values[0].shape[0])
        for i, v in enumerate(values[1:], 1):
            total = jnp.where(ln == i, pltpu.roll(v, i, 1), total)
        return total

    def parted(value, i):
        return pltpu.roll(value, L - i, 1) if i else value

    def corner_row(lev, d, c, a, b, h, place):
        return pl.ds(lev.row(c, 2 + place(lev.X, d[0], a), h, 8 + place(lev.Y, d[1], b)), 1)

    def pack(step, n, which):
        lev, u, m = levs[n], U[n][step], M[n]
        for k in which:
            d = DIRS[k]
            if k >= 4:
                for c in range(2):
                    for h in range(lev.H):
                        scorner[n][step, k - 4, pl.ds(c * lev.H + h, 1), :] = u[
                            corner_row(lev, d, c, 1, 1, h, inner), :
                        ]
                if n:
                    extras = [u[corner_row(lev, d, c, a, b, 0, inner), :] for c, a, b in corner_extras(d)]
                    scorner[n][step, k - 4, pl.ds(2 * lev.H, 1), :] = merged(extras)
                continue
            size = side_size(n, d)
            parts = divergence(step, n, *line(lev, d, 1, 0, 0, inner))
            for at, (kind, c, h) in enumerate(side_pieces(lev, d, n == 1, step)):
                first_row, count, stride = line(lev, d, 1, h, c, inner)
                if kind == "u":
                    value = u[rows_of(first_row, count, stride), :]
                elif kind == "div":
                    value = parts[h]
                elif kind == "wide":
                    value = m[rows_of(WIDE * lev.field_rows() + first_row, count, stride), :]
                else:
                    value = merged([u[rows_of(*line(lev, d, 2, 0, e, inner)), :] for e in range(3)])
                if step == 0:
                    sside0[n][k, pl.ds(at * size, size), :] = value
                else:
                    sside[n][step - 1, k, pl.ds(at * size, size), :] = value

    def start(step, n, which):
        for k in which:
            @pl.when(has(DIRS[k]))
            def _(k=k):
                copy(k, DIRS[k], step, n).start()

    def unpack(step, n, which):
        lev, u, m = levs[n], U[n][step], M[n]
        fr = lev.field_rows()
        for k in which:
            @pl.when(has((-DIRS[k][0], -DIRS[k][1])))
            def _(k=k):
                copy(k, DIRS[k], step, n).wait_recv()

        for k in which:
            d = DIRS[k]
            back = (-d[0], -d[1])
            if k >= 4:
                for c in range(2):
                    for h in range(lev.H):
                        value = rcorner[n][step, k - 4, pl.ds(c * lev.H + h, 1), :]
                        u[corner_row(lev, d, c, 1, 1, h, outer), :] = value
                        if c == 0:
                            beside = lev.row(0, 2 + inner(lev.X, back[0], 1), h, 8 + outer(lev.Y, d[1], 1))
                            sign = back[0]
                        else:
                            beside = lev.row(0, 2 + outer(lev.X, d[0], 1), h, 8 + inner(lev.Y, back[1], 1))
                            sign = back[1]
                        at = pl.ds(DIV * fr + beside, 1)
                        m[at, :] = m[at, :] + (0.5 * sign) * value
                if n:
                    value = rcorner[n][step, k - 4, pl.ds(2 * lev.H, 1), :]
                    for i, (c, a, b) in enumerate(corner_extras(d)):
                        u[corner_row(lev, d, c, a, b, 0, outer), :] = parted(value, i)
                continue
            axis, size = (0 if d[0] else 1), side_size(n, d)
            half = jnp.where(has(back), 0.5 * (d[0] + d[1]), 0.0)
            for at, (kind, c, h) in enumerate(side_pieces(lev, d, n == 1, step)):
                rows = pl.ds(at * size, size)
                got = rside0[n][k, rows, :] if step == 0 else rside[n][step - 1, k, rows, :]
                first_row, count, stride = line(lev, d, 1, h, c, outer)
                if kind == "u":
                    u[rows_of(first_row, count, stride), :] = got
                elif kind == "div":
                    own = u[rows_of(*line(lev, back, 1, h, axis, inner)), :]
                    m[rows_of(DIV * fr + first_row, count, stride), :] = got + half * own
                elif kind == "wide":
                    m[rows_of(WIDE * fr + first_row, count, stride), :] = got
                else:
                    for e in range(3):
                        u[rows_of(*line(lev, d, 2, 0, e, outer)), :] = parted(got, e)

    for n in (1, 0):
        pack(0, n, XS + CS + YS)
    pl.semaphore_wait(barrier, greeted)
    for n in (1, 0):
        start(0, n, YS + CS + XS)
    for i in LATER:
        load(i).wait()

    X, Y = lf.X, lf.Y
    YE = lc.Y + 3
    sub = lax.broadcasted_iota(jnp.int32, (8, Y), 0)
    lan = lax.broadcasted_iota(jnp.int32, (8, Y), 1)
    row8 = lax.broadcasted_iota(jnp.int32, (8, KG), 0)
    cell = lax.broadcasted_iota(jnp.int32, (8, KG), 1)
    near_y = jnp.where(row8 % 2 == 0, 0.75, 0.25)
    cell_x = cell // YE
    cell_y = cell - cell_x * YE - row8 // 2

    def weight(o_all, shift, near):
        return jnp.where(o_all == shift, near, 0.0) + jnp.where(o_all + 1 == shift, 1.0 - near, 0.0)

    for x in range(X):
        near_x = 0.75 if x % 2 == 0 else 0.25
        for b in range(lf.NB):
            both = []
            for axis in range(2):
                o_row = jnp.broadcast_to(offs[axis, pl.ds(x, 1), :], (8, Y))
                o_col = jnp.sum(jnp.where(lan == sub + 8 * b, o_row, 0).astype(jnp.float32), axis=1, keepdims=True)
                both.append(jnp.broadcast_to(o_col, (8, KG)).astype(jnp.int32))
            w = weight(both[0], cell_x - (x // 2 + 1), near_x) * weight(both[1], cell_y - (4 * b + 1), near_y)
            for part in range(3):
                wts[pl.ds(x * Y + 8 * b, 8), pl.ds(part * KG, KG)] = w.astype(jnp.bfloat16)

    for n, lev in enumerate(levs):
        m = M[n]

        @pl.loop(0, lev.X, unroll=4)
        def _(x, n=n, lev=lev, m=m):
            for b in range(lev.NB):
                def at(name, h):
                    return pl.ds(mrow(lev, name, x + 2, h, 8 + 8 * b), 8)

                vs = []
                for h in range(lev.H):
                    src = (x, pl.ds(8 * b, 8), pl.ds(h * L, L))
                    g, de, la, ri = met[n][src], den[n][src], lam[n][src], rig[n][src]
                    rden = 1.0 / de
                    ic = m[at(IC, h), :]
                    inv = ic * (1.0 / coef(lev, h, 8))
                    bb = (FACTOR * (la + ri)) * rden
                    m[at(A, h), :] = FACTOR * inv * rden
                    m[at(B5, h), :] = 0.5 * bb
                    m[at(BZ, h), :] = bb * ic
                    m[at(EN, h), :] = de * g
                    vs.append(ri * inv)
                hi, lo = shifts(vs)
                for h in range(lev.H):
                    m[at(FZP, h), :] = 0.5 * (vs[h] + hi[h])
                    m[at(FZM, h), :] = 0.5 * (vs[h] + lo[h])

    def faces_x(n, xs):
        lev, m = levs[n], M[n]
        for x in xs:
            for h in range(lev.H):
                for b in range(lev.NB):
                    r = 8 + 8 * b
                    w0 = m[pl.ds(mrow(lev, WIDE, x + 1, h, r), 8), :]
                    w1 = m[pl.ds(mrow(lev, WIDE, x + 2, h, r), 8), :]
                    m[pl.ds(mrow(lev, FX, x + 1, h, r), 8), :] = 0.5 * (w0 + w1)

    def faces_y(n):
        lev, m = levs[n], M[n]

        @pl.loop(0, lev.X, unroll=4)
        def _(x):
            for h in range(lev.H):
                for b in range(lev.NB + 1):
                    r = 8 + 8 * b
                    w0 = m[pl.ds(mrow(lev, WIDE, x + 2, h, r - 1), 8), :]
                    w1 = m[pl.ds(mrow(lev, WIDE, x + 2, h, r), 8), :]
                    m[pl.ds(mrow(lev, FY, x + 2, h, r), 8), :] = 0.5 * (w0 + w1)

    def divergences(step, n, xs):
        lev, m = levs[n], M[n]

        def column(x):
            for b in range(lev.NB):
                values = divergence(step, n, lev.row(0, x + 2, 0, 8 + 8 * b), 8, 1)
                for h in range(lev.H):
                    m[pl.ds(mrow(lev, DIV, x + 2, h, 8 + 8 * b), 8), :] = values[h]

        for x in xs:
            column(x)

    def ghosts(step):
        uc = U[1][step]
        for c in range(3):
            for x in range(lc.X + 3):
                for q in range(0, YE, 8):
                    plane[pl.ds(c * KG + x * YE + q, 8), :] = pltpu.roll(
                        uc[pl.ds(lc.row(c, x + 1, 0, 7 + q), 8), :], L - 1, 1
                    )
        for c in range(3):
            left, parts = plane[pl.ds(c * KG, KG), :], []
            for _ in range(3):
                parts.append(left.astype(jnp.bfloat16))
                left = left - parts[-1].astype(jnp.float32)
            ghost[pl.ds(c * lf.X * lf.Y, lf.X * lf.Y), :] = jnp.dot(
                wts[...], jnp.concatenate(parts, axis=0), preferred_element_type=jnp.float32
            )

    def top_ghost(step, x, c):
        uf = U[0][step]
        base = c * lf.Y
        for b in range(lf.NB):
            pair[pl.ds(base + 8 * b, 8), :] = (
                uf[pl.ds(lf.row(c, 2 * x + 2, 0, 8 + 8 * b), 8), :]
                + uf[pl.ds(lf.row(c, 2 * x + 3, 0, 8 + 8 * b), 8), :]
            )
        s = pair[pl.ds(base, 8, 2), :] + pair[pl.ds(base + 1, 8, 2), :]
        return pltpu.roll(0.25 * s, 1, 1)

    def update(step, n, columns, inside_x=None):
        lev = levs[n]
        u, m = U[n][step], M[n]
        SX = lev.H * lev.R
        H = lev.H

        def body(x, acc, comps=(0, 1, 2)):
            for b in range(lev.NB):
                r0 = 8 + 8 * b

                def mat(name, h, off=0):
                    return m[pl.ds(mrow(lev, name, x + 2, h, r0) + off, 8), :]

                dhi, dlo = shifts([mat(DIV, h) for h in range(H)]) if 2 in comps else (None, None)
                cells = [None] * H
                for c in comps:
                    get = lambda h, off=0, c=c: u[pl.ds(lev.row(c, x + 2, h, r0) + off, 8), :]
                    cur = [get(h) for h in range(H)]
                    hi, lo = shifts(cur)
                    if n == 0:
                        g = ghost[pl.ds(((c * lev.X + x) * lev.NB + b) * 8, 8), :]
                        hi[H - 1] = jnp.where(last, g, hi[H - 1])
                    else:
                        hi[H - 1] = jnp.where(last, 0.0, hi[H - 1])
                        lo[0] = jnp.where(first, top_ghost(step, x, c), lo[0])
                    for h in range(H):
                        v = cur[h]
                        flux = mat(FX, h) * (get(h, SX) - v) - mat(FX, h, -SX) * (v - get(h, -SX))
                        flux = flux + (mat(FY, h, 1) * (get(h, 1) - v) - mat(FY, h) * (v - get(h, -1)))
                        flux = flux + (mat(FZP, h) * (hi[h] - v) - mat(FZM, h) * (v - lo[h]))
                        if c == 0:
                            grad = mat(B5, h) * (mat(DIV, h, SX) - mat(DIV, h, -SX))
                        elif c == 1:
                            grad = mat(B5, h) * (mat(DIV, h, 1) - mat(DIV, h, -1))
                        else:
                            grad = mat(BZ, h) * (dhi[h] - dlo[h])
                        rate = mat(A, h) * flux + grad
                        if step == 0:
                            p = prev[n][c, x, pl.ds(8 * b, 8), pl.ds(h * L, L)]
                        else:
                            p = U[n][step - 1][pl.ds(lev.row(c, x + 2, h, r0), 8), :]
                        change = (v - p) + rate
                        new = v + change
                        if step == STEPS - 1:
                            out[n][c, x, pl.ds(8 * b, 8), pl.ds(h * L, L)] = new
                        else:
                            U[n][step + 1][pl.ds(lev.row(c, x + 2, h, r0), 8), :] = new
                        e = change * change - new * rate
                        cells[h] = e if cells[h] is None else cells[h] + e
                for h in range(H):
                    acc = acc + mat(EN, h) * cells[h]
            return acc

        acc = jnp.zeros((8, L), jnp.float32)
        for x, comps in columns:
            acc = body(x, acc, comps)
        if inside_x is not None:
            acc = lax.fori_loop(*inside_x, body, acc, unroll=4)
        row = pl.ds(4 * n + step, 1)
        es[row, :] = es[row, :] + jnp.sum(acc, axis=0, keepdims=True)

    es[...] = jnp.zeros((8, L), jnp.float32)
    ALL = (0, 1, 2)
    for n, lev in enumerate(levs):
        faces_x(n, range(1, lev.X))

    def coarse_start(step):
        unpack(step, 1, YS)
        if step == 0:
            faces_y(1)
        divergences(step, 1, range(1, lc.X - 1))
        update(step, 1, (), (2, lc.X - 2))

    def coarse_halo(step):
        unpack(step, 1, XS + CS)
        if step == 0:
            faces_x(1, (0, lc.X))
        divergences(step, 1, (0, lc.X - 1))

    for step in range(STEPS - 1):
        coarse_start(step)
        coarse_halo(step)
        update(step, 1, [(0, ALL), (1, ALL), (lc.X - 1, ALL), (lc.X - 2, (0,))])
        pack(step + 1, 1, XS + CS)
        start(step + 1, 1, CS + XS)
        update(step, 1, [(lc.X - 2, (1, 2))])
        pack(step + 1, 1, YS)
        start(step + 1, 1, YS)
        ghosts(step)
        unpack(step, 0, YS + XS + CS)
        if step == 0:
            faces_y(0)
            faces_x(0, (0, X))
        divergences(step, 0, (0, 1, 2, X - 3, X - 2, X - 1))
        update(step, 0, [(0, ALL), (X - 1, ALL), (1, (0,)), (X - 2, (0,))])
        pack(step + 1, 0, XS + CS)
        start(step + 1, 0, CS + XS)
        divergences(step, 0, range(3, X - 3))
        update(step, 0, [(1, (1, 2)), (X - 2, (1, 2))], (2, X - 2))
        pack(step + 1, 0, YS)
        start(step + 1, 0, YS)
        if step < len(rings):
            if step:
                ready_wait(step - 1)
            ready_signal(step)
    step = STEPS - 1
    coarse_start(step)
    ghosts(step)
    unpack(step, 0, YS)
    divergences(step, 0, range(1, X - 1))
    update(step, 0, (), (2, X - 4))
    coarse_halo(step)
    update(step, 1, [(x, ALL) for x in (0, 1, lc.X - 2, lc.X - 1)])
    ghosts(step)
    unpack(step, 0, XS + CS)
    divergences(step, 0, (0, X - 1))
    update(step, 0, [(x, ALL) for x in (0, 1, X - 4, X - 3, X - 2, X - 1)])
    for i in range(min(STEPS - 1, len(rings)) - 1, len(rings)):
        if i >= 0:
            ready_wait(i)
        if i + 1 < len(rings):
            ready_signal(i + 1)

    def share(o):
        to, x, y = place(o)
        return pltpu.make_async_remote_copy(
            src_ref=mine, dst_ref=box.at[pl.ds(me, 1)], send_sem=en_send, recv_sem=en_recv,
            device_id={"gx": x, "gy": y}, device_id_type=MESH,
        )

    def all_rows(sem):
        rows = box.at[pl.ds(0, everyone - 1)]
        return pltpu.make_async_copy(rows, rows, sem)

    sums = jnp.sum(es[...], axis=1, keepdims=True)
    diagonal = lane == lax.broadcasted_iota(jnp.int32, (8, L), 0)
    row = jnp.sum(jnp.where(diagonal, sums, 0.0), axis=0, keepdims=True)
    mine[...] = row

    @pl.loop(1, everyone)
    def _(o):
        share(o).start()

    box[pl.ds(me, 1), :] = row

    for step in range(STEPS):
        for k, d in enumerate(DIRS):
            @pl.when(has(d))
            def _(k=k, d=d, step=step):
                for n in range(2):
                    copy(k, d, step, n).wait_send()

    all_rows(en_send).wait()
    all_rows(en_recv).wait()
    total = jnp.sum(box[...], axis=0, keepdims=True)
    for n, lev in enumerate(levs):
        cells = lev.X * n_x * lev.Y * n_y * lev.H * L
        eo[pl.ds(n, 1), :] = total[:, 4 * n : 4 * n + STEPS] / cells


def ready_rings(n_x, n_y):
    rings, reach = [], 2
    while reach < max(n_x, n_y) - 1:
        xs = (-reach, 0, reach) if reach < n_x - 1 else (0,)
        ys = (-reach, 0, reach) if reach < n_y - 1 else (0,)
        rings.append([(x, y) for x in xs for y in ys if x or y])
        reach *= 2
    return rings


def write_out(a, b, c, fine, coarse, energy, sem):
    copies = [
        pltpu.make_async_copy(src, dst, sem.at[i])
        for i, (src, dst) in enumerate(((a, fine), (b, coarse), (c, energy)))
    ]
    for copy in copies:
        copy.start()
    for copy in copies:
        copy.wait()


def plane_rows(lc):
    return -(-(lc.X + 3) * (lc.Y + 3) // L) * L


def side_rows(lev, coarse):
    longer = max(lev.X, lev.Y)
    return [longer * len(side_pieces(lev, (-1, 0), coarse, step)) for step in (1, 0)]


def solution(mesh):
    n_x, n_y = mesh.shape["gx"], mesh.shape["gy"]

    def step(*args):
        lf, lc = Level(args[0].shape), Level(args[2].shape)
        sizes = [side_rows(lf, False), side_rows(lc, True)]
        corners = [corner_rows(lf, False), corner_rows(lc, True)]
        f32 = jnp.float32
        vm = lambda *s: pltpu.VMEM(s, f32)
        results = pl.pallas_call(
            functools.partial(kernel, n_x, n_y, lf, lc),
            out_shape=(
                vm(*args[0].shape),
                vm(*args[2].shape),
                vm(2, STEPS),
            ),
            in_specs=[pl.BlockSpec(memory_space=pl.ANY)] * len(args),
            out_specs=[pl.BlockSpec(memory_space=pltpu.VMEM)] * 3,
            scratch_shapes=(
                [pltpu.VMEM(a.shape, a.dtype) for a in args]
                + [vm(3 * lf.field_rows(), L)] * 3
                + [vm(3 * lc.field_rows(), L)] * 3
                + [
                    vm(11 * lf.field_rows(), L),
                    vm(11 * lc.field_rows(), L),
                    vm(3 * plane_rows(lc) + 8, L),
                    vm(3 * lf.Y, L),
                    pltpu.VMEM((lf.X * lf.Y, 3 * plane_rows(lc)), jnp.bfloat16),
                    vm(3 * lf.X * lf.Y, L),
                ]
                + [vm(4, size[1], L) for size in sizes] * 2
                + [vm(STEPS - 1, 4, size[0], L) for size in sizes] * 2
                + [vm(STEPS, 4, corner, L) for corner in corners] * 2
                + [
                    vm(8, L),
                    vm(1, L),
                    vm(n_x * n_y, L),
                    pltpu.SemaphoreType.DMA((len(args),)),
                    pltpu.SemaphoreType.DMA((2, STEPS, 8)),
                    pltpu.SemaphoreType.DMA((2, STEPS, 8)),
                    pltpu.SemaphoreType.DMA,
                    pltpu.SemaphoreType.DMA,
                    pltpu.SemaphoreType.REGULAR((max(1, len(ready_rings(n_x, n_y))),)),
                ]
            ),
            compiler_params=pltpu.CompilerParams(
                collective_id=0, has_side_effects=True, vmem_limit_bytes=60 * 1024 * 1024
            ),
        )(*args)
        results = [pltpu.with_memory_space_constraint(r, pltpu.VMEM) for r in results]
        fine, coarse, energy = pl.pallas_call(
            write_out,
            out_shape=tuple(jax.ShapeDtypeStruct(r.shape, f32) for r in results),
            in_specs=[pl.BlockSpec(memory_space=pltpu.VMEM)] * 3,
            out_specs=[pl.BlockSpec(memory_space=pl.ANY)] * 3,
            scratch_shapes=[pltpu.SemaphoreType.DMA((3,))],
        )(*results)
        return fine, coarse, energy.T

    field, cells = P(None, "gx", "gy", None), P("gx", "gy", None)
    return jax.shard_map(
        step,
        mesh=mesh,
        in_specs=(field,) * 4 + (cells,) * 8 + (P(None, "gx", "gy"),),
        out_specs=(field, field, P()),
        check_vma=False,
    )
```

```python
import functools

import jax
import jax.numpy as jnp
from jax import lax
from jax.experimental import pallas as pl
from jax.experimental.pallas import tpu as pltpu
from jax.sharding import PartitionSpec as P

STEPS = 3
FACTOR = 0.15
MESH = pl.DeviceIdType.MESH
L = 128
SIDES = ((1, 0), (-1, 0), (0, 1), (0, -1))
CORNERS = ((1, 1), (1, -1), (-1, 1), (-1, -1))


class Level:
    def __init__(self, shape):
        _, self.X, self.Y, Z = shape
        self.H = Z // L
        self.XE = self.X + 4
        self.R = self.Y + 16
        while (self.H * self.R) % 8 != 4:
            self.R += 1
        self.NB = self.Y // 8

    def row(self, c, x, h, r):
        return ((c * self.XE + x) * self.H + h) * self.R + r

    def field_rows(self):
        return self.XE * self.H * self.R


def side_pieces(lev, d, coarse, step):
    out = [("u", c, h) for c in range(3) for h in range(lev.H)]
    out += [("div", 0, h) for h in range(lev.H)]
    if step == 0:
        out += [("wide", 0, h) for h in range(lev.H)]
    if coarse and d[0] + d[1] < 0:
        out += [("plane", 0, 0)]
    return out


def corner_extras(d):
    rings = [(a, b) for a in ((1, 2) if d[0] < 0 else (1,)) for b in ((1, 2) if d[1] < 0 else (1,))]
    return [(2, 1, 1)] + [(c, a, b) for a, b in rings if (a, b) != (1, 1) for c in range(3)]


def corner_rows(lev, coarse):
    return 2 * lev.H + int(coarse)


def inner(length, d, ring):
    return length - ring if d > 0 else ring - 1


def outer(length, d, ring):
    return -ring if d > 0 else length + ring - 1


def line(lev, d, ring, h, c, place):
    if d[0]:
        return lev.row(c, 2 + place(lev.X, d[0], ring), h, 8), lev.Y, 1
    return lev.row(c, 2, h, 8 + place(lev.Y, d[1], ring)), lev.X, lev.H * lev.R


def rows_of(start, count, stride):
    return pl.ds(start, count) if stride == 1 else pl.ds(start, count, stride)


def kernel(n_x, n_y, lf, lc, *refs):
    given, (fo, co, eo) = refs[:13], refs[13:16]
    held = refs[16:29]
    (fd, fp, cd, cp, fden, flam, frig, fmet, cden, clam, crig, cmet, offs) = held
    (uf0, uf1, uf2, uc0, uc1, uc2, mf, mc, plane, pair, wts, ghost,
     ss0f, ss0c, rs0f, rs0c, ssf, ssc, rsf, rsc, scf, scc, rcf, rcc,
     es, mine, box, load_sem, send_sem, recv_sem, en_send, en_recv, inside) = refs[29:]
    U = ((uf0, uf1, uf2), (uc0, uc1, uc2))
    M = (mf, mc)
    levs = (lf, lc)
    sside0, rside0, sside, rside = (ss0f, ss0c), (rs0f, rs0c), (ssf, ssc), (rsf, rsc)
    scorner, rcorner = (scf, scc), (rcf, rcc)
    disp, prev, out = (fd, cd), (fp, cp), (fo, co)
    den, lam, rig, met = (fden, cden), (flam, clam), (frig, crig), (fmet, cmet)
    ix, iy = lax.axis_index("gx"), lax.axis_index("gy")

    def has(d):
        conds = []
        if d[0] > 0:
            conds.append(ix < n_x - 1)
        if d[0] < 0:
            conds.append(ix > 0)
        if d[1] > 0:
            conds.append(iy < n_y - 1)
        if d[1] < 0:
            conds.append(iy > 0)
        return functools.reduce(jnp.logical_and, conds)

    DIRS = SIDES + CORNERS
    KG = plane_rows(lc)
    lane = lax.broadcasted_iota(jnp.int32, (8, L), 1)
    first, last = lane == 0, lane == L - 1

    IC, WIDE, FX, FY, FZP, FZM, A, B5, BZ, EN, DIV = range(11)

    def mrow(lev, name, x, h, r):
        return name * lev.field_rows() + (x * lev.H + h) * lev.R + r

    barrier = pltpu.get_barrier_semaphore()

    def signal(x, y):
        pl.semaphore_signal(barrier, inc=1, device_id={"gx": x, "gy": y}, device_id_type=MESH)

    everyone = n_x * n_y
    me = ix * n_y + iy

    def place(o):
        to = lax.rem(me + o, everyone)
        return to, lax.div(to, n_y), lax.rem(to, n_y)

    greeted = jnp.int32(0)
    for d in DIRS:
        greeted = greeted + has(d).astype(jnp.int32)

        @pl.when(has(d))
        def _(d=d):
            signal(ix + d[0], iy + d[1])

    rings = ready_rings(n_x, n_y)

    def within(d):
        x, y = ix + d[0], iy + d[1]
        return (x >= 0) & (x < n_x) & (y >= 0) & (y < n_y)

    def ready_signal(i):
        for d in rings[i]:
            @pl.when(within(d))
            def _(d=d):
                pl.semaphore_signal(
                    inside.at[i], inc=1, device_id={"gx": ix + d[0], "gy": iy + d[1]}, device_id_type=MESH
                )

    def ready_wait(i):
        pl.semaphore_wait(inside.at[i], sum(within(d).astype(jnp.int32) for d in rings[i]))

    def coef(lev, h, rows):
        ln = lax.broadcasted_iota(jnp.int32, (rows, L), 1)
        value = jnp.full((rows, L), 0.5, jnp.float32)
        if h == 0:
            value = jnp.where(ln == 0, 1.0, value)
        if h == lev.H - 1:
            value = jnp.where(ln == L - 1, 1.0, value)
        return value

    def shifts(vals):
        n = len(vals)
        ups = [pltpu.roll(v, L - 1, 1) for v in vals]
        dns = [pltpu.roll(v, 1, 1) for v in vals]
        lane_v = lane if vals[0].shape[0] == 8 else lax.broadcasted_iota(jnp.int32, vals[0].shape, 1)
        fst, lst = lane_v == 0, lane_v == L - 1
        hi = [jnp.where(lst, ups[i + 1] if i + 1 < n else vals[i], ups[i]) for i in range(n)]
        lo = [jnp.where(fst, dns[i - 1] if i > 0 else vals[i], dns[i]) for i in range(n)]
        return hi, lo

    LOADS = ((2, 11, 10), (0, 7, 6), (1, 3, 4, 5, 8, 9), (12,))

    def load(group):
        for i in LOADS[group]:
            pltpu.make_async_copy(given[i], held[i], load_sem.at[group]).start()

    def wait_rows(sem, rows):
        span = mf.at[pl.ds(0, rows)]
        pltpu.make_async_copy(span, span, sem).wait()

    def loaded(group):
        if group == 3:
            pltpu.make_async_copy(given[12], held[12], load_sem.at[3]).wait()
        else:
            wait_rows(load_sem.at[group], sum(given[i].size // L for i in LOADS[group]))

    load(0)
    load(1)

    zero = jnp.zeros((8, L), jnp.float32)
    for lev, us, m in zip(levs, U, M):
        lines = lev.XE * lev.H

        @pl.loop(0, 3 * lines, unroll=4)
        def _(q, lev=lev, us=us):
            for u in us:
                u[pl.ds(q * lev.R, 8), :] = zero
                u[pl.ds(q * lev.R + lev.Y + 8, 8), :] = zero

        @pl.loop(0, lines, unroll=4)
        def _(q, lev=lev, m=m):
            for name in (WIDE, DIV):
                m[pl.ds(name * lev.field_rows() + q * lev.R, 8), :] = zero
                m[pl.ds(name * lev.field_rows() + q * lev.R + lev.Y + 8, 8), :] = zero

        for x in (0, 1, lev.X + 2, lev.X + 3):
            for h in range(lev.H):
                for b in range(lev.NB):
                    for u in us:
                        for c in range(3):
                            u[pl.ds(lev.row(c, x, h, 8 + 8 * b), 8), :] = zero
                    for name in (WIDE, DIV):
                        m[pl.ds(mrow(lev, name, x, h, 8 + 8 * b), 8), :] = zero

    @pl.loop(0, 3 * KG // 8, unroll=4)
    def _(q):
        plane[pl.ds(8 * q, 8), :] = zero

    plane[pl.ds(3 * KG, 8), :] = zero
    for k, d in enumerate(DIRS):
        @pl.when(jnp.logical_not(has((-d[0], -d[1]))))
        def _(k=k):
            for n in range(2):
                for step in range(STEPS):
                    if k >= 4:
                        rcorner[n][step, k - 4, :, :] = jnp.zeros(rcorner[n].shape[2:], jnp.float32)
                    elif step == 0:
                        rside0[n][k, :, :] = jnp.zeros(rside0[n].shape[1:], jnp.float32)
                    else:
                        rside[n][step - 1, k, :, :] = jnp.zeros(rside[n].shape[2:], jnp.float32)

    def take_in(n):
        lev, us, u_in, m = levs[n], U[n], disp[n], M[n]

        @pl.loop(0, lev.X, unroll=4)
        def _(x):
            for h in range(lev.H):
                for b in range(lev.NB):
                    src = (x, pl.ds(8 * b, 8), pl.ds(h * L, L))
                    g = met[n][src]
                    m[pl.ds(mrow(lev, IC, x + 2, h, 8 + 8 * b), 8), :] = (1.0 / g) * coef(lev, h, 8)
                    m[pl.ds(mrow(lev, WIDE, x + 2, h, 8 + 8 * b), 8), :] = rig[n][src] * g
                    for c in range(3):
                        us[0][pl.ds(lev.row(c, x + 2, h, 8 + 8 * b), 8), :] = u_in[(c,) + src]

    def side_size(n, d):
        return levs[n].Y if d[0] else levs[n].X

    def message_rows(k, step, n):
        if k >= 4:
            return corner_rows(levs[n], n == 1)
        return side_size(n, DIRS[k]) * len(side_pieces(levs[n], DIRS[k], n == 1, step))

    def copy(k, d, step, n):
        if k >= 4:
            s, r = scorner[n].at[step, k - 4], rcorner[n].at[step, k - 4]
        else:
            rows = pl.ds(0, message_rows(k, step, n))
            if step == 0:
                s, r = sside0[n].at[k, rows], rside0[n].at[k, rows]
            else:
                s, r = sside[n].at[step - 1, k, rows], rside[n].at[step - 1, k, rows]
        return pltpu.make_async_remote_copy(
            src_ref=s, dst_ref=r, send_sem=send_sem,
            recv_sem=recv_sem.at[n, step, int(k not in (2, 3))],
            device_id={"gx": ix + d[0], "gy": iy + d[1]}, device_id_type=MESH,
        )

    def wait_present(sem, which, rows_of_k, arriving):
        def options(i, n):
            low, high = i > 0, i < n - 1
            signs = (1, -1) if arriving else (-1, 1)
            return (
                (jnp.logical_and(low, high), (0, 1, -1)),
                (jnp.logical_and(low, jnp.logical_not(high)), (0, signs[0])),
                (jnp.logical_and(jnp.logical_not(low), high), (0, signs[1])),
            )

        along_x = options(ix, n_x) if any(DIRS[k][0] for k in which) else ((None, (0,)),)
        along_y = options(iy, n_y) if any(DIRS[k][1] for k in which) else ((None, (0,)),)
        for in_x, dxs in along_x:
            for in_y, dys in along_y:
                conds = [cond for cond in (in_x, in_y) if cond is not None]
                rows = sum(rows_of_k(k) for k in which if DIRS[k][0] in dxs and DIRS[k][1] in dys)

                @pl.when(functools.reduce(jnp.logical_and, conds))
                def _(rows=rows):
                    wait_rows(sem, rows)

    XS, YS, CS = (0, 1), (2, 3), (4, 5, 6, 7)

    def divergence(step, n, start, count, stride):
        lev, u, m = levs[n], U[n][step], M[n]
        SX, cs = lev.H * lev.R, lev.field_rows()
        get = lambda c, h, off: u[rows_of(start + c * cs + h * lev.R + off, count, stride), :]
        hi, lo = shifts([get(2, h, 0) for h in range(lev.H)])
        values = []
        for h in range(lev.H):
            v = 0.5 * ((get(0, h, SX) - get(0, h, -SX)) + (get(1, h, 1) - get(1, h, -1)))
            ic = m[rows_of(IC * cs + start + h * lev.R, count, stride), :]
            values.append(v + ic * (hi[h] - lo[h]))
        return values

    def lanes_of(rows):
        return lax.broadcasted_iota(jnp.int32, (rows, L), 1)

    def merged(values):
        total, ln = values[0], lanes_of(values[0].shape[0])
        for i, v in enumerate(values[1:], 1):
            total = jnp.where(ln == i, pltpu.roll(v, i, 1), total)
        return total

    def parted(value, i):
        return pltpu.roll(value, L - i, 1) if i else value

    def corner_row(lev, d, c, a, b, h, place):
        return pl.ds(lev.row(c, 2 + place(lev.X, d[0], a), h, 8 + place(lev.Y, d[1], b)), 1)

    def pack(step, n, which):
        lev, u, m = levs[n], U[n][step], M[n]
        for k in which:
            d = DIRS[k]
            if k >= 4:
                for c in range(2):
                    for h in range(lev.H):
                        scorner[n][step, k - 4, pl.ds(c * lev.H + h, 1), :] = u[
                            corner_row(lev, d, c, 1, 1, h, inner), :
                        ]
                if n:
                    extras = [u[corner_row(lev, d, c, a, b, 0, inner), :] for c, a, b in corner_extras(d)]
                    scorner[n][step, k - 4, pl.ds(2 * lev.H, 1), :] = merged(extras)
                continue
            size = side_size(n, d)
            parts = divergence(step, n, *line(lev, d, 1, 0, 0, inner))
            for at, (kind, c, h) in enumerate(side_pieces(lev, d, n == 1, step)):
                first_row, count, stride = line(lev, d, 1, h, c, inner)
                if kind == "u":
                    value = u[rows_of(first_row, count, stride), :]
                elif kind == "div":
                    value = parts[h]
                elif kind == "wide":
                    value = m[rows_of(WIDE * lev.field_rows() + first_row, count, stride), :]
                else:
                    value = merged([u[rows_of(*line(lev, d, 2, 0, e, inner)), :] for e in range(3)])
                if step == 0:
                    sside0[n][k, pl.ds(at * size, size), :] = value
                else:
                    sside[n][step - 1, k, pl.ds(at * size, size), :] = value

    def start(step, n, which):
        for k in which:
            @pl.when(has(DIRS[k]))
            def _(k=k):
                copy(k, DIRS[k], step, n).start()

    def unpack(step, n, which):
        lev, u, m = levs[n], U[n][step], M[n]
        fr = lev.field_rows()
        for g, group in enumerate((YS, XS + CS)):
            if group[0] in which:
                wait_present(recv_sem.at[n, step, g], group, lambda k: message_rows(k, step, n), True)

        for k in which:
            d = DIRS[k]
            back = (-d[0], -d[1])
            if k >= 4:
                for c in range(2):
                    for h in range(lev.H):
                        value = rcorner[n][step, k - 4, pl.ds(c * lev.H + h, 1), :]
                        u[corner_row(lev, d, c, 1, 1, h, outer), :] = value
                        if c == 0:
                            beside = lev.row(0, 2 + inner(lev.X, back[0], 1), h, 8 + outer(lev.Y, d[1], 1))
                            sign = back[0]
                        else:
                            beside = lev.row(0, 2 + outer(lev.X, d[0], 1), h, 8 + inner(lev.Y, back[1], 1))
                            sign = back[1]
                        at = pl.ds(DIV * fr + beside, 1)
                        m[at, :] = m[at, :] + (0.5 * sign) * value
                if n:
                    value = rcorner[n][step, k - 4, pl.ds(2 * lev.H, 1), :]
                    for i, (c, a, b) in enumerate(corner_extras(d)):
                        u[corner_row(lev, d, c, a, b, 0, outer), :] = parted(value, i)
                continue
            axis, size = (0 if d[0] else 1), side_size(n, d)
            half = jnp.where(has(back), 0.5 * (d[0] + d[1]), 0.0)
            for at, (kind, c, h) in enumerate(side_pieces(lev, d, n == 1, step)):
                rows = pl.ds(at * size, size)
                got = rside0[n][k, rows, :] if step == 0 else rside[n][step - 1, k, rows, :]
                first_row, count, stride = line(lev, d, 1, h, c, outer)
                if kind == "u":
                    u[rows_of(first_row, count, stride), :] = got
                elif kind == "div":
                    own = u[rows_of(*line(lev, back, 1, h, axis, inner)), :]
                    m[rows_of(DIV * fr + first_row, count, stride), :] = got + half * own
                elif kind == "wide":
                    m[rows_of(WIDE * fr + first_row, count, stride), :] = got
                else:
                    for e in range(3):
                        u[rows_of(*line(lev, d, 2, 0, e, outer)), :] = parted(got, e)

    loaded(0)
    take_in(1)
    pack(0, 1, XS + CS + YS)
    pl.semaphore_wait(barrier, greeted)
    start(0, 1, CS + XS + YS)
    loaded(1)
    load(3)
    load(2)
    take_in(0)
    pack(0, 0, XS + CS + YS)
    loaded(3)

    X, Y = lf.X, lf.Y
    YE = lc.Y + 3
    sub = lax.broadcasted_iota(jnp.int32, (8, Y), 0)
    lan = lax.broadcasted_iota(jnp.int32, (8, Y), 1)
    row8 = lax.broadcasted_iota(jnp.int32, (8, KG), 0)
    cell = lax.broadcasted_iota(jnp.int32, (8, KG), 1)
    near_y = jnp.where(row8 % 2 == 0, 0.75, 0.25)
    cell_x = cell // YE
    cell_y = cell - cell_x * YE - row8 // 2

    def weight(o_all, shift, near):
        return jnp.where(o_all == shift, near, 0.0) + jnp.where(o_all + 1 == shift, 1.0 - near, 0.0)

    for x in range(X):
        near_x = 0.75 if x % 2 == 0 else 0.25
        for b in range(lf.NB):
            both = []
            for axis in range(2):
                o_row = jnp.broadcast_to(offs[axis, pl.ds(x, 1), :], (8, Y))
                o_col = jnp.sum(jnp.where(lan == sub + 8 * b, o_row, 0).astype(jnp.float32), axis=1, keepdims=True)
                both.append(jnp.broadcast_to(o_col, (8, KG)).astype(jnp.int32))
            w = weight(both[0], cell_x - (x // 2 + 1), near_x) * weight(both[1], cell_y - (4 * b + 1), near_y)
            for part in range(3):
                wts[pl.ds(x * Y + 8 * b, 8), pl.ds(part * KG, KG)] = w.astype(jnp.bfloat16)

    start(0, 0, CS + XS + YS)
    loaded(2)

    for n, lev in enumerate(levs):
        m = M[n]

        @pl.loop(0, lev.X, unroll=4)
        def _(x, n=n, lev=lev, m=m):
            for b in range(lev.NB):
                def at(name, h):
                    return pl.ds(mrow(lev, name, x + 2, h, 8 + 8 * b), 8)

                vs = []
                for h in range(lev.H):
                    src = (x, pl.ds(8 * b, 8), pl.ds(h * L, L))
                    g, de, la, ri = met[n][src], den[n][src], lam[n][src], rig[n][src]
                    rden = 1.0 / de
                    ic = m[at(IC, h), :]
                    inv = ic * (1.0 / coef(lev, h, 8))
                    bb = (FACTOR * (la + ri)) * rden
                    m[at(A, h), :] = FACTOR * inv * rden
                    m[at(B5, h), :] = 0.5 * bb
                    m[at(BZ, h), :] = bb * ic
                    m[at(EN, h), :] = de * g
                    vs.append(ri * inv)
                hi, lo = shifts(vs)
                for h in range(lev.H):
                    m[at(FZP, h), :] = 0.5 * (vs[h] + hi[h])
                    m[at(FZM, h), :] = 0.5 * (vs[h] + lo[h])

    def faces_x(n, xs):
        lev, m = levs[n], M[n]
        for x in xs:
            for h in range(lev.H):
                for b in range(lev.NB):
                    r = 8 + 8 * b
                    w0 = m[pl.ds(mrow(lev, WIDE, x + 1, h, r), 8), :]
                    w1 = m[pl.ds(mrow(lev, WIDE, x + 2, h, r), 8), :]
                    m[pl.ds(mrow(lev, FX, x + 1, h, r), 8), :] = 0.5 * (w0 + w1)

    def faces_y(n):
        lev, m = levs[n], M[n]

        @pl.loop(0, lev.X, unroll=4)
        def _(x):
            for h in range(lev.H):
                for b in range(lev.NB + 1):
                    r = 8 + 8 * b
                    w0 = m[pl.ds(mrow(lev, WIDE, x + 2, h, r - 1), 8), :]
                    w1 = m[pl.ds(mrow(lev, WIDE, x + 2, h, r), 8), :]
                    m[pl.ds(mrow(lev, FY, x + 2, h, r), 8), :] = 0.5 * (w0 + w1)

    def divergences(step, n, xs):
        lev, m = levs[n], M[n]

        def column(x):
            for b in range(lev.NB):
                values = divergence(step, n, lev.row(0, x + 2, 0, 8 + 8 * b), 8, 1)
                for h in range(lev.H):
                    m[pl.ds(mrow(lev, DIV, x + 2, h, 8 + 8 * b), 8), :] = values[h]

        for x in xs:
            column(x)

    def ghosts(step):
        uc = U[1][step]
        for c in range(3):
            for x in range(lc.X + 3):
                for q in range(0, YE, 8):
                    plane[pl.ds(c * KG + x * YE + q, 8), :] = pltpu.roll(
                        uc[pl.ds(lc.row(c, x + 1, 0, 7 + q), 8), :], L - 1, 1
                    )
        for c in range(3):
            left, parts = plane[pl.ds(c * KG, KG), :], []
            for _ in range(3):
                parts.append(left.astype(jnp.bfloat16))
                left = left - parts[-1].astype(jnp.float32)
            ghost[pl.ds(c * lf.X * lf.Y, lf.X * lf.Y), :] = jnp.dot(
                wts[...], jnp.concatenate(parts, axis=0), preferred_element_type=jnp.float32
            )

    def top_ghost(step, x, c):
        uf = U[0][step]
        base = c * lf.Y
        for b in range(lf.NB):
            pair[pl.ds(base + 8 * b, 8), :] = (
                uf[pl.ds(lf.row(c, 2 * x + 2, 0, 8 + 8 * b), 8), :]
                + uf[pl.ds(lf.row(c, 2 * x + 3, 0, 8 + 8 * b), 8), :]
            )
        s = pair[pl.ds(base, 8, 2), :] + pair[pl.ds(base + 1, 8, 2), :]
        return pltpu.roll(0.25 * s, 1, 1)

    def update(step, n, columns, inside_x=None):
        lev = levs[n]
        u, m = U[n][step], M[n]
        SX = lev.H * lev.R
        H = lev.H

        def body(x, acc, comps=(0, 1, 2)):
            for b in range(lev.NB):
                r0 = 8 + 8 * b

                def mat(name, h, off=0):
                    return m[pl.ds(mrow(lev, name, x + 2, h, r0) + off, 8), :]

                dhi, dlo = shifts([mat(DIV, h) for h in range(H)]) if 2 in comps else (None, None)
                cells = [None] * H
                for c in comps:
                    get = lambda h, off=0, c=c: u[pl.ds(lev.row(c, x + 2, h, r0) + off, 8), :]
                    cur = [get(h) for h in range(H)]
                    hi, lo = shifts(cur)
                    if n == 0:
                        g = ghost[pl.ds(((c * lev.X + x) * lev.NB + b) * 8, 8), :]
                        hi[H - 1] = jnp.where(last, g, hi[H - 1])
                    else:
                        hi[H - 1] = jnp.where(last, 0.0, hi[H - 1])
                        lo[0] = jnp.where(first, top_ghost(step, x, c), lo[0])
                    for h in range(H):
                        v = cur[h]
                        flux = mat(FX, h) * (get(h, SX) - v) - mat(FX, h, -SX) * (v - get(h, -SX))
                        flux = flux + (mat(FY, h, 1) * (get(h, 1) - v) - mat(FY, h) * (v - get(h, -1)))
                        flux = flux + (mat(FZP, h) * (hi[h] - v) - mat(FZM, h) * (v - lo[h]))
                        if c == 0:
                            grad = mat(B5, h) * (mat(DIV, h, SX) - mat(DIV, h, -SX))
                        elif c == 1:
                            grad = mat(B5, h) * (mat(DIV, h, 1) - mat(DIV, h, -1))
                        else:
                            grad = mat(BZ, h) * (dhi[h] - dlo[h])
                        rate = mat(A, h) * flux + grad
                        if step == 0:
                            p = prev[n][c, x, pl.ds(8 * b, 8), pl.ds(h * L, L)]
                        else:
                            p = U[n][step - 1][pl.ds(lev.row(c, x + 2, h, r0), 8), :]
                        change = (v - p) + rate
                        new = v + change
                        if step == STEPS - 1:
                            out[n][c, x, pl.ds(8 * b, 8), pl.ds(h * L, L)] = new
                        else:
                            U[n][step + 1][pl.ds(lev.row(c, x + 2, h, r0), 8), :] = new
                        e = change * change - new * rate
                        cells[h] = e if cells[h] is None else cells[h] + e
                for h in range(H):
                    acc = acc + mat(EN, h) * cells[h]
            return acc

        acc = jnp.zeros((8, L), jnp.float32)
        for x, comps in columns:
            acc = body(x, acc, comps)
        if inside_x is not None:
            acc = lax.fori_loop(*inside_x, body, acc, unroll=4)
        row = pl.ds(4 * n + step, 1)
        es[row, :] = es[row, :] + jnp.sum(acc, axis=0, keepdims=True)

    es[...] = jnp.zeros((8, L), jnp.float32)
    ALL = (0, 1, 2)
    for n, lev in enumerate(levs):
        faces_x(n, range(1, lev.X))

    def coarse_start(step):
        unpack(step, 1, YS)
        if step == 0:
            faces_y(1)
        divergences(step, 1, range(1, lc.X - 1))
        update(step, 1, (), (2, lc.X - 2))

    def coarse_halo(step):
        unpack(step, 1, XS + CS)
        if step == 0:
            faces_x(1, (0, lc.X))
        divergences(step, 1, (0, lc.X - 1))

    for step in range(STEPS - 1):
        coarse_start(step)
        coarse_halo(step)
        update(step, 1, [(x, ALL) for x in (0, 1, lc.X - 2, lc.X - 1)])
        pack(step + 1, 1, CS + XS + YS)
        start(step + 1, 1, CS + XS + YS)
        ghosts(step)
        unpack(step, 0, YS + XS + CS)
        if step == 0:
            faces_y(0)
            faces_x(0, (0, X))
        divergences(step, 0, (0, 1, 2, X - 3, X - 2, X - 1))
        update(step, 0, [(0, ALL), (X - 1, ALL), (1, (0,)), (X - 2, (0,))])
        pack(step + 1, 0, XS + CS)
        start(step + 1, 0, CS + XS)
        divergences(step, 0, range(3, X - 3))
        update(step, 0, [(1, (1, 2)), (X - 2, (1, 2))], (2, X - 2))
        pack(step + 1, 0, YS)
        start(step + 1, 0, YS)
        if step < len(rings):
            if step:
                ready_wait(step - 1)
            ready_signal(step)
    step = STEPS - 1
    coarse_start(step)
    coarse_halo(step)
    update(step, 1, [(x, ALL) for x in (0, 1, lc.X - 2, lc.X - 1)])
    ghosts(step)
    unpack(step, 0, YS)
    divergences(step, 0, range(1, X - 1))
    update(step, 0, (), (2, X - 2))
    unpack(step, 0, XS + CS)
    divergences(step, 0, (0, X - 1))
    update(step, 0, [(x, ALL) for x in (0, 1, X - 2, X - 1)])
    for i in range(min(STEPS - 1, len(rings)) - 1, len(rings)):
        if i >= 0:
            ready_wait(i)
        if i + 1 < len(rings):
            ready_signal(i + 1)

    def share(o):
        to, x, y = place(o)
        return pltpu.make_async_remote_copy(
            src_ref=mine, dst_ref=box.at[pl.ds(me, 1)], send_sem=en_send, recv_sem=en_recv,
            device_id={"gx": x, "gy": y}, device_id_type=MESH,
        )

    def all_rows(sem):
        rows = box.at[pl.ds(0, everyone - 1)]
        return pltpu.make_async_copy(rows, rows, sem)

    sums = jnp.sum(es[...], axis=1, keepdims=True)
    diagonal = lane == lax.broadcasted_iota(jnp.int32, (8, L), 0)
    row = jnp.sum(jnp.where(diagonal, sums, 0.0), axis=0, keepdims=True)
    mine[...] = row

    if everyone > 64:
        @pl.loop(1, everyone)
        def _(o):
            share(o).start()
    else:
        for o in range(everyone - 1, 0, -1):
            share(o).start()

    box[pl.ds(me, 1), :] = row

    wait_present(
        send_sem, range(8),
        lambda k: sum(message_rows(k, step, n) for step in range(STEPS) for n in range(2)), False,
    )
    all_rows(en_send).wait()
    all_rows(en_recv).wait()
    total = jnp.sum(box[...], axis=0, keepdims=True)
    for n, lev in enumerate(levs):
        cells = lev.X * n_x * lev.Y * n_y * lev.H * L
        eo[pl.ds(n, 1), :] = total[:, 4 * n : 4 * n + STEPS] / cells


def ready_rings(n_x, n_y):
    rings, reach = [], 2
    while reach < max(n_x, n_y) - 1:
        xs = (-reach, 0, reach) if reach < n_x - 1 else (0,)
        ys = (-reach, 0, reach) if reach < n_y - 1 else (0,)
        rings.append([(x, y) for x in xs for y in ys if x or y])
        reach *= 2
    return rings


def write_out(a, b, c, fine, coarse, energy, sem):
    copies = [
        pltpu.make_async_copy(src, dst, sem.at[i])
        for i, (src, dst) in enumerate(((a, fine), (b, coarse), (c, energy)))
    ]
    for copy in copies:
        copy.start()
    for copy in copies:
        copy.wait()


def plane_rows(lc):
    return -(-(lc.X + 3) * (lc.Y + 3) // L) * L


def side_rows(lev, coarse):
    longer = max(lev.X, lev.Y)
    return [longer * len(side_pieces(lev, (-1, 0), coarse, step)) for step in (1, 0)]


def solution(mesh):
    n_x, n_y = mesh.shape["gx"], mesh.shape["gy"]

    def step(*args):
        lf, lc = Level(args[0].shape), Level(args[2].shape)
        sizes = [side_rows(lf, False), side_rows(lc, True)]
        corners = [corner_rows(lf, False), corner_rows(lc, True)]
        f32 = jnp.float32
        vm = lambda *s: pltpu.VMEM(s, f32)
        results = pl.pallas_call(
            functools.partial(kernel, n_x, n_y, lf, lc),
            out_shape=(
                vm(*args[0].shape),
                vm(*args[2].shape),
                vm(2, STEPS),
            ),
            in_specs=[pl.BlockSpec(memory_space=pl.ANY)] * len(args),
            out_specs=[pl.BlockSpec(memory_space=pltpu.VMEM)] * 3,
            scratch_shapes=(
                [pltpu.VMEM(a.shape, a.dtype) for a in args]
                + [vm(3 * lf.field_rows(), L)] * 3
                + [vm(3 * lc.field_rows(), L)] * 3
                + [
                    vm(11 * lf.field_rows(), L),
                    vm(11 * lc.field_rows(), L),
                    vm(3 * plane_rows(lc) + 8, L),
                    vm(3 * lf.Y, L),
                    pltpu.VMEM((lf.X * lf.Y, 3 * plane_rows(lc)), jnp.bfloat16),
                    vm(3 * lf.X * lf.Y, L),
                ]
                + [vm(4, size[1], L) for size in sizes] * 2
                + [vm(STEPS - 1, 4, size[0], L) for size in sizes] * 2
                + [vm(STEPS, 4, corner, L) for corner in corners] * 2
                + [
                    vm(8, L),
                    vm(1, L),
                    vm(n_x * n_y, L),
                    pltpu.SemaphoreType.DMA((4,)),
                    pltpu.SemaphoreType.DMA,
                    pltpu.SemaphoreType.DMA((2, STEPS, 2)),
                    pltpu.SemaphoreType.DMA,
                    pltpu.SemaphoreType.DMA,
                    pltpu.SemaphoreType.REGULAR((max(1, len(ready_rings(n_x, n_y))),)),
                ]
            ),
            compiler_params=pltpu.CompilerParams(
                collective_id=0, has_side_effects=True, vmem_limit_bytes=60 * 1024 * 1024
            ),
        )(*args)
        results = [pltpu.with_memory_space_constraint(r, pltpu.VMEM) for r in results]
        fine, coarse, energy = pl.pallas_call(
            write_out,
            out_shape=tuple(jax.ShapeDtypeStruct(r.shape, f32) for r in results),
            in_specs=[pl.BlockSpec(memory_space=pltpu.VMEM)] * 3,
            out_specs=[pl.BlockSpec(memory_space=pl.ANY)] * 3,
            scratch_shapes=[pltpu.SemaphoreType.DMA((3,))],
        )(*results)
        return fine, coarse, energy.T

    field, cells = P(None, "gx", "gy", None), P("gx", "gy", None)
    return jax.shard_map(
        step,
        mesh=mesh,
        in_specs=(field,) * 4 + (cells,) * 8 + (P(None, "gx", "gy"),),
        out_specs=(field, field, P()),
        check_vma=False,
    )
```

```python
import functools

import jax
import jax.numpy as jnp
from jax import lax
from jax.experimental import pallas as pl
from jax.experimental.pallas import tpu as pltpu
from jax.sharding import PartitionSpec as P

STEPS = 3
FACTOR = 0.15
MESH = pl.DeviceIdType.MESH
L = 128
SIDES = ((1, 0), (-1, 0), (0, 1), (0, -1))
CORNERS = ((1, 1), (1, -1), (-1, 1), (-1, -1))


class Level:
    def __init__(self, shape):
        _, self.X, self.Y, Z = shape
        self.H = Z // L
        self.XE = self.X + 4
        self.R = self.Y + 16
        while (self.H * self.R) % 8 != 4:
            self.R += 1
        self.NB = self.Y // 8

    def row(self, c, x, h, r):
        return ((c * self.XE + x) * self.H + h) * self.R + r

    def field_rows(self):
        return self.XE * self.H * self.R


def side_pieces(lev, d, coarse, step):
    out = [("u", c, h) for c in range(3) for h in range(lev.H)]
    out += [("div", 0, h) for h in range(lev.H)]
    if step == 0:
        out += [("wide", 0, h) for h in range(lev.H)]
    if coarse and d[0] + d[1] < 0:
        out += [("plane", 0, 0)]
    return out


def corner_extras(d):
    rings = [(a, b) for a in ((1, 2) if d[0] < 0 else (1,)) for b in ((1, 2) if d[1] < 0 else (1,))]
    return [(2, 1, 1)] + [(c, a, b) for a, b in rings if (a, b) != (1, 1) for c in range(3)]


def corner_rows(lev, coarse):
    return 2 * lev.H + int(coarse)


def inner(length, d, ring):
    return length - ring if d > 0 else ring - 1


def outer(length, d, ring):
    return -ring if d > 0 else length + ring - 1


def line(lev, d, ring, h, c, place):
    if d[0]:
        return lev.row(c, 2 + place(lev.X, d[0], ring), h, 8), lev.Y, 1
    return lev.row(c, 2, h, 8 + place(lev.Y, d[1], ring)), lev.X, lev.H * lev.R


def rows_of(start, count, stride):
    return pl.ds(start, count) if stride == 1 else pl.ds(start, count, stride)


def kernel(n_x, n_y, lf, lc, *refs):
    given, (fo, co, eo) = refs[:13], refs[13:16]
    held = refs[16:29]
    (fd, fp, cd, cp, fden, flam, frig, fmet, cden, clam, crig, cmet, offs) = held
    (uf0, uf1, uf2, uc0, uc1, uc2, mf, mc, plane, pair, wts, ghost,
     ss0f, ss0c, rs0f, rs0c, ssf, ssc, rsf, rsc, scf, scc, rcf, rcc,
     es, mine, box, load_sem, send_sem, recv_sem, en_send, en_recv, inside) = refs[29:]
    U = ((uf0, uf1, uf2), (uc0, uc1, uc2))
    M = (mf, mc)
    levs = (lf, lc)
    sside0, rside0, sside, rside = (ss0f, ss0c), (rs0f, rs0c), (ssf, ssc), (rsf, rsc)
    scorner, rcorner = (scf, scc), (rcf, rcc)
    disp, prev, out = (fd, cd), (fp, cp), (fo, co)
    den, lam, rig, met = (fden, cden), (flam, clam), (frig, crig), (fmet, cmet)
    ix, iy = lax.axis_index("gx"), lax.axis_index("gy")

    def has(d):
        conds = []
        if d[0] > 0:
            conds.append(ix < n_x - 1)
        if d[0] < 0:
            conds.append(ix > 0)
        if d[1] > 0:
            conds.append(iy < n_y - 1)
        if d[1] < 0:
            conds.append(iy > 0)
        return functools.reduce(jnp.logical_and, conds)

    DIRS = SIDES + CORNERS
    KG = plane_rows(lc)
    lane = lax.broadcasted_iota(jnp.int32, (8, L), 1)
    first, last = lane == 0, lane == L - 1

    IC, WIDE, FX, FY, FZP, FZM, A, B5, BZ, EN, DIV = range(11)

    def mrow(lev, name, x, h, r):
        return name * lev.field_rows() + (x * lev.H + h) * lev.R + r

    barrier = pltpu.get_barrier_semaphore()

    def signal(x, y):
        pl.semaphore_signal(barrier, inc=1, device_id={"gx": x, "gy": y}, device_id_type=MESH)

    everyone = n_x * n_y
    me = ix * n_y + iy

    greeted = jnp.int32(0)
    for d in DIRS:
        greeted = greeted + has(d).astype(jnp.int32)

        @pl.when(has(d))
        def _(d=d):
            signal(ix + d[0], iy + d[1])

    rings = ready_rings(n_x, n_y)

    def within(d):
        x, y = ix + d[0], iy + d[1]
        return (x >= 0) & (x < n_x) & (y >= 0) & (y < n_y)

    def ready_signal(i):
        for d in rings[i]:
            @pl.when(within(d))
            def _(d=d):
                pl.semaphore_signal(
                    inside.at[i], inc=1, device_id={"gx": ix + d[0], "gy": iy + d[1]}, device_id_type=MESH
                )

    def ready_wait(i):
        pl.semaphore_wait(inside.at[i], sum(within(d).astype(jnp.int32) for d in rings[i]))

    def coef(lev, h, rows):
        ln = lax.broadcasted_iota(jnp.int32, (rows, L), 1)
        value = jnp.full((rows, L), 0.5, jnp.float32)
        if h == 0:
            value = jnp.where(ln == 0, 1.0, value)
        if h == lev.H - 1:
            value = jnp.where(ln == L - 1, 1.0, value)
        return value

    def shifts(vals):
        n = len(vals)
        ups = [pltpu.roll(v, L - 1, 1) for v in vals]
        dns = [pltpu.roll(v, 1, 1) for v in vals]
        lane_v = lane if vals[0].shape[0] == 8 else lax.broadcasted_iota(jnp.int32, vals[0].shape, 1)
        fst, lst = lane_v == 0, lane_v == L - 1
        hi = [jnp.where(lst, ups[i + 1] if i + 1 < n else vals[i], ups[i]) for i in range(n)]
        lo = [jnp.where(fst, dns[i - 1] if i > 0 else vals[i], dns[i]) for i in range(n)]
        return hi, lo

    LOADS = ((2, 11, 10), (0, 7, 6), (1, 3, 4, 5, 8, 9), (12,))

    def load(group):
        for i in LOADS[group]:
            pltpu.make_async_copy(given[i], held[i], load_sem.at[group]).start()

    def wait_rows(sem, rows):
        span = mf.at[pl.ds(0, rows)]
        pltpu.make_async_copy(span, span, sem).wait()

    def loaded(group):
        if group == 3:
            pltpu.make_async_copy(given[12], held[12], load_sem.at[3]).wait()
        else:
            wait_rows(load_sem.at[group], sum(given[i].size // L for i in LOADS[group]))

    load(0)
    load(1)

    zero = jnp.zeros((8, L), jnp.float32)
    for lev, us, m in zip(levs, U, M):
        lines = lev.XE * lev.H

        @pl.loop(0, 3 * lines, unroll=4)
        def _(q, lev=lev, us=us):
            for u in us:
                u[pl.ds(q * lev.R, 8), :] = zero
                u[pl.ds(q * lev.R + lev.Y + 8, 8), :] = zero

        @pl.loop(0, lines, unroll=4)
        def _(q, lev=lev, m=m):
            for name in (WIDE, DIV):
                m[pl.ds(name * lev.field_rows() + q * lev.R, 8), :] = zero
                m[pl.ds(name * lev.field_rows() + q * lev.R + lev.Y + 8, 8), :] = zero

        for x in (0, 1, lev.X + 2, lev.X + 3):
            for h in range(lev.H):
                for b in range(lev.NB):
                    for u in us:
                        for c in range(3):
                            u[pl.ds(lev.row(c, x, h, 8 + 8 * b), 8), :] = zero
                    for name in (WIDE, DIV):
                        m[pl.ds(mrow(lev, name, x, h, 8 + 8 * b), 8), :] = zero

    @pl.loop(0, 3 * KG // 8, unroll=4)
    def _(q):
        plane[pl.ds(8 * q, 8), :] = zero

    plane[pl.ds(3 * KG, 8), :] = zero
    for k, d in enumerate(DIRS):
        @pl.when(jnp.logical_not(has((-d[0], -d[1]))))
        def _(k=k):
            for n in range(2):
                for step in range(STEPS):
                    if k >= 4:
                        rcorner[n][step, k - 4, :, :] = jnp.zeros(rcorner[n].shape[2:], jnp.float32)
                    elif step == 0:
                        rside0[n][k, :, :] = jnp.zeros(rside0[n].shape[1:], jnp.float32)
                    else:
                        rside[n][step - 1, k, :, :] = jnp.zeros(rside[n].shape[2:], jnp.float32)

    def take_in(n):
        lev, us, u_in, m = levs[n], U[n], disp[n], M[n]

        @pl.loop(0, lev.X, unroll=4)
        def _(x):
            for h in range(lev.H):
                for b in range(lev.NB):
                    src = (x, pl.ds(8 * b, 8), pl.ds(h * L, L))
                    g = met[n][src]
                    m[pl.ds(mrow(lev, IC, x + 2, h, 8 + 8 * b), 8), :] = (1.0 / g) * coef(lev, h, 8)
                    m[pl.ds(mrow(lev, WIDE, x + 2, h, 8 + 8 * b), 8), :] = rig[n][src] * g
                    for c in range(3):
                        us[0][pl.ds(lev.row(c, x + 2, h, 8 + 8 * b), 8), :] = u_in[(c,) + src]

    def side_size(n, d):
        return levs[n].Y if d[0] else levs[n].X

    def message_rows(k, step, n):
        if k >= 4:
            return corner_rows(levs[n], n == 1)
        return side_size(n, DIRS[k]) * len(side_pieces(levs[n], DIRS[k], n == 1, step))

    def copy(k, d, step, n):
        if k >= 4:
            s, r = scorner[n].at[step, k - 4], rcorner[n].at[step, k - 4]
        else:
            rows = pl.ds(0, message_rows(k, step, n))
            if step == 0:
                s, r = sside0[n].at[k, rows], rside0[n].at[k, rows]
            else:
                s, r = sside[n].at[step - 1, k, rows], rside[n].at[step - 1, k, rows]
        return pltpu.make_async_remote_copy(
            src_ref=s, dst_ref=r, send_sem=send_sem,
            recv_sem=recv_sem.at[n, step, int(k not in (2, 3))],
            device_id={"gx": ix + d[0], "gy": iy + d[1]}, device_id_type=MESH,
        )

    def wait_present(sem, which, rows_of_k, arriving):
        def options(i, n):
            low, high = i > 0, i < n - 1
            signs = (1, -1) if arriving else (-1, 1)
            return (
                (jnp.logical_and(low, high), (0, 1, -1)),
                (jnp.logical_and(low, jnp.logical_not(high)), (0, signs[0])),
                (jnp.logical_and(jnp.logical_not(low), high), (0, signs[1])),
            )

        along_x = options(ix, n_x) if any(DIRS[k][0] for k in which) else ((None, (0,)),)
        along_y = options(iy, n_y) if any(DIRS[k][1] for k in which) else ((None, (0,)),)
        for in_x, dxs in along_x:
            for in_y, dys in along_y:
                conds = [cond for cond in (in_x, in_y) if cond is not None]
                rows = sum(rows_of_k(k) for k in which if DIRS[k][0] in dxs and DIRS[k][1] in dys)

                @pl.when(functools.reduce(jnp.logical_and, conds))
                def _(rows=rows):
                    wait_rows(sem, rows)

    XS, YS, CS = (0, 1), (2, 3), (4, 5, 6, 7)

    def divergence(step, n, start, count, stride):
        lev, u, m = levs[n], U[n][step], M[n]
        SX, cs = lev.H * lev.R, lev.field_rows()
        get = lambda c, h, off: u[rows_of(start + c * cs + h * lev.R + off, count, stride), :]
        hi, lo = shifts([get(2, h, 0) for h in range(lev.H)])
        values = []
        for h in range(lev.H):
            v = 0.5 * ((get(0, h, SX) - get(0, h, -SX)) + (get(1, h, 1) - get(1, h, -1)))
            ic = m[rows_of(IC * cs + start + h * lev.R, count, stride), :]
            values.append(v + ic * (hi[h] - lo[h]))
        return values

    def lanes_of(rows):
        return lax.broadcasted_iota(jnp.int32, (rows, L), 1)

    def merged(values):
        total, ln = values[0], lanes_of(values[0].shape[0])
        for i, v in enumerate(values[1:], 1):
            total = jnp.where(ln == i, pltpu.roll(v, i, 1), total)
        return total

    def parted(value, i):
        return pltpu.roll(value, L - i, 1) if i else value

    def corner_row(lev, d, c, a, b, h, place):
        return pl.ds(lev.row(c, 2 + place(lev.X, d[0], a), h, 8 + place(lev.Y, d[1], b)), 1)

    def pack(step, n, which):
        lev, u, m = levs[n], U[n][step], M[n]
        for k in which:
            d = DIRS[k]
            if k >= 4:
                for c in range(2):
                    for h in range(lev.H):
                        scorner[n][step, k - 4, pl.ds(c * lev.H + h, 1), :] = u[
                            corner_row(lev, d, c, 1, 1, h, inner), :
                        ]
                if n:
                    extras = [u[corner_row(lev, d, c, a, b, 0, inner), :] for c, a, b in corner_extras(d)]
                    scorner[n][step, k - 4, pl.ds(2 * lev.H, 1), :] = merged(extras)
                continue
            size = side_size(n, d)
            parts = divergence(step, n, *line(lev, d, 1, 0, 0, inner))
            for at, (kind, c, h) in enumerate(side_pieces(lev, d, n == 1, step)):
                first_row, count, stride = line(lev, d, 1, h, c, inner)
                if kind == "u":
                    value = u[rows_of(first_row, count, stride), :]
                elif kind == "div":
                    value = parts[h]
                elif kind == "wide":
                    value = m[rows_of(WIDE * lev.field_rows() + first_row, count, stride), :]
                else:
                    value = merged([u[rows_of(*line(lev, d, 2, 0, e, inner)), :] for e in range(3)])
                if step == 0:
                    sside0[n][k, pl.ds(at * size, size), :] = value
                else:
                    sside[n][step - 1, k, pl.ds(at * size, size), :] = value

    def start(step, n, which):
        for k in which:
            @pl.when(has(DIRS[k]))
            def _(k=k):
                copy(k, DIRS[k], step, n).start()

    def unpack(step, n, which):
        lev, u, m = levs[n], U[n][step], M[n]
        fr = lev.field_rows()
        for g, group in enumerate((YS, XS + CS)):
            if group[0] in which:
                wait_present(recv_sem.at[n, step, g], group, lambda k: message_rows(k, step, n), True)

        for k in which:
            d = DIRS[k]
            back = (-d[0], -d[1])
            if k >= 4:
                for c in range(2):
                    for h in range(lev.H):
                        value = rcorner[n][step, k - 4, pl.ds(c * lev.H + h, 1), :]
                        u[corner_row(lev, d, c, 1, 1, h, outer), :] = value
                        if c == 0:
                            beside = lev.row(0, 2 + inner(lev.X, back[0], 1), h, 8 + outer(lev.Y, d[1], 1))
                            sign = back[0]
                        else:
                            beside = lev.row(0, 2 + outer(lev.X, d[0], 1), h, 8 + inner(lev.Y, back[1], 1))
                            sign = back[1]
                        at = pl.ds(DIV * fr + beside, 1)
                        m[at, :] = m[at, :] + (0.5 * sign) * value
                if n:
                    value = rcorner[n][step, k - 4, pl.ds(2 * lev.H, 1), :]
                    for i, (c, a, b) in enumerate(corner_extras(d)):
                        u[corner_row(lev, d, c, a, b, 0, outer), :] = parted(value, i)
                continue
            axis, size = (0 if d[0] else 1), side_size(n, d)
            half = jnp.where(has(back), 0.5 * (d[0] + d[1]), 0.0)
            for at, (kind, c, h) in enumerate(side_pieces(lev, d, n == 1, step)):
                rows = pl.ds(at * size, size)
                got = rside0[n][k, rows, :] if step == 0 else rside[n][step - 1, k, rows, :]
                first_row, count, stride = line(lev, d, 1, h, c, outer)
                if kind == "u":
                    u[rows_of(first_row, count, stride), :] = got
                elif kind == "div":
                    own = u[rows_of(*line(lev, back, 1, h, axis, inner)), :]
                    m[rows_of(DIV * fr + first_row, count, stride), :] = got + half * own
                elif kind == "wide":
                    m[rows_of(WIDE * fr + first_row, count, stride), :] = got
                else:
                    for e in range(3):
                        u[rows_of(*line(lev, d, 2, 0, e, outer)), :] = parted(got, e)

    loaded(0)
    take_in(1)
    pack(0, 1, XS + CS + YS)
    pl.semaphore_wait(barrier, greeted)
    start(0, 1, CS + XS + YS)
    loaded(1)
    load(3)
    load(2)
    take_in(0)
    pack(0, 0, XS + CS + YS)
    loaded(3)

    X, Y = lf.X, lf.Y
    YE = lc.Y + 3
    sub = lax.broadcasted_iota(jnp.int32, (8, Y), 0)
    lan = lax.broadcasted_iota(jnp.int32, (8, Y), 1)
    row8 = lax.broadcasted_iota(jnp.int32, (8, KG), 0)
    cell = lax.broadcasted_iota(jnp.int32, (8, KG), 1)
    near_y = jnp.where(row8 % 2 == 0, 0.75, 0.25)
    cell_x = cell // YE
    cell_y = cell - cell_x * YE - row8 // 2

    def weight(o_all, shift, near):
        return jnp.where(o_all == shift, near, 0.0) + jnp.where(o_all + 1 == shift, 1.0 - near, 0.0)

    for x in range(X):
        near_x = 0.75 if x % 2 == 0 else 0.25
        for b in range(lf.NB):
            both = []
            for axis in range(2):
                o_row = jnp.broadcast_to(offs[axis, pl.ds(x, 1), :], (8, Y))
                o_col = jnp.sum(jnp.where(lan == sub + 8 * b, o_row, 0).astype(jnp.float32), axis=1, keepdims=True)
                both.append(jnp.broadcast_to(o_col, (8, KG)).astype(jnp.int32))
            w = weight(both[0], cell_x - (x // 2 + 1), near_x) * weight(both[1], cell_y - (4 * b + 1), near_y)
            for part in range(3):
                wts[pl.ds(x * Y + 8 * b, 8), pl.ds(part * KG, KG)] = w.astype(jnp.bfloat16)

    loaded(2)

    for n, lev in enumerate(levs):
        m = M[n]

        @pl.loop(0, lev.X, unroll=4)
        def _(x, n=n, lev=lev, m=m):
            for b in range(lev.NB):
                def at(name, h):
                    return pl.ds(mrow(lev, name, x + 2, h, 8 + 8 * b), 8)

                vs = []
                for h in range(lev.H):
                    src = (x, pl.ds(8 * b, 8), pl.ds(h * L, L))
                    g, de, la, ri = met[n][src], den[n][src], lam[n][src], rig[n][src]
                    rden = 1.0 / de
                    ic = m[at(IC, h), :]
                    inv = ic * (1.0 / coef(lev, h, 8))
                    bb = (FACTOR * (la + ri)) * rden
                    m[at(A, h), :] = FACTOR * inv * rden
                    m[at(B5, h), :] = 0.5 * bb
                    m[at(BZ, h), :] = bb * ic
                    m[at(EN, h), :] = de * g
                    vs.append(ri * inv)
                hi, lo = shifts(vs)
                for h in range(lev.H):
                    m[at(FZP, h), :] = 0.5 * (vs[h] + hi[h])
                    m[at(FZM, h), :] = 0.5 * (vs[h] + lo[h])

    def faces_x(n, xs):
        lev, m = levs[n], M[n]
        for x in xs:
            for h in range(lev.H):
                for b in range(lev.NB):
                    r = 8 + 8 * b
                    w0 = m[pl.ds(mrow(lev, WIDE, x + 1, h, r), 8), :]
                    w1 = m[pl.ds(mrow(lev, WIDE, x + 2, h, r), 8), :]
                    m[pl.ds(mrow(lev, FX, x + 1, h, r), 8), :] = 0.5 * (w0 + w1)

    def faces_y(n):
        lev, m = levs[n], M[n]

        @pl.loop(0, lev.X, unroll=4)
        def _(x):
            for h in range(lev.H):
                for b in range(lev.NB + 1):
                    r = 8 + 8 * b
                    w0 = m[pl.ds(mrow(lev, WIDE, x + 2, h, r - 1), 8), :]
                    w1 = m[pl.ds(mrow(lev, WIDE, x + 2, h, r), 8), :]
                    m[pl.ds(mrow(lev, FY, x + 2, h, r), 8), :] = 0.5 * (w0 + w1)

    def divergences(step, n, xs):
        lev, m = levs[n], M[n]

        def column(x):
            for b in range(lev.NB):
                values = divergence(step, n, lev.row(0, x + 2, 0, 8 + 8 * b), 8, 1)
                for h in range(lev.H):
                    m[pl.ds(mrow(lev, DIV, x + 2, h, 8 + 8 * b), 8), :] = values[h]

        for x in xs:
            column(x)

    def ghosts(step, late=False):
        uc = U[1][step]
        for c in range(3):
            for x in (0, lc.X + 1, lc.X + 2) if late else range(1, lc.X + 1):
                for q in range(0, YE, 8):
                    count = min(8, YE - q)
                    value = pltpu.roll(uc[pl.ds(lc.row(c, x + 1, 0, 7 + q), 8), :], L - 1, 1)
                    plane[pl.ds(c * KG + x * YE + q, count), :] = value[:count]
        for c in range(3):
            left, parts = plane[pl.ds(c * KG, KG), :], []
            for _ in range(3):
                parts.append(left.astype(jnp.bfloat16))
                left = left - parts[-1].astype(jnp.float32)
            whole = jnp.concatenate(parts, axis=0)
            for x, count in ((0, 2), (X - 4, 4)) if late else ((2, X - 6),):
                ghost[pl.ds((c * X + x) * Y, count * Y), :] = jnp.dot(
                    wts[pl.ds(x * Y, count * Y), :], whole, preferred_element_type=jnp.float32
                )

    def top_ghost(step, x, c):
        uf = U[0][step]
        base = c * lf.Y
        for b in range(lf.NB):
            pair[pl.ds(base + 8 * b, 8), :] = (
                uf[pl.ds(lf.row(c, 2 * x + 2, 0, 8 + 8 * b), 8), :]
                + uf[pl.ds(lf.row(c, 2 * x + 3, 0, 8 + 8 * b), 8), :]
            )
        s = pair[pl.ds(base, 8, 2), :] + pair[pl.ds(base + 1, 8, 2), :]
        return pltpu.roll(0.25 * s, 1, 1)

    def update(step, n, columns, inside_x=None):
        lev = levs[n]
        u, m = U[n][step], M[n]
        SX = lev.H * lev.R
        H = lev.H

        def body(x, acc, comps=(0, 1, 2)):
            for b in range(lev.NB):
                r0 = 8 + 8 * b

                def mat(name, h, off=0):
                    return m[pl.ds(mrow(lev, name, x + 2, h, r0) + off, 8), :]

                dhi, dlo = shifts([mat(DIV, h) for h in range(H)]) if 2 in comps else (None, None)
                fxp, fxm = [mat(FX, h) for h in range(H)], [mat(FX, h, -SX) for h in range(H)]
                fyp, fym = [mat(FY, h, 1) for h in range(H)], [mat(FY, h) for h in range(H)]
                fzp, fzm = [mat(FZP, h) for h in range(H)], [mat(FZM, h) for h in range(H)]
                scale = [mat(A, h) for h in range(H)]
                cells = [None] * H
                for c in comps:
                    get = lambda h, off=0, c=c: u[pl.ds(lev.row(c, x + 2, h, r0) + off, 8), :]
                    cur = [get(h) for h in range(H)]
                    hi, lo = shifts(cur)
                    if n == 0:
                        g = ghost[pl.ds(((c * lev.X + x) * lev.NB + b) * 8, 8), :]
                        hi[H - 1] = jnp.where(last, g, hi[H - 1])
                    else:
                        hi[H - 1] = jnp.where(last, 0.0, hi[H - 1])
                        lo[0] = jnp.where(first, top_ghost(step, x, c), lo[0])
                    for h in range(H):
                        v = cur[h]
                        flux = fxp[h] * (get(h, SX) - v) - fxm[h] * (v - get(h, -SX))
                        flux = flux + (fyp[h] * (get(h, 1) - v) - fym[h] * (v - get(h, -1)))
                        flux = flux + (fzp[h] * (hi[h] - v) - fzm[h] * (v - lo[h]))
                        if c == 0:
                            grad = mat(B5, h) * (mat(DIV, h, SX) - mat(DIV, h, -SX))
                        elif c == 1:
                            grad = mat(B5, h) * (mat(DIV, h, 1) - mat(DIV, h, -1))
                        else:
                            grad = mat(BZ, h) * (dhi[h] - dlo[h])
                        rate = scale[h] * flux + grad
                        if step == 0:
                            p = prev[n][c, x, pl.ds(8 * b, 8), pl.ds(h * L, L)]
                        else:
                            p = U[n][step - 1][pl.ds(lev.row(c, x + 2, h, r0), 8), :]
                        change = (v - p) + rate
                        new = v + change
                        if step == STEPS - 1:
                            out[n][c, x, pl.ds(8 * b, 8), pl.ds(h * L, L)] = new
                        else:
                            U[n][step + 1][pl.ds(lev.row(c, x + 2, h, r0), 8), :] = new
                        e = change * change - new * rate
                        cells[h] = e if cells[h] is None else cells[h] + e
                for h in range(H):
                    acc = acc + mat(EN, h) * cells[h]
            return acc

        acc = jnp.zeros((8, L), jnp.float32)
        for x, comps in columns:
            acc = body(x, acc, comps)
        if inside_x is not None:
            acc = lax.fori_loop(*inside_x, body, acc, unroll=4)
        row = pl.ds(4 * n + step, 1)
        es[row, :] = es[row, :] + jnp.sum(acc, axis=0, keepdims=True)

    es[...] = jnp.zeros((8, L), jnp.float32)
    start(0, 0, CS + XS + YS)
    ALL = (0, 1, 2)
    for n, lev in enumerate(levs):
        faces_x(n, range(1, lev.X))

    def coarse_start(step):
        unpack(step, 1, YS)
        if step == 0:
            faces_y(1)
        divergences(step, 1, range(1, lc.X - 1))
        update(step, 1, (), (2, lc.X - 2))

    def coarse_halo(step):
        unpack(step, 1, XS + CS)
        if step == 0:
            faces_x(1, (0, lc.X))
        divergences(step, 1, (0, lc.X - 1))

    for step in range(STEPS - 1):
        coarse_start(step)
        ghosts(step)
        coarse_halo(step)
        for far in (1, -1):
            @pl.when(lax.rem(ix, 2) == (1 if far > 0 else 0))
            def _(far=far, step=step):
                low, high = (0, 1), (lc.X - 2, lc.X - 1)
                for xs, side in (((high, 1), (low, -1)) if far > 0 else ((low, -1), (high, 1))):
                    update(step, 1, [(x, ALL) for x in xs])
                    which = [k for k in CS + XS if DIRS[k][0] == side]
                    pack(step + 1, 1, which)
                    start(step + 1, 1, which)

        pack(step + 1, 1, YS)
        start(step + 1, 1, YS)
        ghosts(step, True)
        unpack(step, 0, YS + XS + CS)
        if step == 0:
            faces_y(0)
            faces_x(0, (0, X))
        divergences(step, 0, (0, 1, 2, X - 3, X - 2, X - 1))
        update(step, 0, [(0, ALL), (X - 1, ALL), (1, (0,)), (X - 2, (0,))])
        pack(step + 1, 0, XS + CS)
        start(step + 1, 0, CS + XS)
        divergences(step, 0, range(3, X - 3))
        update(step, 0, [(1, (1, 2)), (X - 2, (1, 2))], (2, X - 2))
        pack(step + 1, 0, YS)
        start(step + 1, 0, YS)
        if step < len(rings):
            if step:
                ready_wait(step - 1)
            ready_signal(step)
    step = STEPS - 1
    coarse_start(step)
    ghosts(step)
    coarse_halo(step)
    update(step, 1, [(x, ALL) for x in (0, 1, lc.X - 2, lc.X - 1)])
    ghosts(step, True)
    unpack(step, 0, YS)
    divergences(step, 0, range(1, X - 1))
    update(step, 0, (), (2, X - 2))
    unpack(step, 0, XS + CS)
    divergences(step, 0, (0, X - 1))
    update(step, 0, [(x, ALL) for x in (0, 1, X - 2, X - 1)])
    for i in range(min(STEPS - 1, len(rings)) - 1, len(rings)):
        if i >= 0:
            ready_wait(i)
        if i + 1 < len(rings):
            ready_signal(i + 1)

    def share(x, y):
        return pltpu.make_async_remote_copy(
            src_ref=mine, dst_ref=box.at[pl.ds(me, 1)], send_sem=en_send, recv_sem=en_recv,
            device_id={"gx": x, "gy": y}, device_id_type=MESH,
        )

    def all_rows(sem):
        rows = box.at[pl.ds(0, everyone - 1)]
        return pltpu.make_async_copy(rows, rows, sem)

    sums = jnp.sum(es[...], axis=1, keepdims=True)
    diagonal = lane == lax.broadcasted_iota(jnp.int32, (8, L), 0)
    row = jnp.sum(jnp.where(diagonal, sums, 0.0), axis=0, keepdims=True)
    mine[...] = row

    def share_to(to):
        @pl.when(to != me)
        def _():
            share(lax.div(to, n_y), lax.rem(to, n_y)).start()

    if everyone > 64:
        pl.loop(0, everyone)(share_to)
    else:
        for to in range(everyone):
            share_to(jnp.int32(to))

    box[pl.ds(me, 1), :] = row

    wait_present(
        send_sem, range(8),
        lambda k: sum(message_rows(k, step, n) for step in range(STEPS) for n in range(2)), False,
    )
    all_rows(en_send).wait()
    all_rows(en_recv).wait()
    total = jnp.sum(box[...], axis=0, keepdims=True)
    for n, lev in enumerate(levs):
        cells = lev.X * n_x * lev.Y * n_y * lev.H * L
        eo[pl.ds(n, 1), :] = total[:, 4 * n : 4 * n + STEPS] / cells


def ready_rings(n_x, n_y):
    rings, reach = [], 2
    while reach < max(n_x, n_y) - 1:
        xs = (-reach, 0, reach) if reach < n_x - 1 else (0,)
        ys = (-reach, 0, reach) if reach < n_y - 1 else (0,)
        rings.append([(x, y) for x in xs for y in ys if x or y])
        reach *= 2
    return rings


def write_out(a, b, c, fine, coarse, energy, sem):
    pairs = [(a.at[i], fine.at[i]) for i in range(3)] + [(b.at[i], coarse.at[i]) for i in range(3)] + [(c, energy)]
    copies = [pltpu.make_async_copy(src, dst, sem.at[i]) for i, (src, dst) in enumerate(pairs)]
    for copy in copies:
        copy.start()
    for copy in copies:
        copy.wait()


def plane_rows(lc):
    return -(-(lc.X + 3) * (lc.Y + 3) // L) * L


def side_rows(lev, coarse):
    longer = max(lev.X, lev.Y)
    return [longer * len(side_pieces(lev, (-1, 0), coarse, step)) for step in (1, 0)]


def solution(mesh):
    n_x, n_y = mesh.shape["gx"], mesh.shape["gy"]

    def step(*args):
        lf, lc = Level(args[0].shape), Level(args[2].shape)
        sizes = [side_rows(lf, False), side_rows(lc, True)]
        corners = [corner_rows(lf, False), corner_rows(lc, True)]
        f32 = jnp.float32
        vm = lambda *s: pltpu.VMEM(s, f32)
        results = pl.pallas_call(
            functools.partial(kernel, n_x, n_y, lf, lc),
            out_shape=(
                vm(*args[0].shape),
                vm(*args[2].shape),
                vm(2, STEPS),
            ),
            in_specs=[pl.BlockSpec(memory_space=pl.ANY)] * len(args),
            out_specs=[pl.BlockSpec(memory_space=pltpu.VMEM)] * 3,
            scratch_shapes=(
                [pltpu.VMEM(a.shape, a.dtype) for a in args]
                + [vm(3 * lf.field_rows(), L)] * 3
                + [vm(3 * lc.field_rows(), L)] * 3
                + [
                    vm(11 * lf.field_rows(), L),
                    vm(11 * lc.field_rows(), L),
                    vm(3 * plane_rows(lc) + 8, L),
                    vm(3 * lf.Y, L),
                    pltpu.VMEM((lf.X * lf.Y, 3 * plane_rows(lc)), jnp.bfloat16),
                    vm(3 * lf.X * lf.Y, L),
                ]
                + [vm(4, size[1], L) for size in sizes] * 2
                + [vm(STEPS - 1, 4, size[0], L) for size in sizes] * 2
                + [vm(STEPS, 4, corner, L) for corner in corners] * 2
                + [
                    vm(8, L),
                    vm(1, L),
                    vm(n_x * n_y, L),
                    pltpu.SemaphoreType.DMA((4,)),
                    pltpu.SemaphoreType.DMA,
                    pltpu.SemaphoreType.DMA((2, STEPS, 2)),
                    pltpu.SemaphoreType.DMA,
                    pltpu.SemaphoreType.DMA,
                    pltpu.SemaphoreType.REGULAR((max(1, len(ready_rings(n_x, n_y))),)),
                ]
            ),
            compiler_params=pltpu.CompilerParams(
                collective_id=0, has_side_effects=True, vmem_limit_bytes=60 * 1024 * 1024
            ),
        )(*args)
        results = [pltpu.with_memory_space_constraint(r, pltpu.VMEM) for r in results]
        fine, coarse, energy = pl.pallas_call(
            write_out,
            out_shape=tuple(jax.ShapeDtypeStruct(r.shape, f32) for r in results),
            in_specs=[pl.BlockSpec(memory_space=pltpu.VMEM)] * 3,
            out_specs=[pl.BlockSpec(memory_space=pl.ANY)] * 3,
            scratch_shapes=[pltpu.SemaphoreType.DMA((7,))],
        )(*results)
        return fine, coarse, energy.T

    field, cells = P(None, "gx", "gy", None), P("gx", "gy", None)
    return jax.shard_map(
        step,
        mesh=mesh,
        in_specs=(field,) * 4 + (cells,) * 8 + (P(None, "gx", "gy"),),
        out_specs=(field, field, P()),
        check_vma=False,
    )
```

```python
import functools

import jax
import jax.numpy as jnp
from jax import lax
from jax.experimental import pallas as pl
from jax.experimental.pallas import tpu as pltpu
from jax.sharding import PartitionSpec as P

STEPS = 3
FACTOR = 0.15
MESH = pl.DeviceIdType.MESH
L = 128
SIDES = ((1, 0), (-1, 0), (0, 1), (0, -1))
CORNERS = ((1, 1), (1, -1), (-1, 1), (-1, -1))


class Level:
    def __init__(self, shape):
        _, self.X, self.Y, Z = shape
        self.H = Z // L
        self.XE = self.X + 4
        self.R = self.Y + 16
        while (self.H * self.R) % 8 != 4:
            self.R += 1
        self.NB = self.Y // 8

    def row(self, c, x, h, r):
        return ((c * self.XE + x) * self.H + h) * self.R + r

    def field_rows(self):
        return self.XE * self.H * self.R


def side_pieces(lev, d, coarse, step):
    out = [("u", c, h) for c in range(3) for h in range(lev.H)]
    out += [("div", 0, h) for h in range(lev.H)]
    if step == 0:
        out += [("wide", 0, h) for h in range(lev.H)]
    if coarse and d[0] + d[1] < 0:
        out += [("plane", 0, 0)]
    return out


def corner_extras(d):
    rings = [(a, b) for a in ((1, 2) if d[0] < 0 else (1,)) for b in ((1, 2) if d[1] < 0 else (1,))]
    return [(2, 1, 1)] + [(c, a, b) for a, b in rings if (a, b) != (1, 1) for c in range(3)]


def corner_rows(lev, coarse):
    return 2 * lev.H + int(coarse)


def inner(length, d, ring):
    return length - ring if d > 0 else ring - 1


def outer(length, d, ring):
    return -ring if d > 0 else length + ring - 1


def line(lev, d, ring, h, c, place):
    if d[0]:
        return lev.row(c, 2 + place(lev.X, d[0], ring), h, 8), lev.Y, 1
    return lev.row(c, 2, h, 8 + place(lev.Y, d[1], ring)), lev.X, lev.H * lev.R


def rows_of(start, count, stride):
    return pl.ds(start, count) if stride == 1 else pl.ds(start, count, stride)


def kernel(n_x, n_y, lf, lc, *refs):
    given, (fo, co, eo) = refs[:13], refs[13:16]
    held = refs[16:29]
    (fd, fp, cd, cp, fden, flam, frig, fmet, cden, clam, crig, cmet, offs) = held
    (uf0, uf1, uf2, uc0, uc1, uc2, mf, mc, plane, pair, wts, ghost,
     ss0f, ss0c, rs0f, rs0c, ssf, ssc, rsf, rsc, scf, scc, rcf, rcc,
     es, mine, box, load_sem, send_sem, recv_sem, en_send, en_recv, inside) = refs[29:]
    U = ((uf0, uf1, uf2), (uc0, uc1, uc2))
    M = (mf, mc)
    levs = (lf, lc)
    sside0, rside0, sside, rside = (ss0f, ss0c), (rs0f, rs0c), (ssf, ssc), (rsf, rsc)
    scorner, rcorner = (scf, scc), (rcf, rcc)
    disp, prev, out = (fd, cd), (fp, cp), (fo, co)
    den, lam, rig, met = (fden, cden), (flam, clam), (frig, crig), (fmet, cmet)
    ix, iy = lax.axis_index("gx"), lax.axis_index("gy")

    def has(d):
        conds = []
        if d[0] > 0:
            conds.append(ix < n_x - 1)
        if d[0] < 0:
            conds.append(ix > 0)
        if d[1] > 0:
            conds.append(iy < n_y - 1)
        if d[1] < 0:
            conds.append(iy > 0)
        return functools.reduce(jnp.logical_and, conds)

    DIRS = SIDES + CORNERS
    KG = plane_rows(lc)
    lane = lax.broadcasted_iota(jnp.int32, (8, L), 1)
    first, last = lane == 0, lane == L - 1

    IC, WIDE, FX, FY, FZP, FZM, A, B5, BZ, EN, DIV = range(11)

    def mrow(lev, name, x, h, r):
        return name * lev.field_rows() + (x * lev.H + h) * lev.R + r

    barrier = pltpu.get_barrier_semaphore()

    def signal(x, y):
        pl.semaphore_signal(barrier, inc=1, device_id={"gx": x, "gy": y}, device_id_type=MESH)

    everyone = n_x * n_y
    me = ix * n_y + iy

    greeted = jnp.int32(0)
    for d in DIRS:
        greeted = greeted + has(d).astype(jnp.int32)

        @pl.when(has(d))
        def _(d=d):
            signal(ix + d[0], iy + d[1])

    rings = ready_rings(n_x, n_y)

    def within(d):
        x, y = ix + d[0], iy + d[1]
        return (x >= 0) & (x < n_x) & (y >= 0) & (y < n_y)

    def ready_signal(i):
        for d in rings[i]:
            @pl.when(within(d))
            def _(d=d):
                pl.semaphore_signal(
                    inside.at[i], inc=1, device_id={"gx": ix + d[0], "gy": iy + d[1]}, device_id_type=MESH
                )

    def ready_wait(i):
        pl.semaphore_wait(inside.at[i], sum(within(d).astype(jnp.int32) for d in rings[i]))

    def coef(lev, h, rows):
        ln = lax.broadcasted_iota(jnp.int32, (rows, L), 1)
        value = jnp.full((rows, L), 0.5, jnp.float32)
        if h == 0:
            value = jnp.where(ln == 0, 1.0, value)
        if h == lev.H - 1:
            value = jnp.where(ln == L - 1, 1.0, value)
        return value

    def shifts(vals):
        n = len(vals)
        ups = [pltpu.roll(v, L - 1, 1) for v in vals]
        dns = [pltpu.roll(v, 1, 1) for v in vals]
        lane_v = lane if vals[0].shape[0] == 8 else lax.broadcasted_iota(jnp.int32, vals[0].shape, 1)
        fst, lst = lane_v == 0, lane_v == L - 1
        hi = [jnp.where(lst, ups[i + 1] if i + 1 < n else vals[i], ups[i]) for i in range(n)]
        lo = [jnp.where(fst, dns[i - 1] if i > 0 else vals[i], dns[i]) for i in range(n)]
        return hi, lo

    LOADS = ((2, 11, 10), (0, 7, 6), (1, 3, 4, 5, 8, 9), (12,))

    def load(group):
        for i in LOADS[group]:
            pltpu.make_async_copy(given[i], held[i], load_sem.at[group]).start()

    def wait_rows(sem, rows):
        span = mf.at[pl.ds(0, rows)]
        pltpu.make_async_copy(span, span, sem).wait()

    def loaded(group):
        if group == 3:
            pltpu.make_async_copy(given[12], held[12], load_sem.at[3]).wait()
        else:
            wait_rows(load_sem.at[group], sum(given[i].size // L for i in LOADS[group]))

    load(0)
    load(1)

    zero = jnp.zeros((8, L), jnp.float32)
    for lev, us, m in zip(levs, U, M):
        lines = lev.XE * lev.H

        @pl.loop(0, 3 * lines, unroll=4)
        def _(q, lev=lev, us=us):
            for u in us:
                u[pl.ds(q * lev.R, 8), :] = zero
                u[pl.ds(q * lev.R + lev.Y + 8, 8), :] = zero

        @pl.loop(0, lines, unroll=4)
        def _(q, lev=lev, m=m):
            for name in (WIDE, DIV):
                m[pl.ds(name * lev.field_rows() + q * lev.R, 8), :] = zero
                m[pl.ds(name * lev.field_rows() + q * lev.R + lev.Y + 8, 8), :] = zero

        for x in (0, 1, lev.X + 2, lev.X + 3):
            for h in range(lev.H):
                for b in range(lev.NB):
                    for u in us:
                        for c in range(3):
                            u[pl.ds(lev.row(c, x, h, 8 + 8 * b), 8), :] = zero
                    for name in (WIDE, DIV):
                        m[pl.ds(mrow(lev, name, x, h, 8 + 8 * b), 8), :] = zero

    @pl.loop(0, 3 * KG // 8, unroll=4)
    def _(q):
        plane[pl.ds(8 * q, 8), :] = zero

    plane[pl.ds(3 * KG, 8), :] = zero
    for k, d in enumerate(DIRS):
        @pl.when(jnp.logical_not(has((-d[0], -d[1]))))
        def _(k=k):
            for n in range(2):
                for step in range(STEPS):
                    if k >= 4:
                        rcorner[n][step, k - 4, :, :] = jnp.zeros(rcorner[n].shape[2:], jnp.float32)
                    elif step == 0:
                        rside0[n][k, :, :] = jnp.zeros(rside0[n].shape[1:], jnp.float32)
                    else:
                        rside[n][step - 1, k, :, :] = jnp.zeros(rside[n].shape[2:], jnp.float32)

    def take_in(n):
        lev, us, u_in, m = levs[n], U[n], disp[n], M[n]

        @pl.loop(0, lev.X, unroll=4)
        def _(x):
            for h in range(lev.H):
                for b in range(lev.NB):
                    src = (x, pl.ds(8 * b, 8), pl.ds(h * L, L))
                    g = met[n][src]
                    m[pl.ds(mrow(lev, IC, x + 2, h, 8 + 8 * b), 8), :] = (1.0 / g) * coef(lev, h, 8)
                    m[pl.ds(mrow(lev, WIDE, x + 2, h, 8 + 8 * b), 8), :] = rig[n][src] * g
                    for c in range(3):
                        us[0][pl.ds(lev.row(c, x + 2, h, 8 + 8 * b), 8), :] = u_in[(c,) + src]

    def side_size(n, d):
        return levs[n].Y if d[0] else levs[n].X

    def message_rows(k, step, n):
        if k >= 4:
            return corner_rows(levs[n], n == 1)
        return side_size(n, DIRS[k]) * len(side_pieces(levs[n], DIRS[k], n == 1, step))

    def copy(k, d, step, n):
        if k >= 4:
            s, r = scorner[n].at[step, k - 4], rcorner[n].at[step, k - 4]
        else:
            rows = pl.ds(0, message_rows(k, step, n))
            if step == 0:
                s, r = sside0[n].at[k, rows], rside0[n].at[k, rows]
            else:
                s, r = sside[n].at[step - 1, k, rows], rside[n].at[step - 1, k, rows]
        return pltpu.make_async_remote_copy(
            src_ref=s, dst_ref=r, send_sem=send_sem,
            recv_sem=recv_sem.at[n, step, int(k not in (2, 3))],
            device_id={"gx": ix + d[0], "gy": iy + d[1]}, device_id_type=MESH,
        )

    def wait_present(sem, which, rows_of_k, arriving):
        def options(i, n):
            low, high = i > 0, i < n - 1
            signs = (1, -1) if arriving else (-1, 1)
            return (
                (jnp.logical_and(low, high), (0, 1, -1)),
                (jnp.logical_and(low, jnp.logical_not(high)), (0, signs[0])),
                (jnp.logical_and(jnp.logical_not(low), high), (0, signs[1])),
            )

        along_x = options(ix, n_x) if any(DIRS[k][0] for k in which) else ((None, (0,)),)
        along_y = options(iy, n_y) if any(DIRS[k][1] for k in which) else ((None, (0,)),)
        for in_x, dxs in along_x:
            for in_y, dys in along_y:
                conds = [cond for cond in (in_x, in_y) if cond is not None]
                rows = sum(rows_of_k(k) for k in which if DIRS[k][0] in dxs and DIRS[k][1] in dys)

                @pl.when(functools.reduce(jnp.logical_and, conds))
                def _(rows=rows):
                    wait_rows(sem, rows)

    XS, YS, CS = (0, 1), (2, 3), (4, 5, 6, 7)

    def divergence(step, n, start, count, stride):
        lev, u, m = levs[n], U[n][step], M[n]
        SX, cs = lev.H * lev.R, lev.field_rows()
        get = lambda c, h, off: u[rows_of(start + c * cs + h * lev.R + off, count, stride), :]
        hi, lo = shifts([get(2, h, 0) for h in range(lev.H)])
        values = []
        for h in range(lev.H):
            v = 0.5 * ((get(0, h, SX) - get(0, h, -SX)) + (get(1, h, 1) - get(1, h, -1)))
            ic = m[rows_of(IC * cs + start + h * lev.R, count, stride), :]
            values.append(v + ic * (hi[h] - lo[h]))
        return values

    def lanes_of(rows):
        return lax.broadcasted_iota(jnp.int32, (rows, L), 1)

    def merged(values):
        total, ln = values[0], lanes_of(values[0].shape[0])
        for i, v in enumerate(values[1:], 1):
            total = jnp.where(ln == i, pltpu.roll(v, i, 1), total)
        return total

    def parted(value, i):
        return pltpu.roll(value, L - i, 1) if i else value

    def corner_row(lev, d, c, a, b, h, place):
        return pl.ds(lev.row(c, 2 + place(lev.X, d[0], a), h, 8 + place(lev.Y, d[1], b)), 1)

    def pack(step, n, which):
        lev, u, m = levs[n], U[n][step], M[n]
        for k in which:
            d = DIRS[k]
            if k >= 4:
                for c in range(2):
                    for h in range(lev.H):
                        scorner[n][step, k - 4, pl.ds(c * lev.H + h, 1), :] = u[
                            corner_row(lev, d, c, 1, 1, h, inner), :
                        ]
                if n:
                    extras = [u[corner_row(lev, d, c, a, b, 0, inner), :] for c, a, b in corner_extras(d)]
                    scorner[n][step, k - 4, pl.ds(2 * lev.H, 1), :] = merged(extras)
                continue
            size = side_size(n, d)
            parts = divergence(step, n, *line(lev, d, 1, 0, 0, inner))
            for at, (kind, c, h) in enumerate(side_pieces(lev, d, n == 1, step)):
                first_row, count, stride = line(lev, d, 1, h, c, inner)
                if kind == "u":
                    value = u[rows_of(first_row, count, stride), :]
                elif kind == "div":
                    value = parts[h]
                elif kind == "wide":
                    value = m[rows_of(WIDE * lev.field_rows() + first_row, count, stride), :]
                else:
                    value = merged([u[rows_of(*line(lev, d, 2, 0, e, inner)), :] for e in range(3)])
                if step == 0:
                    sside0[n][k, pl.ds(at * size, size), :] = value
                else:
                    sside[n][step - 1, k, pl.ds(at * size, size), :] = value

    def start(step, n, which):
        for k in which:
            @pl.when(has(DIRS[k]))
            def _(k=k):
                copy(k, DIRS[k], step, n).start()

    def start_far_first(n):
        for far in (1, -1):
            @pl.when(lax.rem(ix, 2) == (1 if far > 0 else 0))
            def _(far=far):
                for side in (far, -far):
                    start(0, n, [k for k in CS + XS if DIRS[k][0] == side])
        start(0, n, YS)

    def unpack(step, n, which):
        lev, u, m = levs[n], U[n][step], M[n]
        fr = lev.field_rows()
        for g, group in enumerate((YS, XS + CS)):
            if group[0] in which:
                wait_present(recv_sem.at[n, step, g], group, lambda k: message_rows(k, step, n), True)

        for k in which:
            d = DIRS[k]
            back = (-d[0], -d[1])
            if k >= 4:
                for c in range(2):
                    for h in range(lev.H):
                        value = rcorner[n][step, k - 4, pl.ds(c * lev.H + h, 1), :]
                        u[corner_row(lev, d, c, 1, 1, h, outer), :] = value
                        if c == 0:
                            beside = lev.row(0, 2 + inner(lev.X, back[0], 1), h, 8 + outer(lev.Y, d[1], 1))
                            sign = back[0]
                        else:
                            beside = lev.row(0, 2 + outer(lev.X, d[0], 1), h, 8 + inner(lev.Y, back[1], 1))
                            sign = back[1]
                        at = pl.ds(DIV * fr + beside, 1)
                        m[at, :] = m[at, :] + (0.5 * sign) * value
                if n:
                    value = rcorner[n][step, k - 4, pl.ds(2 * lev.H, 1), :]
                    for i, (c, a, b) in enumerate(corner_extras(d)):
                        u[corner_row(lev, d, c, a, b, 0, outer), :] = parted(value, i)
                continue
            axis, size = (0 if d[0] else 1), side_size(n, d)
            half = jnp.where(has(back), 0.5 * (d[0] + d[1]), 0.0)
            for at, (kind, c, h) in enumerate(side_pieces(lev, d, n == 1, step)):
                rows = pl.ds(at * size, size)
                got = rside0[n][k, rows, :] if step == 0 else rside[n][step - 1, k, rows, :]
                first_row, count, stride = line(lev, d, 1, h, c, outer)
                if kind == "u":
                    u[rows_of(first_row, count, stride), :] = got
                elif kind == "div":
                    own = u[rows_of(*line(lev, back, 1, h, axis, inner)), :]
                    m[rows_of(DIV * fr + first_row, count, stride), :] = got + half * own
                elif kind == "wide":
                    m[rows_of(WIDE * fr + first_row, count, stride), :] = got
                else:
                    for e in range(3):
                        u[rows_of(*line(lev, d, 2, 0, e, outer)), :] = parted(got, e)

    loaded(0)
    take_in(1)
    pack(0, 1, XS + CS + YS)
    pl.semaphore_wait(barrier, greeted)
    start_far_first(1)
    loaded(1)
    load(3)
    load(2)
    take_in(0)
    pack(0, 0, XS + CS + YS)
    loaded(3)

    X, Y = lf.X, lf.Y
    YE = lc.Y + 3
    sub = lax.broadcasted_iota(jnp.int32, (8, Y), 0)
    lan = lax.broadcasted_iota(jnp.int32, (8, Y), 1)
    row8 = lax.broadcasted_iota(jnp.int32, (8, KG), 0)
    cell = lax.broadcasted_iota(jnp.int32, (8, KG), 1)
    near_y = jnp.where(row8 % 2 == 0, 0.75, 0.25)
    cell_x = cell // YE
    cell_y = cell - cell_x * YE - row8 // 2

    def weight(o_all, shift, near):
        return jnp.where(o_all == shift, near, 0.0) + jnp.where(o_all + 1 == shift, 1.0 - near, 0.0)

    for x in range(X):
        near_x = 0.75 if x % 2 == 0 else 0.25
        for b in range(lf.NB):
            both = []
            for axis in range(2):
                o_row = jnp.broadcast_to(offs[axis, pl.ds(x, 1), :], (8, Y))
                o_col = jnp.sum(jnp.where(lan == sub + 8 * b, o_row, 0).astype(jnp.float32), axis=1, keepdims=True)
                both.append(jnp.broadcast_to(o_col, (8, KG)).astype(jnp.int32))
            w = weight(both[0], cell_x - (x // 2 + 1), near_x) * weight(both[1], cell_y - (4 * b + 1), near_y)
            for part in range(3):
                wts[pl.ds(x * Y + 8 * b, 8), pl.ds(part * KG, KG)] = w.astype(jnp.bfloat16)

    loaded(2)

    for n, lev in enumerate(levs):
        m = M[n]

        @pl.loop(0, lev.X, unroll=4)
        def _(x, n=n, lev=lev, m=m):
            for b in range(lev.NB):
                def at(name, h):
                    return pl.ds(mrow(lev, name, x + 2, h, 8 + 8 * b), 8)

                vs = []
                for h in range(lev.H):
                    src = (x, pl.ds(8 * b, 8), pl.ds(h * L, L))
                    g, de, la, ri = met[n][src], den[n][src], lam[n][src], rig[n][src]
                    rden = 1.0 / de
                    ic = m[at(IC, h), :]
                    inv = ic * (1.0 / coef(lev, h, 8))
                    bb = (FACTOR * (la + ri)) * rden
                    m[at(A, h), :] = FACTOR * inv * rden
                    m[at(B5, h), :] = 0.5 * bb
                    m[at(BZ, h), :] = bb * ic
                    m[at(EN, h), :] = de * g
                    vs.append(ri * inv)
                hi, lo = shifts(vs)
                for h in range(lev.H):
                    m[at(FZP, h), :] = 0.5 * (vs[h] + hi[h])
                    m[at(FZM, h), :] = 0.5 * (vs[h] + lo[h])

    def faces_x(n, xs):
        lev, m = levs[n], M[n]
        for x in xs:
            for h in range(lev.H):
                for b in range(lev.NB):
                    r = 8 + 8 * b
                    w0 = m[pl.ds(mrow(lev, WIDE, x + 1, h, r), 8), :]
                    w1 = m[pl.ds(mrow(lev, WIDE, x + 2, h, r), 8), :]
                    m[pl.ds(mrow(lev, FX, x + 1, h, r), 8), :] = 0.5 * (w0 + w1)

    def faces_y(n):
        lev, m = levs[n], M[n]

        @pl.loop(0, lev.X, unroll=4)
        def _(x):
            for h in range(lev.H):
                for b in range(lev.NB + 1):
                    r = 8 + 8 * b
                    w0 = m[pl.ds(mrow(lev, WIDE, x + 2, h, r - 1), 8), :]
                    w1 = m[pl.ds(mrow(lev, WIDE, x + 2, h, r), 8), :]
                    m[pl.ds(mrow(lev, FY, x + 2, h, r), 8), :] = 0.5 * (w0 + w1)

    def divergences(step, n, xs):
        lev, m = levs[n], M[n]

        def column(x):
            for b in range(lev.NB):
                values = divergence(step, n, lev.row(0, x + 2, 0, 8 + 8 * b), 8, 1)
                for h in range(lev.H):
                    m[pl.ds(mrow(lev, DIV, x + 2, h, 8 + 8 * b), 8), :] = values[h]

        for x in xs:
            column(x)

    def ghosts(step, late=False):
        uc = U[1][step]
        for c in range(3):
            for x in (0, lc.X + 1, lc.X + 2) if late else range(1, lc.X + 1):
                for q in range(0, YE, 8):
                    count = min(8, YE - q)
                    value = pltpu.roll(uc[pl.ds(lc.row(c, x + 1, 0, 7 + q), 8), :], L - 1, 1)
                    plane[pl.ds(c * KG + x * YE + q, count), :] = value[:count]
        for c in range(3):
            left, parts = plane[pl.ds(c * KG, KG), :], []
            for _ in range(3):
                parts.append(left.astype(jnp.bfloat16))
                left = left - parts[-1].astype(jnp.float32)
            whole = jnp.concatenate(parts, axis=0)
            for x, count in ((0, 2), (X - 4, 4)) if late else ((2, X - 6),):
                ghost[pl.ds((c * X + x) * Y, count * Y), :] = jnp.dot(
                    wts[pl.ds(x * Y, count * Y), :], whole, preferred_element_type=jnp.float32
                )

    def top_ghost(step, x, c):
        uf = U[0][step]
        base = c * lf.Y
        for b in range(lf.NB):
            pair[pl.ds(base + 8 * b, 8), :] = (
                uf[pl.ds(lf.row(c, 2 * x + 2, 0, 8 + 8 * b), 8), :]
                + uf[pl.ds(lf.row(c, 2 * x + 3, 0, 8 + 8 * b), 8), :]
            )
        s = pair[pl.ds(base, 8, 2), :] + pair[pl.ds(base + 1, 8, 2), :]
        return pltpu.roll(0.25 * s, 1, 1)

    def update(step, n, columns, inside_x=None):
        lev = levs[n]
        u, m = U[n][step], M[n]
        SX = lev.H * lev.R
        H = lev.H

        def body(x, acc, comps=(0, 1, 2)):
            for b in range(lev.NB):
                r0 = 8 + 8 * b

                def mat(name, h, off=0):
                    return m[pl.ds(mrow(lev, name, x + 2, h, r0) + off, 8), :]

                dhi, dlo = shifts([mat(DIV, h) for h in range(H)]) if 2 in comps else (None, None)
                fxp, fxm = [mat(FX, h) for h in range(H)], [mat(FX, h, -SX) for h in range(H)]
                fyp, fym = [mat(FY, h, 1) for h in range(H)], [mat(FY, h) for h in range(H)]
                fzp, fzm = [mat(FZP, h) for h in range(H)], [mat(FZM, h) for h in range(H)]
                scale = [mat(A, h) for h in range(H)]
                cells = [None] * H
                for c in comps:
                    get = lambda h, off=0, c=c: u[pl.ds(lev.row(c, x + 2, h, r0) + off, 8), :]
                    cur = [get(h) for h in range(H)]
                    hi, lo = shifts(cur)
                    if n == 0:
                        g = ghost[pl.ds(((c * lev.X + x) * lev.NB + b) * 8, 8), :]
                        hi[H - 1] = jnp.where(last, g, hi[H - 1])
                    else:
                        hi[H - 1] = jnp.where(last, 0.0, hi[H - 1])
                        lo[0] = jnp.where(first, top_ghost(step, x, c), lo[0])
                    for h in range(H):
                        v = cur[h]
                        flux = fxp[h] * (get(h, SX) - v) - fxm[h] * (v - get(h, -SX))
                        flux = flux + (fyp[h] * (get(h, 1) - v) - fym[h] * (v - get(h, -1)))
                        flux = flux + (fzp[h] * (hi[h] - v) - fzm[h] * (v - lo[h]))
                        if c == 0:
                            grad = mat(B5, h) * (mat(DIV, h, SX) - mat(DIV, h, -SX))
                        elif c == 1:
                            grad = mat(B5, h) * (mat(DIV, h, 1) - mat(DIV, h, -1))
                        else:
                            grad = mat(BZ, h) * (dhi[h] - dlo[h])
                        rate = scale[h] * flux + grad
                        if step == 0:
                            p = prev[n][c, x, pl.ds(8 * b, 8), pl.ds(h * L, L)]
                        else:
                            p = U[n][step - 1][pl.ds(lev.row(c, x + 2, h, r0), 8), :]
                        change = (v - p) + rate
                        new = v + change
                        if step == STEPS - 1:
                            out[n][c, x, pl.ds(8 * b, 8), pl.ds(h * L, L)] = new
                        else:
                            U[n][step + 1][pl.ds(lev.row(c, x + 2, h, r0), 8), :] = new
                        e = change * change - new * rate
                        cells[h] = e if cells[h] is None else cells[h] + e
                for h in range(H):
                    acc = acc + mat(EN, h) * cells[h]
            return acc

        acc = jnp.zeros((8, L), jnp.float32)
        for x, comps in columns:
            acc = body(x, acc, comps)
        if inside_x is not None:
            acc = lax.fori_loop(*inside_x, body, acc, unroll=4)
        row = pl.ds(4 * n + step, 1)
        es[row, :] = es[row, :] + jnp.sum(acc, axis=0, keepdims=True)

    es[...] = jnp.zeros((8, L), jnp.float32)
    start_far_first(0)
    ALL = (0, 1, 2)
    for n, lev in enumerate(levs):
        faces_x(n, range(1, lev.X))

    def coarse_start(step):
        unpack(step, 1, YS)
        if step == 0:
            faces_y(1)
        divergences(step, 1, range(1, lc.X - 1))
        update(step, 1, (), (2, lc.X - 2))

    def coarse_halo(step):
        unpack(step, 1, XS + CS)
        if step == 0:
            faces_x(1, (0, lc.X))
        divergences(step, 1, (0, lc.X - 1))

    for step in range(STEPS - 1):
        coarse_start(step)
        ghosts(step)
        coarse_halo(step)
        for far in (1, -1):
            @pl.when(lax.rem(ix, 2) == (1 if far > 0 else 0))
            def _(far=far, step=step):
                low, high = (0, 1), (lc.X - 2, lc.X - 1)
                for xs, side in (((high, 1), (low, -1)) if far > 0 else ((low, -1), (high, 1))):
                    update(step, 1, [(x, ALL) for x in xs])
                    which = [k for k in CS + XS if DIRS[k][0] == side]
                    pack(step + 1, 1, which)
                    start(step + 1, 1, which)

        pack(step + 1, 1, YS)
        start(step + 1, 1, YS)
        ghosts(step, True)
        unpack(step, 0, YS + XS + CS)
        if step == 0:
            faces_y(0)
            faces_x(0, (0, X))
        divergences(step, 0, (0, 1, 2, X - 3, X - 2, X - 1))
        update(step, 0, [(0, ALL), (X - 1, ALL), (1, (0,)), (X - 2, (0,))])
        pack(step + 1, 0, XS + CS)
        start(step + 1, 0, CS + XS)
        divergences(step, 0, range(3, X - 3))
        update(step, 0, [(1, (1, 2)), (X - 2, (1, 2))], (2, X - 2))
        pack(step + 1, 0, YS)
        start(step + 1, 0, YS)
        if step < len(rings):
            if step:
                ready_wait(step - 1)
            ready_signal(step)
    step = STEPS - 1
    coarse_start(step)
    ghosts(step)
    coarse_halo(step)
    update(step, 1, [(x, ALL) for x in (0, 1, lc.X - 2, lc.X - 1)])
    ghosts(step, True)
    unpack(step, 0, YS)
    divergences(step, 0, range(1, X - 1))
    update(step, 0, (), (2, X - 2))
    unpack(step, 0, XS + CS)
    divergences(step, 0, (0, X - 1))
    update(step, 0, [(x, ALL) for x in (0, 1, X - 2, X - 1)])
    for i in range(min(STEPS - 1, len(rings)) - 1, len(rings)):
        if i >= 0:
            ready_wait(i)
        if i + 1 < len(rings):
            ready_signal(i + 1)

    def share(x, y):
        return pltpu.make_async_remote_copy(
            src_ref=mine, dst_ref=box.at[pl.ds(me, 1)], send_sem=en_send, recv_sem=en_recv,
            device_id={"gx": x, "gy": y}, device_id_type=MESH,
        )

    def all_rows(sem):
        rows = box.at[pl.ds(0, everyone - 1)]
        return pltpu.make_async_copy(rows, rows, sem)

    sums = jnp.sum(es[...], axis=1, keepdims=True)
    diagonal = lane == lax.broadcasted_iota(jnp.int32, (8, L), 0)
    row = jnp.sum(jnp.where(diagonal, sums, 0.0), axis=0, keepdims=True)
    mine[...] = row

    def share_to(to):
        @pl.when(to != me)
        def _():
            share(lax.div(to, n_y), lax.rem(to, n_y)).start()

    if everyone > 64:
        pl.loop(0, everyone)(share_to)
    else:
        for to in range(everyone):
            share_to(jnp.int32(to))

    box[pl.ds(me, 1), :] = row

    wait_present(
        send_sem, range(8),
        lambda k: sum(message_rows(k, step, n) for step in range(STEPS) for n in range(2)), False,
    )
    all_rows(en_send).wait()
    all_rows(en_recv).wait()
    total = jnp.sum(box[...], axis=0, keepdims=True)
    for n, lev in enumerate(levs):
        cells = lev.X * n_x * lev.Y * n_y * lev.H * L
        eo[pl.ds(n, 1), :] = total[:, 4 * n : 4 * n + STEPS] / cells


def ready_rings(n_x, n_y):
    rings, reach = [], 2
    while reach < max(n_x, n_y) - 1:
        xs = (-reach, 0, reach) if reach < n_x - 1 else (0,)
        ys = (-reach, 0, reach) if reach < n_y - 1 else (0,)
        rings.append([(x, y) for x in xs for y in ys if x or y])
        reach *= 2
    return rings


def write_out(a, b, c, fine, coarse, energy, sem):
    pairs = [(a.at[i], fine.at[i]) for i in range(3)] + [(b.at[i], coarse.at[i]) for i in range(3)] + [(c, energy)]
    copies = [pltpu.make_async_copy(src, dst, sem.at[i]) for i, (src, dst) in enumerate(pairs)]
    for copy in copies:
        copy.start()
    for copy in copies:
        copy.wait()


def plane_rows(lc):
    return -(-(lc.X + 3) * (lc.Y + 3) // L) * L


def side_rows(lev, coarse):
    longer = max(lev.X, lev.Y)
    return [longer * len(side_pieces(lev, (-1, 0), coarse, step)) for step in (1, 0)]


def solution(mesh):
    n_x, n_y = mesh.shape["gx"], mesh.shape["gy"]

    def step(*args):
        lf, lc = Level(args[0].shape), Level(args[2].shape)
        sizes = [side_rows(lf, False), side_rows(lc, True)]
        corners = [corner_rows(lf, False), corner_rows(lc, True)]
        f32 = jnp.float32
        vm = lambda *s: pltpu.VMEM(s, f32)
        results = pl.pallas_call(
            functools.partial(kernel, n_x, n_y, lf, lc),
            out_shape=(
                vm(*args[0].shape),
                vm(*args[2].shape),
                vm(2, STEPS),
            ),
            in_specs=[pl.BlockSpec(memory_space=pl.ANY)] * len(args),
            out_specs=[pl.BlockSpec(memory_space=pltpu.VMEM)] * 3,
            scratch_shapes=(
                [pltpu.VMEM(a.shape, a.dtype) for a in args]
                + [vm(3 * lf.field_rows(), L)] * 3
                + [vm(3 * lc.field_rows(), L)] * 3
                + [
                    vm(11 * lf.field_rows(), L),
                    vm(11 * lc.field_rows(), L),
                    vm(3 * plane_rows(lc) + 8, L),
                    vm(3 * lf.Y, L),
                    pltpu.VMEM((lf.X * lf.Y, 3 * plane_rows(lc)), jnp.bfloat16),
                    vm(3 * lf.X * lf.Y, L),
                ]
                + [vm(4, size[1], L) for size in sizes] * 2
                + [vm(STEPS - 1, 4, size[0], L) for size in sizes] * 2
                + [vm(STEPS, 4, corner, L) for corner in corners] * 2
                + [
                    vm(8, L),
                    vm(1, L),
                    vm(n_x * n_y, L),
                    pltpu.SemaphoreType.DMA((4,)),
                    pltpu.SemaphoreType.DMA,
                    pltpu.SemaphoreType.DMA((2, STEPS, 2)),
                    pltpu.SemaphoreType.DMA,
                    pltpu.SemaphoreType.DMA,
                    pltpu.SemaphoreType.REGULAR((max(1, len(ready_rings(n_x, n_y))),)),
                ]
            ),
            compiler_params=pltpu.CompilerParams(
                collective_id=0, has_side_effects=True, vmem_limit_bytes=60 * 1024 * 1024
            ),
        )(*args)
        results = [pltpu.with_memory_space_constraint(r, pltpu.VMEM) for r in results]
        fine, coarse, energy = pl.pallas_call(
            write_out,
            out_shape=tuple(jax.ShapeDtypeStruct(r.shape, f32) for r in results),
            in_specs=[pl.BlockSpec(memory_space=pltpu.VMEM)] * 3,
            out_specs=[pl.BlockSpec(memory_space=pl.ANY)] * 3,
            scratch_shapes=[pltpu.SemaphoreType.DMA((7,))],
        )(*results)
        return fine, coarse, energy.T

    field, cells = P(None, "gx", "gy", None), P("gx", "gy", None)
    return jax.shard_map(
        step,
        mesh=mesh,
        in_specs=(field,) * 4 + (cells,) * 8 + (P(None, "gx", "gy"),),
        out_specs=(field, field, P()),
        check_vma=False,
    )
```
